128 devices in a mesh: tp: 4 (over x), sp: 32 (over z, y, core).
Axes of the slice: x: 4, y: 4, z: 4, core: 2. Of those that a mesh axis runs over, the one named last changes fastest.
Arguments:
- x_tok: bfloat16 [256, 3584], replicated
- seq_lens: int32 [256], replicated
- k_cache: bfloat16 [256, 1024, 4, 128], P(None, 'sp', 'tp')
- v_cache: bfloat16 [256, 1024, 4, 128], P(None, 'sp', 'tp')
- g_attn: bfloat16 [3584], replicated
- w_q: bfloat16 [3584, 3584], P(None, 'tp')
- w_k: bfloat16 [3584, 512], P(None, 'tp')
- w_v: bfloat16 [3584, 512], P(None, 'tp')
- w_o: bfloat16 [3584, 3584], P('tp')
- g_mlp: bfloat16 [3584], replicated
- w_gate: bfloat16 [3584, 18944], P(None, 'tp')
- w_up: bfloat16 [3584, 18944], P(None, 'tp')
- w_down: bfloat16 [18944, 3584], P('tp')
Outputs:
- output 1: bfloat16 [256, 3584], replicated
- output 2: bfloat16 [256, 1024, 4, 128], P(None, 'sp', 'tp')
- output 3: bfloat16 [256, 1024, 4, 128], P(None, 'sp', 'tp')
All inputs are finite; a program needn't handle non-finite values.
Results may differ from the reference program's by a relative error of at most 0.0140962.
Values sent between devices are 32-bit elements.
A program may use at most 1 GiB of HBM per device.

```python
import math
import jax
import jax.numpy as jnp
from jax import lax

MODEL_DIM = 3584
Q_HEADS = 28
KV_HEADS = 4
HEAD_DIM = 128
FF_DIM = 18944
BATCH_SIZE = 256
SEQ_LEN = 1024

ROPE_BASE = 500000.0
NORM_EPS = 1e-5


def gauss_draw(rng_key, arr_shape):
    return jax.random.normal(rng_key, arr_shape, jnp.float32)


def draw_lens(rng_key):
    low_len = SEQ_LEN // 4
    key_len, key_hi, key_lo = jax.random.split(rng_key, 3)
    lens_raw = jax.random.randint(key_len, (BATCH_SIZE,), low_len, SEQ_LEN)
    idx_hi = jax.random.randint(key_hi, (), 0, BATCH_SIZE)
    idx_lo = (idx_hi + jax.random.randint(key_lo, (), 1, BATCH_SIZE)) % BATCH_SIZE
    row_ids = jnp.arange(BATCH_SIZE)
    lens_raw = jnp.where(row_ids == idx_hi, SEQ_LEN - 1, lens_raw)
    lens_raw = jnp.where(row_ids == idx_lo, low_len, lens_raw)
    return lens_raw.astype(jnp.int32)


def setup_inputs(seed: int = 0) -> dict:
    key_list = jax.random.split(jax.random.key(seed), 14)
    q_width = Q_HEADS * HEAD_DIM
    kv_width = KV_HEADS * HEAD_DIM
    groups = Q_HEADS // KV_HEADS
    cache_shape = (BATCH_SIZE, SEQ_LEN, KV_HEADS, HEAD_DIM)
    w_q32 = gauss_draw(key_list[4], (MODEL_DIM, q_width)) * MODEL_DIM ** -0.5
    self_gain = (math.log(SEQ_LEN) - 0.6) * math.sqrt(groups / HEAD_DIM)
    group_sum = jnp.sum(w_q32.reshape(MODEL_DIM, KV_HEADS, groups, HEAD_DIM), axis=2).reshape(MODEL_DIM, kv_width)
    w_k32 = group_sum * (self_gain / math.sqrt(groups)) + gauss_draw(key_list[5], (MODEL_DIM, kv_width)) * (0.5 * MODEL_DIM ** -0.5)
    value_scale = 0.5 * math.sqrt(SEQ_LEN)
    return {
        "x_tok": gauss_draw(key_list[0], (BATCH_SIZE, MODEL_DIM)).astype(jnp.bfloat16),
        "seq_lens": draw_lens(key_list[1]),
        "k_cache": gauss_draw(key_list[2], cache_shape).astype(jnp.bfloat16),
        "v_cache": (gauss_draw(key_list[3], cache_shape) * value_scale).astype(jnp.bfloat16),
        "g_attn": (1.0 + 0.2 * gauss_draw(key_list[6], (MODEL_DIM,))).astype(jnp.bfloat16),
        "w_q": w_q32.astype(jnp.bfloat16),
        "w_k": w_k32.astype(jnp.bfloat16),
        "w_v": (gauss_draw(key_list[7], (MODEL_DIM, kv_width)) * MODEL_DIM ** -0.5).astype(jnp.bfloat16),
        "w_o": (gauss_draw(key_list[8], (q_width, MODEL_DIM)) * q_width ** -0.5).astype(jnp.bfloat16),
        "g_mlp": (1.0 + 0.2 * gauss_draw(key_list[9], (MODEL_DIM,))).astype(jnp.bfloat16),
        "w_gate": (gauss_draw(key_list[10], (MODEL_DIM, FF_DIM)) * MODEL_DIM ** -0.5).astype(jnp.bfloat16),
        "w_up": (gauss_draw(key_list[11], (MODEL_DIM, FF_DIM)) * MODEL_DIM ** -0.5).astype(jnp.bfloat16),
        "w_down": (gauss_draw(key_list[12], (FF_DIM, MODEL_DIM)) * FF_DIM ** -0.5).astype(jnp.bfloat16),
    }


def rms_norm(x_in, norm_gain):
    x_f32 = x_in.astype(jnp.float32)
    inv_rms = lax.rsqrt(jnp.mean(x_f32 * x_f32, axis=-1, keepdims=True) + NORM_EPS)
    return (x_f32 * inv_rms * norm_gain.astype(jnp.float32)).astype(jnp.bfloat16)


def apply_rope(heads_in, positions):
    head_dim = heads_in.shape[-1]
    half_dim = head_dim // 2
    inv_freq = jnp.power(jnp.float32(ROPE_BASE), jnp.arange(half_dim, dtype=jnp.float32) * (-2.0 / head_dim))
    angles = positions.astype(jnp.float32)[:, None, None] * inv_freq
    cos_a = jnp.cos(angles)
    sin_a = jnp.sin(angles)
    heads_f32 = heads_in.astype(jnp.float32)
    first_half = heads_f32[..., :half_dim]
    second_half = heads_f32[..., half_dim:]
    rotated = jnp.concatenate([first_half * cos_a - second_half * sin_a, second_half * cos_a + first_half * sin_a], axis=-1)
    return rotated.astype(jnp.bfloat16)


def reference(x_tok, seq_lens, k_cache, v_cache, g_attn, w_q, w_k, w_v, w_o, g_mlp, w_gate, w_up, w_down):
    groups = Q_HEADS // KV_HEADS
    x_norm = rms_norm(x_tok, g_attn)
    q_new = jnp.dot(x_norm, w_q, preferred_element_type=jnp.float32).astype(jnp.bfloat16).reshape(BATCH_SIZE, Q_HEADS, HEAD_DIM)
    k_new = jnp.dot(x_norm, w_k, preferred_element_type=jnp.float32).astype(jnp.bfloat16).reshape(BATCH_SIZE, KV_HEADS, HEAD_DIM)
    v_new = jnp.dot(x_norm, w_v, preferred_element_type=jnp.float32).astype(jnp.bfloat16).reshape(BATCH_SIZE, KV_HEADS, HEAD_DIM)
    q_rot = apply_rope(q_new, seq_lens)
    k_rot = apply_rope(k_new, seq_lens)
    row_ids = jnp.arange(BATCH_SIZE)
    k_out = k_cache.at[row_ids, seq_lens].set(k_rot)
    v_out = v_cache.at[row_ids, seq_lens].set(v_new)
    score_scale = HEAD_DIM ** -0.5

    def attend_row(row_inputs):
        q_row, k_rows, v_rows, row_len = row_inputs
        scores = jnp.einsum("kgd,tkd->kgt", q_row.astype(jnp.float32), k_rows.astype(jnp.float32)) * score_scale
        is_valid = jnp.arange(SEQ_LEN) <= row_len
        masked = jnp.where(is_valid, scores, -jnp.inf)
        row_max = jnp.max(masked, axis=-1, keepdims=True)
        weights = jnp.exp(masked - row_max)
        row_sum = jnp.sum(weights, axis=-1, keepdims=True)
        mixed = jnp.einsum("kgt,tkd->kgd", weights.astype(jnp.bfloat16).astype(jnp.float32), v_rows.astype(jnp.float32))
        return (mixed / row_sum).astype(jnp.bfloat16)

    attn_heads = lax.map(attend_row, (q_rot.reshape(BATCH_SIZE, KV_HEADS, groups, HEAD_DIM), k_out, v_out, seq_lens))
    attn_flat = attn_heads.reshape(BATCH_SIZE, Q_HEADS * HEAD_DIM)
    attn_proj = jnp.dot(attn_flat, w_o, preferred_element_type=jnp.float32)
    hidden = (x_tok.astype(jnp.float32) + attn_proj).astype(jnp.bfloat16)
    h_norm = rms_norm(hidden, g_mlp)
    gate_proj = jnp.dot(h_norm, w_gate, preferred_element_type=jnp.float32).astype(jnp.bfloat16)
    up_proj = jnp.dot(h_norm, w_up, preferred_element_type=jnp.float32).astype(jnp.bfloat16)
    act_prod = (jax.nn.silu(gate_proj.astype(jnp.float32)) * up_proj.astype(jnp.float32)).astype(jnp.bfloat16)
    mlp_out = jnp.dot(act_prod, w_down, preferred_element_type=jnp.float32)
    y_out = (hidden.astype(jnp.float32) + mlp_out).astype(jnp.bfloat16)
    return (y_out, k_out, v_out)
```

```python
import functools

import jax
import jax.numpy as jnp
from jax import lax
from jax.experimental import pallas as pl
from jax.experimental.pallas import tpu as pltpu
from jax.sharding import PartitionSpec as P

ROPE_BASE = 500000.0
NORM_EPS = 1e-5
MESH = pl.DeviceIdType.MESH
F32 = jnp.float32
BF16 = jnp.bfloat16
NX, NZ, NY, NC = 4, 4, 4, 2
LANE = 128


def rms_norm(x_in, norm_gain):
    x_f32 = x_in.astype(F32)
    inv_rms = lax.rsqrt(jnp.mean(x_f32 * x_f32, axis=-1, keepdims=True) + NORM_EPS)
    return (x_f32 * inv_rms * norm_gain.astype(F32)).astype(BF16)


def apply_rope(heads_in, positions):
    head_dim = heads_in.shape[-1]
    half_dim = head_dim // 2
    inv_freq = jnp.power(F32(ROPE_BASE), jnp.arange(half_dim, dtype=F32) * (-2.0 / head_dim))
    angles = positions.astype(F32)[:, None, None] * inv_freq
    cos_a = jnp.cos(angles)
    sin_a = jnp.sin(angles)
    heads_f32 = heads_in.astype(F32)
    first_half = heads_f32[..., :half_dim]
    second_half = heads_f32[..., half_dim:]
    rotated = jnp.concatenate([first_half * cos_a - second_half * sin_a, second_half * cos_a + first_half * sin_a], axis=-1)
    return rotated.astype(BF16)


def coords():
    s = lax.axis_index("sp")
    return lax.axis_index("tp"), s // (NY * NC), (s // NC) % NY, s % NC


def dev(x, z, y, c):
    return (x, (z * NY + y) * NC + c)


def turn(v, d, n):
    return lax.rem(v + d, n)


def entry_barrier(peers):
    barrier = pltpu.get_barrier_semaphore()
    for peer in peers:
        pl.semaphore_signal(barrier, inc=1, device_id=peer, device_id_type=MESH)
    pl.semaphore_wait(barrier, len(peers))


def remote(src, dst, send_sem, recv_sem, peer):
    return pltpu.make_async_remote_copy(
        src_ref=src, dst_ref=dst, send_sem=send_sem, recv_sem=recv_sem, device_id=peer, device_id_type=MESH
    )


def row_chunk(z, y, c):
    return (z * NC + c) * NY + y


def combine_kernel(in_ref, out_ref, slots, send_sem, recv_sem):
    x, z, y, c = coords()
    hops = [(dz, dy, dc) for dz in range(NZ) for dy in range(NY) for dc in range(NC)][1:]
    peers = [(turn(z, dz, NZ), turn(y, dy, NY), turn(c, dc, NC)) for dz, dy, dc in hops]
    entry_barrier([dev(x, *p) for p in peers])
    copies = []
    for k, p in enumerate(peers):
        rows = pl.ds(pl.multiple_of(row_chunk(*p) * 8, 8), 8)
        copies.append(remote(in_ref.at[rows, :], slots.at[k], send_sem.at[k], recv_sem.at[k], dev(x, *p)))
    for copy in copies:
        copy.start()
    heads = out_ref.shape[1] // LANE
    hd = heads * LANE
    mine = pl.ds(pl.multiple_of(row_chunk(z, y, c) * 8, 8), 8)
    top = in_ref[mine, hd:]
    for k, copy in enumerate(copies):
        copy.wait_recv()
    for k in range(len(copies)):
        top = jnp.maximum(top, slots[k, :, hd:])

    def add(stats, mix, acc, total):
        factor = jnp.exp(stats - top)
        total = total + pltpu.roll(factor, LANE // 2, 1) * stats
        parts = [acc[:, h * LANE:(h + 1) * LANE] + factor[:, h:h + 1] * mix[:, h * LANE:(h + 1) * LANE] for h in range(heads)]
        return jnp.concatenate(parts, axis=1), total

    acc, total = add(in_ref[mine, hd:], in_ref[mine, :hd], jnp.zeros((8, hd), F32), jnp.zeros((8, LANE), F32))

    def body(k, carry):
        return add(slots[k, :, hd:], slots[k, :, :hd], *carry)

    acc, total = lax.fori_loop(0, len(copies), body, (acc, total))
    half = LANE // 2
    out = [acc[:, h * LANE:(h + 1) * LANE] / total[:, half + h:half + h + 1] for h in range(heads)]
    out_ref[...] = jnp.concatenate(out, axis=1).astype(out_ref.dtype)
    for copy in copies:
        copy.wait_send()


def combine(packed, heads):
    width = packed.shape[1]
    return pl.pallas_call(
        combine_kernel,
        name="combine",
        out_shape=jax.ShapeDtypeStruct((8, heads * LANE), BF16),
        in_specs=[pl.BlockSpec(memory_space=pltpu.VMEM)],
        out_specs=pl.BlockSpec(memory_space=pltpu.VMEM),
        scratch_shapes=[
            pltpu.VMEM((31, 8, width), F32),
            pltpu.SemaphoreType.DMA((31,)),
            pltpu.SemaphoreType.DMA((31,)),
        ],
        compiler_params=pltpu.CompilerParams(collective_id=0, has_side_effects=True),
    )(packed)


XY = [(dx, dy) for dx in range(NX) for dy in range(NY)][1:]


def hidden_kernel(part_ref, res_ref, hid_ref, slots, chunk, rs_send, rs_recv, ag_send, ag_recv):
    x, z, y, c = coords()
    w = chunk.shape[1]
    plane = [(turn(x, dx, NX), turn(y, dy, NY)) for dx, dy in XY]
    entry_barrier([dev(px, z, py, c) for px, py in plane])
    rs = []
    for k in range(1, NX):
        px = turn(x, k, NX)
        cols = pl.ds(pl.multiple_of(px * w, LANE), w)
        rs.append(remote(part_ref.at[:, cols], slots.at[k - 1], rs_send.at[k - 1], rs_recv.at[k - 1], dev(px, z, y, c)))
    for copy in rs:
        copy.start()
    my_cols = pl.ds(pl.multiple_of(x * w, LANE), w)
    my_rows = pl.ds(pl.multiple_of(y * 8, 8), 8)
    total = part_ref[:, my_cols]
    for k, copy in enumerate(rs):
        copy.wait_recv()
        total = total + slots[k]
    hidden = (res_ref[...] + total).astype(BF16).astype(F32)
    chunk[...] = hidden
    ag = []
    for k, (px, py) in enumerate(plane):
        ag.append(remote(chunk, hid_ref.at[my_rows, my_cols], ag_send.at[k], ag_recv.at[k], dev(px, z, py, c)))
    for copy in ag:
        copy.start()
    hid_ref[my_rows, my_cols] = hidden
    for copy in ag:
        copy.wait_recv()
    for copy in rs + ag:
        copy.wait_send()


def gather_hidden(part, res):
    width = part.shape[1]
    w = width // NX
    return pl.pallas_call(
        hidden_kernel,
        name="gather_hidden",
        out_shape=jax.ShapeDtypeStruct((8 * NY, width), F32),
        in_specs=[pl.BlockSpec(memory_space=pltpu.VMEM)] * 2,
        out_specs=pl.BlockSpec(memory_space=pltpu.VMEM),
        scratch_shapes=[
            pltpu.VMEM((NX - 1, 8, w), F32),
            pltpu.VMEM((8, w), F32),
            pltpu.SemaphoreType.DMA((NX - 1,)),
            pltpu.SemaphoreType.DMA((NX - 1,)),
            pltpu.SemaphoreType.DMA((15,)),
            pltpu.SemaphoreType.DMA((15,)),
        ],
        compiler_params=pltpu.CompilerParams(collective_id=1, has_side_effects=True),
    )(part, res)


WIN = 256


def mlp_kernel(hid_ref, g_ref, wg_hbm, wu_hbm, wd_hbm, out_ref, wg, wu, wd, hn, sem):
    _, _, y, _ = coords()
    steps = wg.shape[0]
    ff_tiles = wg_hbm.shape[1] // LANE
    win_tiles = steps * WIN // LANE
    lo = (y * ff_tiles + NY - 1) // NY
    hi = ((y + 1) * ff_tiles + NY - 1) // NY
    first = jnp.minimum(lo, ff_tiles - win_tiles)
    base = first * LANE

    def fetch(i):
        cols = pl.ds(pl.multiple_of(base + i * WIN, LANE), WIN)
        return (
            pltpu.make_async_copy(wg_hbm.at[:, cols], wg.at[i], sem.at[0, i]),
            pltpu.make_async_copy(wu_hbm.at[:, cols], wu.at[i], sem.at[1, i]),
            pltpu.make_async_copy(wd_hbm.at[cols, :], wd.at[i], sem.at[2, i]),
        )

    for i in range(steps):
        for copy in fetch(i):
            copy.start()
    hid = hid_ref[...]
    inv = lax.rsqrt(jnp.mean(hid * hid, axis=-1, keepdims=True) + NORM_EPS)
    hn[...] = (hid * inv * g_ref[...].astype(F32)).astype(BF16)
    out_ref[...] = jnp.zeros_like(out_ref)

    def body(i, carry):
        cg, cu, cd = fetch(i)
        cg.wait()
        gate = jnp.dot(hn[...], wg[i], preferred_element_type=F32).astype(BF16).astype(F32)
        cu.wait()
        up = jnp.dot(hn[...], wu[i], preferred_element_type=F32).astype(BF16).astype(F32)
        act = jax.nn.silu(gate) * up
        col = lax.broadcasted_iota(jnp.int32, act.shape, 1) + (base + i * WIN)
        act = jnp.where((col >= lo * LANE) & (col < hi * LANE), act, 0.0).astype(BF16)
        cd.wait()
        out_ref[...] += jnp.dot(act, wd[i], preferred_element_type=F32)
        return carry

    lax.fori_loop(0, steps, body, 0)


def mlp(hid, g, wg, wu, wd):
    rows, width = hid.shape
    ff_tiles = wg.shape[1] // LANE
    steps = -(-(-(-ff_tiles // NY)) * LANE // WIN)
    return pl.pallas_call(
        mlp_kernel,
        name="mlp",
        out_shape=jax.ShapeDtypeStruct((rows, width), F32),
        in_specs=[pl.BlockSpec(memory_space=pltpu.VMEM)] * 2 + [pl.BlockSpec(memory_space=pl.ANY)] * 3,
        out_specs=pl.BlockSpec(memory_space=pltpu.VMEM),
        scratch_shapes=[
            pltpu.VMEM((steps, width, WIN), BF16),
            pltpu.VMEM((steps, width, WIN), BF16),
            pltpu.VMEM((steps, WIN, width), BF16),
            pltpu.VMEM((rows, width), BF16),
            pltpu.SemaphoreType.DMA((3, steps)),
        ],
        compiler_params=pltpu.CompilerParams(vmem_limit_bytes=48 * 2**20),
        cost_estimate=pl.CostEstimate(flops=6 * rows * width * steps * WIN, bytes_accessed=6 * width * steps * WIN, transcendentals=0),
    )(hid, g.reshape(1, -1), wg, wu, wd)


def output_kernel(part_ref, hid_ref, buf, slots, chunk, rs_send, rs_recv, p1_send, p1_recv, p2_send, p2_recv, cc_send, cc_recv):
    x, z, y, c = coords()
    w = chunk.shape[1]
    cut = [(0, 256), (256, 256), (512, w - 512)]
    plane = [(turn(x, dx, NX), turn(y, dy, NY)) for dx, dy in XY]
    first = [
        [(turn(x, a, NX), z, turn(y, b, NY)) for a, b in XY],
        [(x, turn(z, a, NZ), turn(y, b, NY)) for a, b in XY],
        [(turn(x, a, NX), turn(z, b, NZ), y) for a, b in XY],
    ]
    second = [
        [(x, turn(z, k, NZ), y) for k in range(1, 4)],
        [(turn(x, k, NX), z, y) for k in range(1, 4)],
        [(x, z, turn(y, k, NY)) for k in range(1, 4)],
    ]
    partner = dev(x, z, y, turn(c, 1, NC))
    near = [(turn(x, a, NX), z, turn(y, b, NY)) for a, b in XY]
    near += [(x, turn(z, a, NZ), turn(y, b, NY)) for a in range(1, NZ) for b in range(NY)]
    near += [(turn(x, a, NX), turn(z, b, NZ), y) for a in range(1, NX) for b in range(1, NZ)]
    entry_barrier([dev(*p, c) for p in near] + [partner])
    rs = []
    for k, (px, py) in enumerate(plane):
        rows = pl.ds(pl.multiple_of(py * 8, 8), 8)
        cols = pl.ds(pl.multiple_of(px * w, LANE), w)
        rs.append(remote(part_ref.at[rows, cols], slots.at[k], rs_send.at[k], rs_recv.at[k], dev(px, z, py, c)))
    for copy in rs:
        copy.start()
    my_rows = pl.ds(pl.multiple_of(y * 8, 8), 8)
    my_cols = pl.ds(pl.multiple_of(x * w, LANE), w)
    total = part_ref[my_rows, my_cols]
    for k, copy in enumerate(rs):
        copy.wait_recv()
        total = total + slots[k]
    out = (hid_ref[my_rows, my_cols] + total).astype(BF16).astype(F32)
    chunk[...] = out
    p1 = []
    for part, (lo, n) in enumerate(cut):
        for k, p in enumerate(first[part]):
            src = chunk.at[:, lo:lo + n]
            dst = buf.at[z, c, y, x, :, lo:lo + n]
            p1.append(remote(src, dst, p1_send.at[part, k], p1_recv.at[part, k], dev(*p, c)))
    for copy in p1:
        copy.start()
    buf[z, c, y, x] = out
    p2 = []
    for part, (lo, n) in enumerate(cut):
        for copy in p1[part * 15:(part + 1) * 15]:
            copy.wait_recv()
        block = [
            buf.at[z, c, :, :, :, lo:lo + n],
            buf.at[:, c, :, x, :, lo:lo + n],
            buf.at[:, c, y, :, :, lo:lo + n],
        ][part]
        for k, p in enumerate(second[part]):
            copy = remote(block, block, p2_send.at[part, k], p2_recv.at[part, k], dev(*p, c))
            copy.start()
            p2.append(copy)
    for copy in p2:
        copy.wait_recv()
    across = remote(buf.at[:, c], buf.at[:, c], cc_send, cc_recv, partner)
    across.start()
    across.wait_recv()
    for copy in rs + p1 + p2 + [across]:
        copy.wait_send()


def gather_output(part, hid):
    width = part.shape[1]
    w = width // NX
    sem = pltpu.SemaphoreType.DMA
    return pl.pallas_call(
        output_kernel,
        name="gather_output",
        out_shape=jax.ShapeDtypeStruct((NZ, NC, NY, NX, 8, w), F32),
        in_specs=[pl.BlockSpec(memory_space=pltpu.VMEM)] * 2,
        out_specs=pl.BlockSpec(memory_space=pltpu.VMEM),
        scratch_shapes=[
            pltpu.VMEM((15, 8, w), F32),
            pltpu.VMEM((8, w), F32),
            sem((15,)), sem((15,)), sem((3, 15)), sem((3, 15)), sem((3, 3)), sem((3, 3)), sem, sem,
        ],
        compiler_params=pltpu.CompilerParams(collective_id=2, has_side_effects=True),
    )(part, hid)


def solution(mesh):
    cache_spec = P(None, "sp", "tp", None)
    col_spec = P(None, "tp")
    row_spec = P("tp", None)
    full_spec = P()

    def local_step(x_tok, seq_lens, k_blk, v_blk, g_attn, wq_loc, wk_loc, wv_loc, wo_loc, g_mlp, wg_loc, wu_loc, wd_loc):
        batch_rows, seq_blk, kv_loc, head_dim = k_blk.shape
        q_loc = wq_loc.shape[1] // head_dim
        groups = q_loc // kv_loc
        x, z, y, c = coords()
        w = x_tok.shape[1] // NX
        res = lax.dynamic_slice(x_tok, (row_chunk(z, y, c) * 8, x * w), (8, w)).astype(F32)
        x_norm = rms_norm(x_tok, g_attn)
        q_new = jnp.dot(x_norm, wq_loc, preferred_element_type=F32).astype(BF16).reshape(batch_rows, q_loc, head_dim)
        k_new = jnp.dot(x_norm, wk_loc, preferred_element_type=F32).astype(BF16).reshape(batch_rows, kv_loc, head_dim)
        v_new = jnp.dot(x_norm, wv_loc, preferred_element_type=F32).astype(BF16).reshape(batch_rows, kv_loc, head_dim)
        q_rot = apply_rope(q_new, seq_lens)
        k_rot = apply_rope(k_new, seq_lens)
        local_pos = lax.axis_index("sp") * seq_blk + jnp.arange(seq_blk)
        is_new = (local_pos[None, :] == seq_lens[:, None])[:, :, None, None]
        k_out = jnp.where(is_new, k_rot[:, None], k_blk)
        v_out = jnp.where(is_new, v_new[:, None], v_blk)
        q_grp = q_rot.reshape(batch_rows, kv_loc, groups, head_dim)
        scores = jnp.einsum("bkgd,bskd->bkgs", q_grp, k_out, preferred_element_type=F32) * (head_dim ** -0.5)
        is_valid = (local_pos[None, :] <= seq_lens[:, None])[:, None, None, :]
        masked = jnp.where(is_valid, scores, -1e30)
        blk_max = jnp.max(masked, axis=-1, keepdims=True)
        weights = jnp.where(is_valid, jnp.exp(masked - blk_max), 0.0)
        blk_sum = jnp.sum(weights, axis=-1, keepdims=True)
        blk_mix = jnp.einsum("bkgs,bskd->bkgd", weights.astype(BF16), v_out, preferred_element_type=F32)
        half = LANE // 2
        pad = jnp.zeros((batch_rows, half - q_loc), F32)
        packed = jnp.concatenate(
            [blk_mix.reshape(batch_rows, q_loc * head_dim), blk_max.reshape(batch_rows, q_loc), pad, blk_sum.reshape(batch_rows, q_loc), pad], axis=1
        )
        attn_out = combine(packed, q_loc)
        part = jnp.dot(attn_out, wo_loc, preferred_element_type=F32)
        hid = gather_hidden(part, res)
        mlp_part = mlp(hid, g_mlp, wg_loc, wu_loc, wd_loc)
        buf = gather_output(mlp_part, hid)
        y_out = buf.transpose(0, 1, 2, 4, 3, 5).reshape(x_tok.shape).astype(BF16)
        return y_out, k_out, v_out

    return jax.shard_map(local_step, mesh=mesh, in_specs=(full_spec, full_spec, cache_spec, cache_spec, full_spec, col_spec, col_spec, col_spec, row_spec, full_spec, col_spec, col_spec, row_spec), out_specs=(full_spec, cache_spec, cache_spec), check_vma=False)
```

```python
import functools

import jax
import jax.numpy as jnp
from jax import lax
from jax.experimental import pallas as pl
from jax.experimental.pallas import tpu as pltpu
from jax.sharding import PartitionSpec as P

ROPE_BASE = 500000.0
NORM_EPS = 1e-5
MESH = pl.DeviceIdType.MESH
F32 = jnp.float32
BF16 = jnp.bfloat16
NX, NZ, NY, NC = 4, 4, 4, 2
LANE = 128


def coords():
    s = lax.axis_index("sp")
    return lax.axis_index("tp"), s // (NY * NC), (s // NC) % NY, s % NC


def dev(x, z, y, c):
    return (x, (z * NY + y) * NC + c)


def turn(v, d, n):
    return lax.rem(v + d, n)


def entry_barrier(peers):
    barrier = pltpu.get_barrier_semaphore()
    for peer in peers:
        pl.semaphore_signal(barrier, inc=1, device_id=peer, device_id_type=MESH)
    pl.semaphore_wait(barrier, len(peers))


def remote(src, dst, send_sem, recv_sem, peer):
    return pltpu.make_async_remote_copy(
        src_ref=src, dst_ref=dst, send_sem=send_sem, recv_sem=recv_sem, device_id=peer, device_id_type=MESH
    )


def row_chunk(z, y, c):
    return (z * NC + c) * NY + y


def combine_kernel(in_ref, out_ref, slots, send_sem, recv_sem):
    x, z, y, c = coords()
    hops = [(dz, dy, dc) for dz in range(NZ) for dy in range(NY) for dc in range(NC)][1:]
    peers = [(turn(z, dz, NZ), turn(y, dy, NY), turn(c, dc, NC)) for dz, dy, dc in hops]
    entry_barrier([dev(x, *p) for p in peers])
    copies = []
    for k, p in enumerate(peers):
        rows = pl.ds(pl.multiple_of(row_chunk(*p) * 8, 8), 8)
        copies.append(remote(in_ref.at[rows, :], slots.at[k], send_sem.at[k], recv_sem.at[k], dev(x, *p)))
    for copy in copies:
        copy.start()
    heads = out_ref.shape[1] // LANE
    hd = heads * LANE
    mine = pl.ds(pl.multiple_of(row_chunk(z, y, c) * 8, 8), 8)
    top = in_ref[mine, hd:]
    for k, copy in enumerate(copies):
        copy.wait_recv()
    for k in range(len(copies)):
        top = jnp.maximum(top, slots[k, :, hd:])

    def add(stats, mix, acc, total):
        factor = jnp.exp(stats - top)
        total = total + pltpu.roll(factor, LANE // 2, 1) * stats
        parts = [acc[:, h * LANE:(h + 1) * LANE] + factor[:, h:h + 1] * mix[:, h * LANE:(h + 1) * LANE] for h in range(heads)]
        return jnp.concatenate(parts, axis=1), total

    acc, total = add(in_ref[mine, hd:], in_ref[mine, :hd], jnp.zeros((8, hd), F32), jnp.zeros((8, LANE), F32))

    def body(k, carry):
        return add(slots[k, :, hd:], slots[k, :, :hd], *carry)

    acc, total = lax.fori_loop(0, len(copies), body, (acc, total))
    half = LANE // 2
    out = [acc[:, h * LANE:(h + 1) * LANE] / total[:, half + h:half + h + 1] for h in range(heads)]
    out_ref[...] = jnp.concatenate(out, axis=1).astype(out_ref.dtype)
    for copy in copies:
        copy.wait_send()


def combine(packed, heads):
    width = packed.shape[1]
    return pl.pallas_call(
        combine_kernel,
        name="combine",
        out_shape=jax.ShapeDtypeStruct((8, heads * LANE), BF16),
        in_specs=[pl.BlockSpec(memory_space=pltpu.VMEM)],
        out_specs=pl.BlockSpec(memory_space=pltpu.VMEM),
        scratch_shapes=[
            pltpu.VMEM((31, 8, width), F32),
            pltpu.SemaphoreType.DMA((31,)),
            pltpu.SemaphoreType.DMA((31,)),
        ],
        compiler_params=pltpu.CompilerParams(collective_id=0, has_side_effects=True),
    )(packed)


XY = [(dx, dy) for dx in range(NX) for dy in range(NY)][1:]


def hidden_kernel(part_ref, res_ref, hid_ref, slots, chunk, rs_send, rs_recv, ag_send, ag_recv):
    x, z, y, c = coords()
    w = chunk.shape[1]
    plane = [(turn(x, dx, NX), turn(y, dy, NY)) for dx, dy in XY]
    entry_barrier([dev(px, z, py, c) for px, py in plane])
    rs = []
    for k in range(1, NX):
        px = turn(x, k, NX)
        cols = pl.ds(pl.multiple_of(px * w, LANE), w)
        rs.append(remote(part_ref.at[:, cols], slots.at[k - 1], rs_send.at[k - 1], rs_recv.at[k - 1], dev(px, z, y, c)))
    for copy in rs:
        copy.start()
    my_cols = pl.ds(pl.multiple_of(x * w, LANE), w)
    my_rows = pl.ds(pl.multiple_of(y * 8, 8), 8)
    total = part_ref[:, my_cols]
    for k, copy in enumerate(rs):
        copy.wait_recv()
        total = total + slots[k]
    hidden = (res_ref[...] + total).astype(BF16).astype(F32)
    chunk[...] = hidden
    ag = []
    for k, (px, py) in enumerate(plane):
        ag.append(remote(chunk, hid_ref.at[my_rows, my_cols], ag_send.at[k], ag_recv.at[k], dev(px, z, py, c)))
    for copy in ag:
        copy.start()
    hid_ref[my_rows, my_cols] = hidden
    for copy in ag:
        copy.wait_recv()
    for copy in rs + ag:
        copy.wait_send()


def gather_hidden(part, res):
    width = part.shape[1]
    w = width // NX
    return pl.pallas_call(
        hidden_kernel,
        name="gather_hidden",
        out_shape=jax.ShapeDtypeStruct((8 * NY, width), F32),
        in_specs=[pl.BlockSpec(memory_space=pltpu.VMEM)] * 2,
        out_specs=pl.BlockSpec(memory_space=pltpu.VMEM),
        scratch_shapes=[
            pltpu.VMEM((NX - 1, 8, w), F32),
            pltpu.VMEM((8, w), F32),
            pltpu.SemaphoreType.DMA((NX - 1,)),
            pltpu.SemaphoreType.DMA((NX - 1,)),
            pltpu.SemaphoreType.DMA((15,)),
            pltpu.SemaphoreType.DMA((15,)),
        ],
        compiler_params=pltpu.CompilerParams(collective_id=1, has_side_effects=True),
    )(part, res)


WIN = 256


def mlp_kernel(hid_ref, g_ref, wg_hbm, wu_hbm, wd_hbm, out_ref, wg, wu, wd, hn, sem):
    _, _, y, _ = coords()
    steps = wg.shape[0]
    ff_tiles = wg_hbm.shape[1] // LANE
    win_tiles = steps * WIN // LANE
    lo = (y * ff_tiles + NY - 1) // NY
    hi = ((y + 1) * ff_tiles + NY - 1) // NY
    first = jnp.minimum(lo, ff_tiles - win_tiles)
    base = first * LANE

    def fetch(i):
        cols = pl.ds(pl.multiple_of(base + i * WIN, LANE), WIN)
        return (
            pltpu.make_async_copy(wg_hbm.at[:, cols], wg.at[i], sem.at[0, i]),
            pltpu.make_async_copy(wu_hbm.at[:, cols], wu.at[i], sem.at[1, i]),
            pltpu.make_async_copy(wd_hbm.at[cols, :], wd.at[i], sem.at[2, i]),
        )

    for i in range(steps):
        for copy in fetch(i):
            copy.start()
    hid = hid_ref[...]
    inv = lax.rsqrt(jnp.mean(hid * hid, axis=-1, keepdims=True) + NORM_EPS)
    hn[...] = (hid * inv * g_ref[...].astype(F32)).astype(BF16)
    out_ref[...] = jnp.zeros_like(out_ref)

    def body(i, carry):
        cg, cu, cd = fetch(i)
        cg.wait()
        gate = jnp.dot(hn[...], wg[i], preferred_element_type=F32).astype(BF16).astype(F32)
        cu.wait()
        up = jnp.dot(hn[...], wu[i], preferred_element_type=F32).astype(BF16).astype(F32)
        act = jax.nn.silu(gate) * up
        col = lax.broadcasted_iota(jnp.int32, act.shape, 1) + (base + i * WIN)
        act = jnp.where((col >= lo * LANE) & (col < hi * LANE), act, 0.0).astype(BF16)
        cd.wait()
        out_ref[...] += jnp.dot(act, wd[i], preferred_element_type=F32)
        return carry

    lax.fori_loop(0, steps, body, 0)


def mlp(hid, g, wg, wu, wd):
    rows, width = hid.shape
    ff_tiles = wg.shape[1] // LANE
    steps = -(-(-(-ff_tiles // NY)) * LANE // WIN)
    return pl.pallas_call(
        mlp_kernel,
        name="mlp",
        out_shape=jax.ShapeDtypeStruct((rows, width), F32),
        in_specs=[pl.BlockSpec(memory_space=pltpu.VMEM)] * 2 + [pl.BlockSpec(memory_space=pl.ANY)] * 3,
        out_specs=pl.BlockSpec(memory_space=pltpu.VMEM),
        scratch_shapes=[
            pltpu.VMEM((steps, width, WIN), BF16),
            pltpu.VMEM((steps, width, WIN), BF16),
            pltpu.VMEM((steps, WIN, width), BF16),
            pltpu.VMEM((rows, width), BF16),
            pltpu.SemaphoreType.DMA((3, steps)),
        ],
        compiler_params=pltpu.CompilerParams(vmem_limit_bytes=48 * 2**20),
        cost_estimate=pl.CostEstimate(flops=6 * rows * width * steps * WIN, bytes_accessed=6 * width * steps * WIN, transcendentals=0),
    )(hid, g.reshape(1, -1), wg, wu, wd)


def output_kernel(part_ref, hid_ref, buf, slots, chunk, rs_send, rs_recv, p1_send, p1_recv, p2_send, p2_recv, cc_send, cc_recv):
    x, z, y, c = coords()
    w = chunk.shape[1]
    cut = [(0, 256), (256, 256), (512, w - 512)]
    plane = [(turn(x, dx, NX), turn(y, dy, NY)) for dx, dy in XY]
    first = [
        [(turn(x, a, NX), z, turn(y, b, NY)) for a, b in XY],
        [(x, turn(z, a, NZ), turn(y, b, NY)) for a, b in XY],
        [(turn(x, a, NX), turn(z, b, NZ), y) for a, b in XY],
    ]
    second = [
        [(x, turn(z, k, NZ), y) for k in range(1, 4)],
        [(turn(x, k, NX), z, y) for k in range(1, 4)],
        [(x, z, turn(y, k, NY)) for k in range(1, 4)],
    ]
    partner = dev(x, z, y, turn(c, 1, NC))
    near = [(turn(x, a, NX), z, turn(y, b, NY)) for a, b in XY]
    near += [(x, turn(z, a, NZ), turn(y, b, NY)) for a in range(1, NZ) for b in range(NY)]
    near += [(turn(x, a, NX), turn(z, b, NZ), y) for a in range(1, NX) for b in range(1, NZ)]
    entry_barrier([dev(*p, c) for p in near] + [partner])
    rs = []
    for k, (px, py) in enumerate(plane):
        rows = pl.ds(pl.multiple_of(py * 8, 8), 8)
        cols = pl.ds(pl.multiple_of(px * w, LANE), w)
        rs.append(remote(part_ref.at[rows, cols], slots.at[k], rs_send.at[k], rs_recv.at[k], dev(px, z, py, c)))
    for copy in rs:
        copy.start()
    my_rows = pl.ds(pl.multiple_of(y * 8, 8), 8)
    my_cols = pl.ds(pl.multiple_of(x * w, LANE), w)
    total = part_ref[my_rows, my_cols]
    for k, copy in enumerate(rs):
        copy.wait_recv()
        total = total + slots[k]
    out = (hid_ref[my_rows, my_cols] + total).astype(BF16).astype(F32)
    chunk[...] = out
    p1 = []
    for part, (lo, n) in enumerate(cut):
        for k, p in enumerate(first[part]):
            src = chunk.at[:, lo:lo + n]
            dst = buf.at[z, c, y, x, :, lo:lo + n]
            p1.append(remote(src, dst, p1_send.at[part, k], p1_recv.at[part, k], dev(*p, c)))
    for copy in p1:
        copy.start()
    buf[z, c, y, x] = out
    p2 = []
    for part, (lo, n) in enumerate(cut):
        for copy in p1[part * 15:(part + 1) * 15]:
            copy.wait_recv()
        block = [
            buf.at[z, c, :, :, :, lo:lo + n],
            buf.at[:, c, :, x, :, lo:lo + n],
            buf.at[:, c, y, :, :, lo:lo + n],
        ][part]
        for k, p in enumerate(second[part]):
            copy = remote(block, block, p2_send.at[part, k], p2_recv.at[part, k], dev(*p, c))
            copy.start()
            p2.append(copy)
    for copy in p2:
        copy.wait_recv()
    across = remote(buf.at[:, c], buf.at[:, c], cc_send, cc_recv, partner)
    across.start()
    across.wait_recv()
    for copy in rs + p1 + p2 + [across]:
        copy.wait_send()


def gather_output(part, hid):
    width = part.shape[1]
    w = width // NX
    sem = pltpu.SemaphoreType.DMA
    return pl.pallas_call(
        output_kernel,
        name="gather_output",
        out_shape=jax.ShapeDtypeStruct((NZ, NC, NY, NX, 8, w), F32),
        in_specs=[pl.BlockSpec(memory_space=pltpu.VMEM)] * 2,
        out_specs=pl.BlockSpec(memory_space=pltpu.VMEM),
        scratch_shapes=[
            pltpu.VMEM((15, 8, w), F32),
            pltpu.VMEM((8, w), F32),
            sem((15,)), sem((15,)), sem((3, 15)), sem((3, 15)), sem((3, 3)), sem((3, 3)), sem, sem,
        ],
        compiler_params=pltpu.CompilerParams(collective_id=2, has_side_effects=True),
    )(part, hid)


GRP = 16
SUB = 2


def attend_kernel(lens_ref, lens_row, x_ref, g_ref, freq_ref, k_ref, v_ref, wq_hbm, wk_hbm, wv_hbm, pack_ref, ko_ref, vo_ref, w, q, knew, vnew, pos, sem):
    step = pl.program_id(0)
    rows = x_ref.shape[0]
    heads = wq_hbm.shape[1] // LANE
    seq = k_ref.shape[1]
    half = LANE // 2
    hd = heads * LANE
    base = lax.axis_index("sp") * seq

    @pl.when(step == 0)
    def project():
        odd = hd % (2 * LANE)
        cuts = [(i, 2 * LANE) for i in range(0, hd - odd, 2 * LANE)]
        copies = [[pltpu.make_async_copy(wq_hbm.at[:, a:a + n], w.at[:, a:a + n], sem.at[i])] for i, (a, n) in enumerate(cuts)]
        n = len(cuts)
        last = [
            pltpu.make_async_copy(wq_hbm.at[:, hd - odd:], w.at[:, hd - odd:hd], sem.at[n]),
            pltpu.make_async_copy(wk_hbm, w.at[:, hd:hd + LANE], sem.at[n + 1]),
        ]
        copies += [last, [pltpu.make_async_copy(wv_hbm, w.at[:, hd + LANE:], sem.at[n + 2])]]
        cuts += [(hd - odd, odd + LANE), (hd + LANE, LANE)]
        for group in copies:
            for copy in group:
                copy.start()
        x32 = x_ref[...].astype(F32)
        inv = lax.rsqrt(jnp.mean(x32 * x32, axis=-1, keepdims=True) + NORM_EPS)
        u = (x32 * inv * g_ref[...].astype(F32)).astype(BF16)
        eye = lax.broadcasted_iota(jnp.int32, (LANE, LANE), 0) == lax.broadcasted_iota(jnp.int32, (LANE, LANE), 1)
        cols = []
        for i in range(rows // LANE):
            line = lens_row[i:i + 1, :].astype(F32)
            col = jnp.sum(jnp.where(eye, line, 0.0), axis=1, keepdims=True)
            pos[i * LANE:(i + 1) * LANE, :] = jnp.broadcast_to(col, (LANE, LANE)).astype(jnp.int32)
            cols.append(col)
        low = lax.broadcasted_iota(jnp.int32, (LANE, LANE), 1) < half
        angles = jnp.where(low, cols[0], cols[1]) * freq_ref[...]
        cos = jnp.cos(angles)
        sin = jnp.sin(angles)
        cos_r = pltpu.roll(cos, half, 1)
        sin_r = pltpu.roll(sin, half, 1)
        cos_t = jnp.concatenate([jnp.where(low, cos, cos_r), jnp.where(low, cos_r, cos)], axis=0)
        sin_t = jnp.concatenate([jnp.where(low, -sin, sin_r), jnp.where(low, -sin_r, sin)], axis=0)
        for group, (a, n) in zip(copies, cuts):
            for copy in group:
                copy.wait()
            out = jnp.dot(u, w[:, a:a + n], preferred_element_type=F32).astype(BF16).astype(F32)
            for j in range(0, n, LANE):
                h = (a + j) // LANE
                part = out[:, j:j + LANE]
                if h <= heads:
                    part = (part * cos_t + pltpu.roll(part, half, 1) * sin_t).astype(BF16)
                if h < heads:
                    q[h] = part
                elif h == heads:
                    knew[...] = part.astype(F32)
                else:
                    vnew[...] = part

    ko_ref[...] = k_ref[...]
    vo_ref[...] = v_ref[...]
    first = step * SUB * GRP
    line = lax.broadcasted_iota(jnp.int32, (seq, LANE), 0)

    def put(b, carry):
        at = lens_ref[first + b] - base

        @pl.when((at >= 0) & (at < seq))
        def _():
            here = line == at
            k_row = knew[pl.ds(first + b, 1), :]
            v_row = vnew[pl.ds(first + b, 1), :]
            ko_ref[b] = jnp.where(here, k_row, ko_ref[b].astype(F32)).astype(BF16)
            vo_ref[b] = jnp.where(here, v_row, vo_ref[b].astype(F32)).astype(BF16)

        return carry

    lax.fori_loop(0, SUB * GRP, put, 0)
    span = GRP * seq
    col = lax.broadcasted_iota(jnp.int32, (GRP, span), 1)
    own = (col // seq) == lax.broadcasted_iota(jnp.int32, (GRP, span), 0)
    where_at = base + col % seq
    lane = lax.broadcasted_iota(jnp.int32, (GRP, LANE), 1)
    for s in range(SUB):
        at = pl.ds(pl.multiple_of(first + s * GRP, GRP), GRP)
        block = slice(s * GRP, (s + 1) * GRP)
        qs = jnp.concatenate([q[h, at, :] for h in range(heads)], axis=0)
        ks = ko_ref[block].reshape(span, LANE)
        vs = vo_ref[block].reshape(span, LANE)
        p = jnp.concatenate([pos[at, :]] * (span // LANE), axis=1)
        valid = own & (where_at <= p)
        valid = jnp.concatenate([valid.astype(F32)] * heads, axis=0) > 0.5
        scores = lax.dot_general(qs, ks, (((1,), (1,)), ((), ())), preferred_element_type=F32) * (LANE ** -0.5)
        scores = jnp.where(valid, scores, -1e30)
        top = jnp.max(scores, axis=1, keepdims=True)
        wt = jnp.where(valid, jnp.exp(scores - top), 0.0)
        tot = jnp.sum(wt, axis=1, keepdims=True)
        mix = jnp.dot(wt.astype(BF16), vs, preferred_element_type=F32)
        stats = jnp.zeros((GRP, LANE), F32)
        for h in range(heads):
            part = slice(h * GRP, (h + 1) * GRP)
            pack_ref[block, h * LANE:(h + 1) * LANE] = mix[part]
            stats = jnp.where(lane == h, top[part], stats)
            stats = jnp.where(lane == half + h, tot[part], stats)
        pack_ref[block, hd:] = stats


def attend(x_tok, seq_lens, k_blk, v_blk, g, wq, wk, wv):
    rows, width = x_tok.shape
    seq = k_blk.shape[1]
    hd = wq.shape[1]
    half = LANE // 2
    freq = jnp.power(F32(ROPE_BASE), jnp.arange(half, dtype=F32) * (-2.0 / LANE))
    freq = jnp.concatenate([freq, freq]).reshape(1, LANE)
    step = SUB * GRP
    whole = lambda shape: pl.BlockSpec(shape, lambda i, *_: (0,) * len(shape))
    cache = pl.BlockSpec((step, seq, LANE), lambda i, *_: (i, 0, 0))
    hbm = pl.BlockSpec(memory_space=pl.ANY)
    k3, v3 = k_blk.reshape(rows, seq, LANE), v_blk.reshape(rows, seq, LANE)
    packed, ko, vo = pl.pallas_call(
        attend_kernel,
        name="attend",
        grid_spec=pltpu.PrefetchScalarGridSpec(
            num_scalar_prefetch=1,
            grid=(rows // step,),
            in_specs=[whole((rows // LANE, LANE)), whole((rows, width)), whole((1, width)), whole((1, LANE)), cache, cache, hbm, hbm, hbm],
            out_specs=[pl.BlockSpec((step, hd + LANE), lambda i, *_: (i, 0)), cache, cache],
            scratch_shapes=[
                pltpu.VMEM((width, hd + 2 * LANE), BF16),
                pltpu.VMEM((hd // LANE, rows, LANE), BF16),
                pltpu.VMEM((rows, LANE), F32),
                pltpu.VMEM((rows, LANE), F32),
                pltpu.VMEM((rows, LANE), jnp.int32),
                pltpu.SemaphoreType.DMA((8,)),
            ],
        ),
        out_shape=[
            jax.ShapeDtypeStruct((rows, hd + LANE), F32),
            jax.ShapeDtypeStruct(k3.shape, BF16),
            jax.ShapeDtypeStruct(v3.shape, BF16),
        ],
        compiler_params=pltpu.CompilerParams(dimension_semantics=("arbitrary",), vmem_limit_bytes=40 * 2**20),
    )(seq_lens, seq_lens.reshape(rows // LANE, LANE), x_tok, g.reshape(1, -1), freq, k3, v3, wq, wk, wv)
    return packed, ko.reshape(k_blk.shape), vo.reshape(v_blk.shape)


def solution(mesh):
    cache_spec = P(None, "sp", "tp", None)
    col_spec = P(None, "tp")
    row_spec = P("tp", None)
    full_spec = P()

    def local_step(x_tok, seq_lens, k_blk, v_blk, g_attn, wq_loc, wk_loc, wv_loc, wo_loc, g_mlp, wg_loc, wu_loc, wd_loc):
        x, z, y, c = coords()
        w = x_tok.shape[1] // NX
        res = lax.dynamic_slice(x_tok, (row_chunk(z, y, c) * 8, x * w), (8, w)).astype(F32)
        packed, k_out, v_out = attend(x_tok, seq_lens, k_blk, v_blk, g_attn, wq_loc, wk_loc, wv_loc)
        attn_out = combine(packed, wq_loc.shape[1] // LANE)
        part = jnp.dot(attn_out, wo_loc, preferred_element_type=F32)
        hid = gather_hidden(part, res)
        mlp_part = mlp(hid, g_mlp, wg_loc, wu_loc, wd_loc)
        buf = gather_output(mlp_part, hid)
        y_out = buf.transpose(0, 1, 2, 4, 3, 5).reshape(x_tok.shape).astype(BF16)
        return y_out, k_out, v_out

    return jax.shard_map(local_step, mesh=mesh, in_specs=(full_spec, full_spec, cache_spec, cache_spec, full_spec, col_spec, col_spec, col_spec, row_spec, full_spec, col_spec, col_spec, row_spec), out_specs=(full_spec, cache_spec, cache_spec), check_vma=False)
```

```python
import functools

import jax
import jax.numpy as jnp
from jax import lax
from jax.experimental import pallas as pl
from jax.experimental.pallas import tpu as pltpu
from jax.sharding import PartitionSpec as P

ROPE_BASE = 500000.0
NORM_EPS = 1e-5
MESH = pl.DeviceIdType.MESH
F32 = jnp.float32
BF16 = jnp.bfloat16
NX, NZ, NY, NC = 4, 4, 4, 2
LANE = 128
VMEM_ALL = 67043328


def coords():
    s = lax.axis_index("sp")
    return lax.axis_index("tp"), s // (NY * NC), (s // NC) % NY, s % NC


def dev(x, z, y, c):
    return (x, (z * NY + y) * NC + c)


def turn(v, d, n):
    return lax.rem(v + d, n)


def entry_barrier(peers):
    barrier = pltpu.get_barrier_semaphore()
    for peer in peers:
        pl.semaphore_signal(barrier, inc=1, device_id=peer, device_id_type=MESH)
    pl.semaphore_wait(barrier, len(peers))


def remote(src, dst, send_sem, recv_sem, peer):
    return pltpu.make_async_remote_copy(
        src_ref=src, dst_ref=dst, send_sem=send_sem, recv_sem=recv_sem, device_id=peer, device_id_type=MESH
    )


XY = [(dx, dy) for dx in range(4) for dy in range(4)][1:]
WIN = 256


def layer_kernel(
    in_ref, res_ref, g_ref, wo_hbm, wg_hbm, wu_hbm, wd_hbm, out_ref,
    swap, merged, slots, part, xslots, chunk, hid, hn, acc, cslot, buf,
    wg, wu, wg_t, wu_t, wd,
    w_sem, swap_sem, rs_send, rs_recv, xs_send, xs_recv, ag_send, ag_recv, fw_send, fw_recv,
    c_sem, xo_send, xo_recv, p1_send, p1_recv, p2_send, p2_recv, cc_send, cc_recv,
):
    x, z, y, c = coords()
    w = chunk.shape[1]
    heads = w // LANE
    half = LANE // 2
    mate = turn(c, 1, NC)
    partner = dev(x, z, y, mate)
    steps = wg.shape[0]
    wide = steps * WIN
    ff = wg_hbm.shape[1]
    window = wide + LANE
    first = pl.multiple_of(c * (ff - window), LANE)
    keep = wd.shape[0] - wo_hbm.shape[0]

    def fetch(i):
        cols = pl.ds(pl.multiple_of(first + i * WIN, LANE), WIN)
        return (
            pltpu.make_async_copy(wg_hbm.at[:, cols], wg.at[i], w_sem.at[0, i]),
            pltpu.make_async_copy(wu_hbm.at[:, cols], wu.at[i], w_sem.at[1, i]),
        )

    def fetch_down(i):
        rows = pl.ds(pl.multiple_of(first + i * WIN, LANE), WIN)
        here = pl.ds(pl.multiple_of(i * WIN, LANE), WIN)
        return pltpu.make_async_copy(wd_hbm.at[rows, :], wd.at[here, :], w_sem.at[2, i])

    tail = pl.ds(pl.multiple_of(first + wide, LANE), LANE)
    tails = (
        pltpu.make_async_copy(wg_hbm.at[:, tail], wg_t, w_sem.at[0, steps]),
        pltpu.make_async_copy(wu_hbm.at[:, tail], wu_t, w_sem.at[1, steps]),
        pltpu.make_async_copy(wd_hbm.at[tail, :], wd.at[wide:, :], w_sem.at[2, steps]),
    )
    get_wo = pltpu.make_async_copy(wo_hbm, wd.at[keep:, :], w_sem.at[3, 0])
    n_keep = keep // WIN

    planes = [
        [(turn(x, a, NX), z, turn(y, b, NY)) for a, b in XY],
        [(x, turn(z, a, NZ), turn(y, b, NY)) for a, b in XY],
        [(turn(x, a, NX), turn(z, b, NZ), y) for a, b in XY],
    ]
    near = planes[0] + [(x, turn(z, a, NZ), turn(y, b, NY)) for a in range(1, NZ) for b in range(NY)]
    near += [(turn(x, a, NX), turn(z, b, NZ), y) for a in range(1, NX) for b in range(1, NZ)]
    entry_barrier([dev(*p, c) for p in near] + [partner])

    give = remote(in_ref.at[:, mate], swap, swap_sem.at[0], swap_sem.at[1], partner)
    give.start()
    get_wo.start()
    give.wait_recv()
    low = lax.broadcasted_iota(jnp.int32, (8, LANE), 1) < half

    def pair(g):
        s1, s2 = in_ref[g, c, :, w:], swap[g, :, w:]
        top = jnp.maximum(s1, s2)
        f1, f2 = jnp.exp(s1 - top), jnp.exp(s2 - top)
        total = pltpu.roll(f1, half, 1) * s1 + pltpu.roll(f2, half, 1) * s2
        mix = []
        for h in range(heads):
            cut = slice(h * LANE, (h + 1) * LANE)
            mix.append(f1[:, h:h + 1] * in_ref[g, c, :, cut] + f2[:, h:h + 1] * swap[g, :, cut])
        return mix, jnp.where(low, top, total)

    rs = []
    for k, (_, pz, py) in enumerate(planes[1]):
        g = pz * NY + py
        mix, stats = pair(g)
        for h in range(heads):
            merged[k, :, h * LANE:(h + 1) * LANE] = mix[h]
        merged[k, :, w:] = stats
        copy = remote(merged.at[k], slots.at[k], rs_send.at[k], rs_recv.at[k], dev(x, pz, py, c))
        copy.start()
        rs.append(copy)
    for i in range(n_keep):
        for copy in fetch(i) + (fetch_down(i),):
            copy.start()
    for i in range(n_keep, steps):
        for copy in fetch(i):
            copy.start()
    for copy in tails[:2]:
        copy.start()
    own_mix, own_stats = pair(z * NY + y)
    for copy in rs:
        copy.wait_recv()
    top = own_stats
    for k in range(len(rs)):
        top = jnp.maximum(top, slots[k, :, w:])

    def add(stats, mix, acc_mix, total):
        factor = jnp.exp(stats - top)
        total = total + pltpu.roll(factor, half, 1) * stats
        return [acc_mix[h] + factor[:, h:h + 1] * mix[h] for h in range(heads)], total

    mixed, total = add(own_stats, own_mix, [jnp.zeros((8, LANE), F32)] * heads, jnp.zeros((8, LANE), F32))
    for k in range(len(rs)):
        mix = [slots[k, :, h * LANE:(h + 1) * LANE] for h in range(heads)]
        mixed, total = add(slots[k, :, w:], mix, mixed, total)
    attn = jnp.concatenate([mixed[h] / total[:, half + h:half + h + 1] for h in range(heads)], axis=1).astype(BF16)

    get_wo.wait()
    for n in range(0, part.shape[1], 4 * LANE):
        part[:, n:n + 4 * LANE] = jnp.dot(attn, wd[keep:, n:n + 4 * LANE], preferred_element_type=F32)
    my_cols = pl.ds(pl.multiple_of(x * w, LANE), w)
    my_rows = pl.ds(pl.multiple_of(c * 8, 8), 8)
    line = [turn(x, k, NX) for k in range(1, NX)]
    cols = [pl.ds(pl.multiple_of(px * w, LANE), w) for px in line]
    xs = []
    for k, px in enumerate(line):
        copy = remote(part.at[:, cols[k]], xslots.at[k], xs_send.at[k], xs_recv.at[k], dev(px, z, y, c))
        copy.start()
        xs.append(copy)
    for i in range(n_keep, steps):
        fetch_down(i).start()
    tails[2].start()
    sums = part[:, my_cols]
    for k, copy in enumerate(xs):
        copy.wait_recv()
        sums = sums + xslots[k]
    hidden = (res_ref[...] + sums).astype(BF16).astype(F32)
    chunk[...] = hidden
    ag = []
    for k, px in enumerate(line):
        copy = remote(chunk, hid.at[my_rows, my_cols], ag_send.at[k], ag_recv.at[k], dev(px, z, y, c))
        copy.start()
        ag.append(copy)
    fw = [remote(chunk, hid.at[my_rows, my_cols], fw_send.at[3], fw_recv.at[3], partner)]
    fw[0].start()
    hid[my_rows, my_cols] = hidden
    for k, copy in enumerate(ag):
        copy.wait_recv()
        block = hid.at[my_rows, cols[2 - k]]
        copy = remote(block, block, fw_send.at[k], fw_recv.at[k], partner)
        copy.start()
        fw.append(copy)
    for copy in fw:
        copy.wait_recv()

    h32 = hid[...]
    inv = lax.rsqrt(jnp.mean(h32 * h32, axis=-1, keepdims=True) + NORM_EPS)
    hn[...] = (h32 * inv * g_ref[...].astype(F32)).astype(BF16)
    acc[...] = jnp.zeros_like(acc)
    mid = (ff // LANE + 1) // 2 * LANE

    def gated(gate, up, start):
        gate = gate.astype(BF16).astype(F32)
        up = up.astype(BF16).astype(F32)
        col = lax.broadcasted_iota(jnp.int32, gate.shape, 1) + start
        lo = c * mid
        act = jax.nn.silu(gate) * up
        return jnp.where((col >= lo) & (col < mid + c * ff), act, 0.0).astype(BF16)

    def mlp_step(i, carry):
        cg, cu = fetch(i)
        cg.wait()
        gate = jnp.dot(hn[...], wg[i], preferred_element_type=F32)
        cu.wait()
        up = jnp.dot(hn[...], wu[i], preferred_element_type=F32)
        act = gated(gate, up, first + i * WIN)
        fetch_down(i).wait()
        here = pl.ds(pl.multiple_of(i * WIN, LANE), WIN)
        acc[...] += jnp.dot(act, wd[here, :], preferred_element_type=F32)
        return carry

    lax.fori_loop(0, steps, mlp_step, 0)
    tails[0].wait()
    gate = jnp.dot(hn[...], wg_t[...], preferred_element_type=F32)
    tails[1].wait()
    up = jnp.dot(hn[...], wu_t[...], preferred_element_type=F32)
    act = gated(gate, up, first + wide)
    tails[2].wait()
    acc[...] += jnp.dot(act, wd[wide:, :], preferred_element_type=F32)

    mate_rows = pl.ds(pl.multiple_of(mate * 8, 8), 8)
    back = remote(acc.at[mate_rows, :], cslot, c_sem.at[0], c_sem.at[1], partner)
    back.start()
    for copy in xs:
        copy.wait_send()
    back.wait_recv()
    part[...] = acc[my_rows, :] + cslot[...]
    xo = []
    for k, px in enumerate(line):
        copy = remote(part.at[:, cols[k]], xslots.at[k + 3], xo_send.at[k], xo_recv.at[k], dev(px, z, y, c))
        copy.start()
        xo.append(copy)
    sums = part[:, my_cols]
    for k, copy in enumerate(xo):
        copy.wait_recv()
        sums = sums + xslots[k + 3]
    out = (hidden + sums).astype(BF16).astype(F32)
    for copy in ag + fw[:1]:
        copy.wait_send()
    chunk[...] = out

    cut = [(0, 2 * LANE), (2 * LANE, 2 * LANE), (4 * LANE, w - 4 * LANE)]
    p1 = []
    for p, (lo, n) in enumerate(cut):
        for k, peer in enumerate(planes[p]):
            src, dst = chunk.at[:, lo:lo + n], buf.at[z, y, c, x, :, lo:lo + n]
            copy = remote(src, dst, p1_send.at[p, k], p1_recv.at[p, k], dev(*peer, c))
            copy.start()
            p1.append(copy)
    buf[z, y, c, x] = out

    def block(p, v, h):
        lo, n = cut[p]
        cols_p = slice(lo, lo + n)
        two = slice(2 * h, 2 * h + 2)
        return [buf.at[v, two, c, :, :, cols_p], buf.at[two, :, c, v, :, cols_p], buf.at[two, v, c, :, :, cols_p]][p]

    here = [z, x, y]
    up1 = [dev(x, turn(z, 1, 4), y, c), dev(turn(x, 1, 4), z, y, c), dev(x, z, turn(y, 1, 4), c)]
    dn1 = [dev(x, turn(z, 3, 4), y, c), dev(turn(x, 3, 4), z, y, c), dev(x, z, turn(y, 3, 4), c)]
    done = []

    def send(p, v, h, to, i):
        copy = remote(block(p, v, h), block(p, v, h), p2_send.at[p, i], p2_recv.at[p, i], to)
        copy.start()
        done.append(copy)
        return copy

    def across(p, v, h, i):
        copy = remote(block(p, v, h), block(p, v, h), cc_send.at[p, i], cc_recv.at[p, i], partner)
        copy.start()
        done.append(copy)
        return copy

    direct, relayed, crossed = [], [], []
    for p in range(3):
        for copy in p1[p * 15:(p + 1) * 15]:
            copy.wait_recv()
        v = here[p]
        direct.append([send(p, v, 0, up1[p], 0), send(p, v, 1, dn1[p], 1), send(p, v, 1, up1[p], 2), send(p, v, 0, dn1[p], 3)])
        crossed += [across(p, v, 0, 0), across(p, v, 1, 1)]
    for p in range(3):
        below, above = turn(here[p], 3, 4), turn(here[p], 1, 4)
        direct[p][0].wait_recv()
        far = [send(p, below, 0, up1[p], 4)]
        direct[p][1].wait_recv()
        far += [send(p, above, 1, dn1[p], 5)]
        relayed.append(far)
        crossed += [across(p, below, 0, 2), across(p, above, 1, 3)]
    for p in range(3):
        below, above = turn(here[p], 3, 4), turn(here[p], 1, 4)
        direct[p][2].wait_recv()
        crossed += [across(p, below, 1, 4)]
        direct[p][3].wait_recv()
        crossed += [across(p, above, 0, 5)]
    for p in range(3):
        far = turn(here[p], 2, 4)
        relayed[p][0].wait_recv()
        crossed += [across(p, far, 0, 6)]
        relayed[p][1].wait_recv()
        crossed += [across(p, far, 1, 7)]
    for copy in crossed:
        copy.wait_recv()
    for a in range(NZ):
        for b in range(NY):
            for e in range(NC):
                r = ((a * NY + b) * NC + e) * 8
                for d in range(NX):
                    out_ref[r:r + 8, d * w:(d + 1) * w] = buf[a, b, e, d].astype(BF16)
    for copy in [give, back] + rs + fw[1:] + xo + p1 + done:
        copy.wait_send()


def layer(packed, res, g, wo, wg, wu, wd, rows):
    packed = packed.reshape(NZ * NY, NC, 8, packed.shape[1])
    width = wo.shape[1]
    w = width // NX
    steps = ((wg.shape[1] // LANE + 1) // 2 * LANE) // WIN
    sem = pltpu.SemaphoreType.DMA
    vmem = pl.BlockSpec(memory_space=pltpu.VMEM)
    hbm = pl.BlockSpec(memory_space=pl.ANY)
    return pl.pallas_call(
        layer_kernel,
        name="layer",
        out_shape=jax.ShapeDtypeStruct((rows, width), BF16),
        in_specs=[vmem] * 3 + [hbm] * 4,
        out_specs=vmem,
        scratch_shapes=[
            pltpu.VMEM((NZ * NY, 8, packed.shape[3]), F32),
            pltpu.VMEM((15, 8, packed.shape[3]), F32),
            pltpu.VMEM((15, 8, packed.shape[3]), F32),
            pltpu.VMEM((8, width), F32),
            pltpu.VMEM((6, 8, w), F32),
            pltpu.VMEM((8, w), F32),
            pltpu.VMEM((8 * NC, width), F32),
            pltpu.VMEM((8 * NC, width), BF16),
            pltpu.VMEM((8 * NC, width), F32),
            pltpu.VMEM((8, width), F32),
            pltpu.VMEM((NZ, NY, NC, NX, 8, w), F32),
            pltpu.VMEM((steps, width, WIN), BF16),
            pltpu.VMEM((steps, width, WIN), BF16),
            pltpu.VMEM((width, LANE), BF16),
            pltpu.VMEM((width, LANE), BF16),
            pltpu.VMEM((steps * WIN + LANE, width), BF16),
            sem((4, steps + 1)),
            sem((2,)), sem((15,)), sem((15,)), sem((3,)), sem((3,)), sem((3,)), sem((3,)), sem((4,)), sem((4,)),
            sem((2,)), sem((3,)), sem((3,)), sem((3, 15)), sem((3, 15)), sem((3, 6)), sem((3, 6)), sem((3, 8)), sem((3, 8)),
        ],
        compiler_params=pltpu.CompilerParams(collective_id=0, has_side_effects=True, vmem_limit_bytes=VMEM_ALL),
    )(packed, res, g.reshape(1, -1), wo, wg, wu, wd)


GRP = 16
SUB = 4


def attend_kernel(lens_ref, lens_row, x_ref, g_ref, freq_ref, k_ref, v_ref, wq_hbm, wk_hbm, wv_hbm, pack_ref, ko_ref, vo_ref, w, q, knew, vnew, pos, sem):
    step = pl.program_id(0)
    rows = x_ref.shape[0]
    heads = wq_hbm.shape[1] // LANE
    seq = k_ref.shape[1]
    half = LANE // 2
    hd = heads * LANE
    base = lax.axis_index("sp") * seq

    @pl.when(step == 0)
    def project():
        odd = hd % (2 * LANE)
        cuts = [(i, 2 * LANE) for i in range(0, hd - odd, 2 * LANE)]
        copies = [[pltpu.make_async_copy(wq_hbm.at[:, a:a + n], w.at[:, a:a + n], sem.at[i])] for i, (a, n) in enumerate(cuts)]
        n = len(cuts)
        last = [
            pltpu.make_async_copy(wq_hbm.at[:, hd - odd:], w.at[:, hd - odd:hd], sem.at[n]),
            pltpu.make_async_copy(wk_hbm, w.at[:, hd:hd + LANE], sem.at[n + 1]),
        ]
        copies += [last, [pltpu.make_async_copy(wv_hbm, w.at[:, hd + LANE:], sem.at[n + 2])]]
        cuts += [(hd - odd, odd + LANE), (hd + LANE, LANE)]
        for group in copies:
            for copy in group:
                copy.start()
        x32 = x_ref[...].astype(F32)
        inv = lax.rsqrt(jnp.mean(x32 * x32, axis=-1, keepdims=True) + NORM_EPS)
        u = (x32 * inv * g_ref[...].astype(F32)).astype(BF16)
        eye = lax.broadcasted_iota(jnp.int32, (LANE, LANE), 0) == lax.broadcasted_iota(jnp.int32, (LANE, LANE), 1)
        cols = []
        for i in range(rows // LANE):
            line = lens_row[i:i + 1, :].astype(F32)
            col = jnp.sum(jnp.where(eye, line, 0.0), axis=1, keepdims=True)
            pos[i * LANE:(i + 1) * LANE, :] = jnp.broadcast_to(col, (LANE, LANE)).astype(jnp.int32)
            cols.append(col)
        low = lax.broadcasted_iota(jnp.int32, (LANE, LANE), 1) < half
        angles = jnp.where(low, cols[0], cols[1]) * freq_ref[...]
        cos = jnp.cos(angles)
        sin = jnp.sin(angles)
        cos_r = pltpu.roll(cos, half, 1)
        sin_r = pltpu.roll(sin, half, 1)
        cos_t = jnp.concatenate([jnp.where(low, cos, cos_r), jnp.where(low, cos_r, cos)], axis=0)
        sin_t = jnp.concatenate([jnp.where(low, -sin, sin_r), jnp.where(low, -sin_r, sin)], axis=0)
        for group, (a, n) in zip(copies, cuts):
            for copy in group:
                copy.wait()
            out = jnp.dot(u, w[:, a:a + n], preferred_element_type=F32).astype(BF16).astype(F32)
            for j in range(0, n, LANE):
                h = (a + j) // LANE
                part = out[:, j:j + LANE]
                if h <= heads:
                    part = (part * cos_t + pltpu.roll(part, half, 1) * sin_t).astype(BF16)
                if h < heads:
                    q[h] = part
                elif h == heads:
                    knew[...] = part.astype(F32)
                else:
                    vnew[...] = part

    first = step * SUB * GRP
    line = lax.broadcasted_iota(jnp.int32, (seq, LANE), 0)
    for b in range(SUB * GRP):
        here = line == lens_ref[first + b] - base
        k_row = knew[pl.ds(first + b, 1), :]
        v_row = vnew[pl.ds(first + b, 1), :]
        ko_ref[b] = jnp.where(here, k_row, k_ref[b].astype(F32)).astype(BF16)
        vo_ref[b] = jnp.where(here, v_row, v_ref[b].astype(F32)).astype(BF16)
    span = GRP * seq
    col = lax.broadcasted_iota(jnp.int32, (GRP, span), 1)
    own = (col // seq) == lax.broadcasted_iota(jnp.int32, (GRP, span), 0)
    where_at = base + col % seq
    lane = lax.broadcasted_iota(jnp.int32, (GRP, LANE), 1)
    for s in range(SUB):
        at = pl.ds(pl.multiple_of(first + s * GRP, GRP), GRP)
        block = slice(s * GRP, (s + 1) * GRP)
        qs = jnp.concatenate([q[h, at, :] for h in range(heads)], axis=0)
        ks = ko_ref[block].reshape(span, LANE)
        vs = vo_ref[block].reshape(span, LANE)
        p = jnp.concatenate([pos[at, :]] * (span // LANE), axis=1)
        valid = own & (where_at <= p)
        valid = jnp.concatenate([valid.astype(F32)] * heads, axis=0) > 0.5
        scores = lax.dot_general(qs, ks, (((1,), (1,)), ((), ())), preferred_element_type=F32) * (LANE ** -0.5)
        scores = jnp.where(valid, scores, -1e30)
        top = jnp.max(scores, axis=1, keepdims=True)
        wt = jnp.where(valid, jnp.exp(scores - top), 0.0)
        tot = jnp.sum(wt, axis=1, keepdims=True)
        mix = jnp.dot(wt.astype(BF16), vs, preferred_element_type=F32)
        stats = jnp.zeros((GRP, LANE), F32)
        for h in range(heads):
            part = slice(h * GRP, (h + 1) * GRP)
            pack_ref[block, h * LANE:(h + 1) * LANE] = mix[part]
            stats = jnp.where(lane == h, top[part], stats)
            stats = jnp.where(lane == half + h, tot[part], stats)
        pack_ref[block, hd:] = stats


def attend(x_tok, seq_lens, k_blk, v_blk, g, wq, wk, wv):
    rows, width = x_tok.shape
    seq = k_blk.shape[1]
    hd = wq.shape[1]
    half = LANE // 2
    freq = jnp.power(F32(ROPE_BASE), jnp.arange(half, dtype=F32) * (-2.0 / LANE))
    freq = jnp.concatenate([freq, freq]).reshape(1, LANE)
    step = SUB * GRP
    whole = lambda shape: pl.BlockSpec(shape, lambda i, *_: (0,) * len(shape))
    cache = pl.BlockSpec((step, seq, LANE), lambda i, *_: (i, 0, 0))
    hbm = pl.BlockSpec(memory_space=pl.ANY)
    k3, v3 = k_blk.reshape(rows, seq, LANE), v_blk.reshape(rows, seq, LANE)
    packed, ko, vo = pl.pallas_call(
        attend_kernel,
        name="attend",
        grid_spec=pltpu.PrefetchScalarGridSpec(
            num_scalar_prefetch=1,
            grid=(rows // step,),
            in_specs=[whole((rows // LANE, LANE)), whole((rows, width)), whole((1, width)), whole((1, LANE)), cache, cache, hbm, hbm, hbm],
            out_specs=[pl.BlockSpec((step, hd + LANE), lambda i, *_: (i, 0)), cache, cache],
            scratch_shapes=[
                pltpu.VMEM((width, hd + 2 * LANE), BF16),
                pltpu.VMEM((hd // LANE, rows, LANE), BF16),
                pltpu.VMEM((rows, LANE), F32),
                pltpu.VMEM((rows, LANE), F32),
                pltpu.VMEM((rows, LANE), jnp.int32),
                pltpu.SemaphoreType.DMA((8,)),
            ],
        ),
        out_shape=[
            jax.ShapeDtypeStruct((rows, hd + LANE), F32),
            jax.ShapeDtypeStruct(k3.shape, BF16),
            jax.ShapeDtypeStruct(v3.shape, BF16),
        ],
        compiler_params=pltpu.CompilerParams(dimension_semantics=("arbitrary",), vmem_limit_bytes=VMEM_ALL),
    )(seq_lens, seq_lens.reshape(rows // LANE, LANE), x_tok, g.reshape(1, -1), freq, k3, v3, wq, wk, wv)
    return packed, ko.reshape(k_blk.shape), vo.reshape(v_blk.shape)


def solution(mesh):
    cache_spec = P(None, "sp", "tp", None)
    col_spec = P(None, "tp")
    row_spec = P("tp", None)
    full_spec = P()

    def local_step(x_tok, seq_lens, k_blk, v_blk, g_attn, wq_loc, wk_loc, wv_loc, wo_loc, g_mlp, wg_loc, wu_loc, wd_loc):
        w = x_tok.shape[1] // NX
        res = lax.dynamic_slice(x_tok, (lax.axis_index("sp") * 8, lax.axis_index("tp") * w), (8, w)).astype(F32)
        packed, k_out, v_out = attend(x_tok, seq_lens, k_blk, v_blk, g_attn, wq_loc, wk_loc, wv_loc)
        y_out = layer(packed, res, g_mlp, wo_loc, wg_loc, wu_loc, wd_loc, x_tok.shape[0])
        return y_out, k_out, v_out

    return jax.shard_map(local_step, mesh=mesh, in_specs=(full_spec, full_spec, cache_spec, cache_spec, full_spec, col_spec, col_spec, col_spec, row_spec, full_spec, col_spec, col_spec, row_spec), out_specs=(full_spec, cache_spec, cache_spec), check_vma=False)
```

```python
import jax
import jax.numpy as jnp
import numpy as np
from jax import lax
from jax.experimental import pallas as pl
from jax.experimental.pallas import tpu as pltpu
from jax.sharding import PartitionSpec as P

ROPE_BASE = 500000.0
NORM_EPS = 1e-5
MESH = pl.DeviceIdType.MESH
F32 = jnp.float32
BF16 = jnp.bfloat16
NX, NZ, NY, NC = 4, 4, 4, 2
LANE = 128
VMEM_ALL = 67043328


def coords():
    s = lax.axis_index("sp")
    return lax.axis_index("tp"), s // (NY * NC), (s // NC) % NY, s % NC


def dev(x, z, y, c):
    return (x, (z * NY + y) * NC + c)


def turn(v, d, n):
    return lax.rem(v + d, n)


def entry_barrier(peers):
    barrier = pltpu.get_barrier_semaphore()
    for peer in peers:
        pl.semaphore_signal(barrier, inc=1, device_id=peer, device_id_type=MESH)
    pl.semaphore_wait(barrier, len(peers))


def remote(src, dst, send_sem, recv_sem, peer):
    return pltpu.make_async_remote_copy(
        src_ref=src, dst_ref=dst, send_sem=send_sem, recv_sem=recv_sem, device_id=peer, device_id_type=MESH
    )


XY = [(dx, dy) for dx in range(4) for dy in range(4)][1:]
WIN = 256


def layer_kernel(
    q_ref, pos_ref, g_ref, x_hbm, k_hbm, v_hbm, wo_hbm, wg_hbm, wu_hbm, wd_hbm, out_ref,
    kv, res, pack, swap, merged, slots, part, xslots, chunk, hid, hn, acc, cslot, buf,
    wg, wu, wd,
    w_sem, in_sem, gv_send, gv_recv, rs_send, rs_recv, xs_send, xs_recv, ag_send, ag_recv, fw_send, fw_recv,
    c_sem, xo_send, xo_recv, p1_send, p1_recv, p2_send, p2_recv, cc_send, cc_recv,
):
    x, z, y, c = coords()
    w = chunk.shape[1]
    heads = w // LANE
    half = LANE // 2
    mate = turn(c, 1, NC)
    partner = dev(x, z, y, mate)
    steps = wg.shape[0]
    wide = steps * WIN
    ff = wg_hbm.shape[1]
    window = wide + LANE
    first = pl.multiple_of(c * (ff - window), LANE)
    keep = wd.shape[0] - wo_hbm.shape[0]

    def fetch(i):
        cols = pl.ds(pl.multiple_of(first + i * WIN, LANE), WIN)
        return (
            pltpu.make_async_copy(wg_hbm.at[:, cols], wg.at[i], w_sem.at[0, i]),
            pltpu.make_async_copy(wu_hbm.at[:, cols], wu.at[i], w_sem.at[1, i]),
        )

    def fetch_down(i):
        rows = pl.ds(pl.multiple_of(first + i * WIN, LANE), WIN)
        here = pl.ds(pl.multiple_of(i * WIN, LANE), WIN)
        return pltpu.make_async_copy(wd_hbm.at[rows, :], wd.at[here, :], w_sem.at[2, i])

    wg_t, wu_t = kv.at[0, :wg.shape[1], :], kv.at[1, :wu.shape[1], :]
    tail = pl.ds(pl.multiple_of(first + wide, LANE), LANE)
    tails = (
        pltpu.make_async_copy(wg_hbm.at[:, tail], wg_t, w_sem.at[0, steps]),
        pltpu.make_async_copy(wu_hbm.at[:, tail], wu_t, w_sem.at[1, steps]),
        pltpu.make_async_copy(wd_hbm.at[tail, :], wd.at[wide:, :], w_sem.at[2, steps]),
    )
    get_wo = pltpu.make_async_copy(wo_hbm, wd.at[keep:, :], w_sem.at[3, 0])
    n_keep = keep // WIN

    at_me = lax.axis_index("sp")
    get_in = [
        pltpu.make_async_copy(k_hbm, kv.at[0], in_sem.at[0]),
        pltpu.make_async_copy(v_hbm, kv.at[1], in_sem.at[1]),
        pltpu.make_async_copy(x_hbm.at[pl.ds(pl.multiple_of(at_me * 8, 8), 8), pl.ds(pl.multiple_of(x * w, LANE), w)], res, in_sem.at[2]),
        get_wo,
    ]
    for copy in get_in:
        copy.start()
    planes = [
        [(turn(x, a, NX), z, turn(y, b, NY)) for a, b in XY],
        [(x, turn(z, a, NZ), turn(y, b, NY)) for a, b in XY],
        [(turn(x, a, NX), turn(z, b, NZ), y) for a, b in XY],
    ]
    near = planes[0] + [(x, turn(z, a, NZ), turn(y, b, NY)) for a in range(1, NZ) for b in range(NY)]
    near += [(turn(x, a, NX), turn(z, b, NZ), y) for a in range(1, NX) for b in range(1, NZ)]
    entry_barrier([dev(*p, c) for p in near] + [partner])

    n_grp = NZ * NY
    seq = kv.shape[1] // q_ref.shape[1]
    span = GRP * seq
    low = lax.broadcasted_iota(jnp.int32, (8, LANE), 1) < half

    def place(k):
        return turn(z, ((k + 1) // NY) % NZ, NZ), turn(y, (k + 1) % NY, NY)

    def give(k):
        return remote(pack.at[k, mate], swap.at[k], gv_send.at[k], gv_recv.at[k], partner)

    def deliver(k):
        pz, py = place(k)
        return remote(merged.at[k], slots.at[k], rs_send.at[k], rs_recv.at[k], dev(x, pz, py, c))

    def attend(k):
        pz, py = place(k)
        g = pz * NY + py
        at = pl.ds(pl.multiple_of(g * GRP, GRP), GRP)
        keys = pl.ds(pl.multiple_of(g * span, span), span)
        qs = jnp.concatenate([q_ref[h, at, :] for h in range(heads)], axis=0)
        col = lax.broadcasted_iota(jnp.int32, (GRP, span), 1)
        own = (col // seq) == lax.broadcasted_iota(jnp.int32, (GRP, span), 0)
        p = jnp.concatenate([pos_ref[at, :]] * (span // LANE), axis=1)
        valid = own & (at_me * seq + col % seq <= p)
        valid = jnp.concatenate([valid.astype(F32)] * heads, axis=0) > 0.5
        scores = lax.dot_general(qs, kv[0, keys, :], (((1,), (1,)), ((), ())), preferred_element_type=F32) * (LANE ** -0.5)
        scores = jnp.where(valid, scores, -1e30)
        top = jnp.max(scores, axis=1, keepdims=True)
        wt = jnp.where(valid, jnp.exp(scores - top), 0.0)
        tot = jnp.sum(wt, axis=1, keepdims=True)
        mix = jnp.dot(wt.astype(BF16), kv[1, keys, :], preferred_element_type=F32)
        lane = lax.broadcasted_iota(jnp.int32, (8, LANE), 1)
        for e in range(NC):
            stats = jnp.zeros((8, LANE), F32)
            for h in range(heads):
                rows = slice(h * GRP + e * 8, h * GRP + e * 8 + 8)
                pack[k, e, :, h * LANE:(h + 1) * LANE] = mix[rows]
                stats = jnp.where(lane == h, top[rows], stats)
                stats = jnp.where(lane == half + h, tot[rows], stats)
            pack[k, e, :, w:] = stats
        give(k).start()

    def pair(k):
        give(k).wait_recv()
        s1, s2 = pack[k, c, :, w:], swap[k, :, w:]
        top = jnp.maximum(s1, s2)
        f1, f2 = jnp.exp(s1 - top), jnp.exp(s2 - top)
        total = pltpu.roll(f1, half, 1) * s1 + pltpu.roll(f2, half, 1) * s2
        mix = []
        for h in range(heads):
            cut = slice(h * LANE, (h + 1) * LANE)
            mix.append(f1[:, h:h + 1] * pack[k, c, :, cut] + f2[:, h:h + 1] * swap[k, :, cut])
        return mix, jnp.where(low, top, total)

    def pass_on(k):
        mix, stats = pair(k)
        for h in range(heads):
            merged[k, :, h * LANE:(h + 1) * LANE] = mix[h]
        merged[k, :, w:] = stats
        deliver(k).start()

    lag = 4
    for copy in get_in[:2]:
        copy.wait()

    def begin(k, carry):
        attend(k)
        return carry

    def both(k, carry):
        attend(k)
        pass_on(k - lag)
        return carry

    def finish(k, carry):
        pass_on(k)
        return carry

    lax.fori_loop(0, lag, begin, 0)
    lax.fori_loop(lag, n_grp, both, 0)
    lax.fori_loop(n_grp - lag, n_grp - 1, finish, 0)
    rs = [deliver(k) for k in range(n_grp - 1)]
    gives = [give(k) for k in range(n_grp)]
    for i in range(n_keep):
        for copy in fetch(i) + (fetch_down(i),):
            copy.start()
    for i in range(n_keep, steps):
        for copy in fetch(i):
            copy.start()
    for copy in tails[:2]:
        copy.start()
    own_mix, own_stats = pair(n_grp - 1)
    for copy in rs:
        copy.wait_recv()
    top = own_stats
    for k in range(len(rs)):
        top = jnp.maximum(top, slots[k, :, w:])

    def add(stats, mix, acc_mix, total):
        factor = jnp.exp(stats - top)
        total = total + pltpu.roll(factor, half, 1) * stats
        return [acc_mix[h] + factor[:, h:h + 1] * mix[h] for h in range(heads)], total

    mixed, total = add(own_stats, own_mix, [jnp.zeros((8, LANE), F32)] * heads, jnp.zeros((8, LANE), F32))
    for k in range(len(rs)):
        mix = [slots[k, :, h * LANE:(h + 1) * LANE] for h in range(heads)]
        mixed, total = add(slots[k, :, w:], mix, mixed, total)
    attn = jnp.concatenate([mixed[h] / total[:, half + h:half + h + 1] for h in range(heads)], axis=1).astype(BF16)

    get_wo.wait()
    for n in range(0, part.shape[1], 4 * LANE):
        part[:, n:n + 4 * LANE] = jnp.dot(attn, wd[keep:, n:n + 4 * LANE], preferred_element_type=F32)
    my_cols = pl.ds(pl.multiple_of(x * w, LANE), w)
    my_rows = pl.ds(pl.multiple_of(c * 8, 8), 8)
    line = [turn(x, k, NX) for k in range(1, NX)]
    cols = [pl.ds(pl.multiple_of(px * w, LANE), w) for px in line]
    xs = []
    for k, px in enumerate(line):
        copy = remote(part.at[:, cols[k]], xslots.at[k], xs_send.at[k], xs_recv.at[k], dev(px, z, y, c))
        copy.start()
        xs.append(copy)
    for i in range(n_keep, steps):
        fetch_down(i).start()
    tails[2].start()
    sums = part[:, my_cols]
    for k, copy in enumerate(xs):
        copy.wait_recv()
        sums = sums + xslots[k]
    get_in[2].wait()
    hidden = (res[...].astype(F32) + sums).astype(BF16).astype(F32)
    chunk[...] = hidden
    ag = []
    for k, px in enumerate(line):
        copy = remote(chunk, hid.at[my_rows, my_cols], ag_send.at[k], ag_recv.at[k], dev(px, z, y, c))
        copy.start()
        ag.append(copy)
    fw = [remote(chunk, hid.at[my_rows, my_cols], fw_send.at[3], fw_recv.at[3], partner)]
    fw[0].start()
    hid[my_rows, my_cols] = hidden
    for k, copy in enumerate(ag):
        copy.wait_recv()
        block = hid.at[my_rows, cols[2 - k]]
        copy = remote(block, block, fw_send.at[k], fw_recv.at[k], partner)
        copy.start()
        fw.append(copy)
    for copy in fw:
        copy.wait_recv()

    h32 = hid[...]
    inv = lax.rsqrt(jnp.mean(h32 * h32, axis=-1, keepdims=True) + NORM_EPS)
    hn[...] = (h32 * inv * g_ref[...].astype(F32)).astype(BF16)
    acc[...] = jnp.zeros_like(acc)
    mid = (ff // LANE + 1) // 2 * LANE

    def gated(gate, up, start):
        gate = gate.astype(BF16).astype(F32)
        up = up.astype(BF16).astype(F32)
        col = lax.broadcasted_iota(jnp.int32, gate.shape, 1) + start
        lo = c * mid
        act = jax.nn.silu(gate) * up
        return jnp.where((col >= lo) & (col < mid + c * ff), act, 0.0).astype(BF16)

    def mlp_step(i, carry):
        cg, cu = fetch(i)
        cg.wait()
        gate = jnp.dot(hn[...], wg[i], preferred_element_type=F32)
        cu.wait()
        up = jnp.dot(hn[...], wu[i], preferred_element_type=F32)
        act = gated(gate, up, first + i * WIN)
        fetch_down(i).wait()
        here = pl.ds(pl.multiple_of(i * WIN, LANE), WIN)
        acc[...] += jnp.dot(act, wd[here, :], preferred_element_type=F32)
        return carry

    lax.fori_loop(0, steps, mlp_step, 0)
    tails[0].wait()
    gate = jnp.dot(hn[...], wg_t[...], preferred_element_type=F32)
    tails[1].wait()
    up = jnp.dot(hn[...], wu_t[...], preferred_element_type=F32)
    act = gated(gate, up, first + wide)
    tails[2].wait()
    acc[...] += jnp.dot(act, wd[wide:, :], preferred_element_type=F32)

    mate_rows = pl.ds(pl.multiple_of(mate * 8, 8), 8)
    back = remote(acc.at[mate_rows, :], cslot, c_sem.at[0], c_sem.at[1], partner)
    back.start()
    for copy in xs:
        copy.wait_send()
    back.wait_recv()
    part[...] = acc[my_rows, :] + cslot[...]
    xo = []
    for k, px in enumerate(line):
        copy = remote(part.at[:, cols[k]], xslots.at[k + 3], xo_send.at[k], xo_recv.at[k], dev(px, z, y, c))
        copy.start()
        xo.append(copy)
    sums = part[:, my_cols]
    for k, copy in enumerate(xo):
        copy.wait_recv()
        sums = sums + xslots[k + 3]
    out = (hidden + sums).astype(BF16).astype(F32)
    for copy in ag + fw[:1]:
        copy.wait_send()
    chunk[...] = out

    cut = [(0, 2 * LANE), (2 * LANE, 2 * LANE), (4 * LANE, w - 4 * LANE)]
    p1 = []
    for p, (lo, n) in enumerate(cut):
        for k, peer in enumerate(planes[p]):
            src, dst = chunk.at[:, lo:lo + n], buf.at[z, y, c, x, :, lo:lo + n]
            copy = remote(src, dst, p1_send.at[p, k], p1_recv.at[p, k], dev(*peer, c))
            copy.start()
            p1.append(copy)
    buf[z, y, c, x] = out

    def block(p, v, h):
        lo, n = cut[p]
        cols_p = slice(lo, lo + n)
        two = slice(2 * h, 2 * h + 2)
        return [buf.at[v, two, c, :, :, cols_p], buf.at[two, :, c, v, :, cols_p], buf.at[two, v, c, :, :, cols_p]][p]

    here = [z, x, y]
    up1 = [dev(x, turn(z, 1, 4), y, c), dev(turn(x, 1, 4), z, y, c), dev(x, z, turn(y, 1, 4), c)]
    dn1 = [dev(x, turn(z, 3, 4), y, c), dev(turn(x, 3, 4), z, y, c), dev(x, z, turn(y, 3, 4), c)]
    done = []

    def send(p, v, h, to, i):
        copy = remote(block(p, v, h), block(p, v, h), p2_send.at[p, i], p2_recv.at[p, i], to)
        copy.start()
        done.append(copy)
        return copy

    def across(p, v, h, i):
        copy = remote(block(p, v, h), block(p, v, h), cc_send.at[p, i], cc_recv.at[p, i], partner)
        copy.start()
        done.append(copy)
        return copy

    direct, relayed, crossed = [], [], []
    for p in range(3):
        for copy in p1[p * 15:(p + 1) * 15]:
            copy.wait_recv()
        v = here[p]
        direct.append([send(p, v, 0, up1[p], 0), send(p, v, 1, dn1[p], 1), send(p, v, 1, up1[p], 2), send(p, v, 0, dn1[p], 3)])
        crossed += [across(p, v, 0, 0), across(p, v, 1, 1)]
    for p in range(3):
        below, above = turn(here[p], 3, 4), turn(here[p], 1, 4)
        direct[p][0].wait_recv()
        far = [send(p, below, 0, up1[p], 4)]
        direct[p][1].wait_recv()
        far += [send(p, above, 1, dn1[p], 5)]
        relayed.append(far)
        crossed += [across(p, below, 0, 2), across(p, above, 1, 3)]
    for p in range(3):
        below, above = turn(here[p], 3, 4), turn(here[p], 1, 4)
        direct[p][2].wait_recv()
        crossed += [across(p, below, 1, 4)]
        direct[p][3].wait_recv()
        crossed += [across(p, above, 0, 5)]
    for p in range(3):
        far = turn(here[p], 2, 4)
        relayed[p][0].wait_recv()
        crossed += [across(p, far, 0, 6)]
        relayed[p][1].wait_recv()
        crossed += [across(p, far, 1, 7)]
    for copy in crossed:
        copy.wait_recv()
    for a in range(NZ):
        for b in range(NY):
            for e in range(NC):
                r = ((a * NY + b) * NC + e) * 8
                for d in range(NX):
                    out_ref[r:r + 8, d * w:(d + 1) * w] = buf[a, b, e, d].astype(BF16)
    for copy in gives + [back] + rs + fw[1:] + xo + p1 + done:
        copy.wait_send()


def layer(q, pos, x_tok, ko, vo, g, wo, wg, wu, wd):
    rows, width = x_tok.shape
    w = width // NX
    keys = rows * ko.shape[1]
    steps = ((wg.shape[1] // LANE + 1) // 2 * LANE) // WIN
    sem = pltpu.SemaphoreType.DMA
    vmem = pl.BlockSpec(memory_space=pltpu.VMEM)
    hbm = pl.BlockSpec(memory_space=pl.ANY)
    return pl.pallas_call(
        layer_kernel,
        name="layer",
        out_shape=jax.ShapeDtypeStruct((rows, width), BF16),
        in_specs=[vmem] * 3 + [hbm] * 7,
        out_specs=vmem,
        scratch_shapes=[
            pltpu.VMEM((2, keys, LANE), BF16),
            pltpu.VMEM((8, w), BF16),
            pltpu.VMEM((NZ * NY, NC, 8, w + LANE), F32),
            pltpu.VMEM((NZ * NY, 8, w + LANE), F32),
            pltpu.VMEM((15, 8, w + LANE), F32),
            pltpu.VMEM((15, 8, w + LANE), F32),
            pltpu.VMEM((8, width), F32),
            pltpu.VMEM((6, 8, w), F32),
            pltpu.VMEM((8, w), F32),
            pltpu.VMEM((8 * NC, width), F32),
            pltpu.VMEM((8 * NC, width), BF16),
            pltpu.VMEM((8 * NC, width), F32),
            pltpu.VMEM((8, width), F32),
            pltpu.VMEM((NZ, NY, NC, NX, 8, w), F32),
            pltpu.VMEM((steps, width, WIN), BF16),
            pltpu.VMEM((steps, width, WIN), BF16),
            pltpu.VMEM((steps * WIN + LANE, width), BF16),
            sem((4, steps + 1)),
            sem((3,)), sem((16,)), sem((16,)), sem((15,)), sem((15,)), sem((3,)), sem((3,)), sem((3,)), sem((3,)), sem((4,)), sem((4,)),
            sem((2,)), sem((3,)), sem((3,)), sem((3, 15)), sem((3, 15)), sem((3, 6)), sem((3, 6)), sem((3, 8)), sem((3, 8)),
        ],
        compiler_params=pltpu.CompilerParams(collective_id=0, has_side_effects=True, vmem_limit_bytes=VMEM_ALL),
    )(q, pos, g, x_tok, ko.reshape(keys, LANE), vo.reshape(keys, LANE), wo, wg, wu, wd)


GRP = 16


def project_kernel(lens_ref, lens_row, g_ref, freq_ref, x_hbm, k_hbm, v_hbm, wq_hbm, wk_hbm, wv_hbm, q_ref, pos_ref, ko_hbm, vo_hbm, xs, u, w, kv, knew, vnew, sem, out_sem):
    rows, width = xs.shape
    heads = q_ref.shape[0]
    hd = heads * LANE
    seq = kv.shape[2]
    half = LANE // 2
    base = lax.axis_index("sp") * seq
    n_x, n_out = 2, 4
    part = rows // n_x
    get_x = [pltpu.make_async_copy(x_hbm.at[i * part:(i + 1) * part], xs.at[i * part:(i + 1) * part], sem.at[i]) for i in range(n_x)]
    get_kv = [
        pltpu.make_async_copy(wk_hbm, w.at[:, hd:hd + LANE], sem.at[2]),
        pltpu.make_async_copy(wv_hbm, w.at[:, hd + LANE:], sem.at[3]),
    ]
    get_cache = [pltpu.make_async_copy(k_hbm, kv.at[0], sem.at[4]), pltpu.make_async_copy(v_hbm, kv.at[1], sem.at[5])]
    cuts = [(i, min(2 * LANE, hd - i)) for i in range(0, hd, 2 * LANE)]
    get_q = [pltpu.make_async_copy(wq_hbm.at[:, i:i + n], w.at[:, i:i + n], sem.at[6 + j]) for j, (i, n) in enumerate(cuts)]
    for copy in get_x + get_kv + get_cache + get_q:
        copy.start()

    eye = lax.broadcasted_iota(jnp.int32, (LANE, LANE), 0) == lax.broadcasted_iota(jnp.int32, (LANE, LANE), 1)
    cols = []
    for i in range(rows // LANE):
        line = lens_row[i:i + 1, :].astype(F32)
        col = jnp.sum(jnp.where(eye, line, 0.0), axis=1, keepdims=True)
        pos_ref[i * LANE:(i + 1) * LANE, :] = jnp.broadcast_to(col, (LANE, LANE)).astype(jnp.int32)
        cols.append(col)
    low = lax.broadcasted_iota(jnp.int32, (LANE, LANE), 1) < half
    angles = jnp.where(low, cols[0], cols[1]) * freq_ref[...]
    cos = jnp.cos(angles)
    sin = jnp.sin(angles)
    cos_r = pltpu.roll(cos, half, 1)
    sin_r = pltpu.roll(sin, half, 1)
    cos_t = jnp.concatenate([jnp.where(low, cos, cos_r), jnp.where(low, cos_r, cos)], axis=0)
    sin_t = jnp.concatenate([jnp.where(low, -sin, sin_r), jnp.where(low, -sin_r, sin)], axis=0)

    def norm(i, carry):
        at = pl.ds(pl.multiple_of(i * GRP, GRP), GRP)
        x32 = xs[at, :].astype(F32)
        inv = lax.rsqrt(jnp.mean(x32 * x32, axis=-1, keepdims=True) + NORM_EPS)
        u[at, :] = (x32 * inv * g_ref[...].astype(F32)).astype(BF16)
        return carry

    for i in range(n_x):
        get_x[i].wait()
        lax.fori_loop(i * part // GRP, (i + 1) * part // GRP, norm, 0)

    def rope(t):
        return (t * cos_t + pltpu.roll(t, half, 1) * sin_t).astype(BF16)

    for copy in get_kv:
        copy.wait()
    out = jnp.dot(u[...], w[:, hd:], preferred_element_type=F32).astype(BF16).astype(F32)
    knew[...] = rope(out[:, :LANE]).astype(F32)
    vnew[...] = out[:, LANE:]
    for copy in get_cache:
        copy.wait()
    line = lax.broadcasted_iota(jnp.int32, (seq, LANE), 0)

    def put(i, carry):
        for j in range(GRP):
            b = i * GRP + j
            here = line == lens_ref[b] - base
            kv[0, b] = jnp.where(here, knew[pl.ds(b, 1), :], kv[0, b].astype(F32)).astype(BF16)
            kv[1, b] = jnp.where(here, vnew[pl.ds(b, 1), :], kv[1, b].astype(F32)).astype(BF16)
        return carry

    puts = []
    part = rows // n_out
    for i in range(n_out):
        lax.fori_loop(i * part // GRP, (i + 1) * part // GRP, put, 0)
        at = slice(i * part, (i + 1) * part)
        for j, ref in enumerate((ko_hbm, vo_hbm)):
            copy = pltpu.make_async_copy(kv.at[j, at], ref.at[at], out_sem.at[j, i])
            copy.start()
            puts.append(copy)
    for copy, (a, n) in zip(get_q, cuts):
        copy.wait()
        out = jnp.dot(u[...], w[:, a:a + n], preferred_element_type=F32).astype(BF16).astype(F32)
        for j in range(0, n, LANE):
            q_ref[(a + j) // LANE] = rope(out[:, j:j + LANE])
    for copy in puts:
        copy.wait()


def project(x_tok, seq_lens, k_blk, v_blk, g, wq, wk, wv):
    rows, width = x_tok.shape
    seq = k_blk.shape[1]
    hd = wq.shape[1]
    half = LANE // 2
    freq = np.float32(ROPE_BASE) ** (np.arange(half, dtype=np.float32) * np.float32(-2.0 / LANE))
    freq = jnp.asarray(np.concatenate([freq, freq]).reshape(1, LANE).astype(np.float32))
    vmem = pl.BlockSpec(memory_space=pltpu.VMEM)
    hbm = pl.BlockSpec(memory_space=pl.ANY)
    sem = pltpu.SemaphoreType.DMA
    cache = jax.ShapeDtypeStruct((rows, seq, LANE), BF16)
    return pl.pallas_call(
        project_kernel,
        name="project",
        out_shape=[
            jax.ShapeDtypeStruct((hd // LANE, rows, LANE), BF16),
            jax.ShapeDtypeStruct((rows, LANE), jnp.int32),
            cache,
            cache,
        ],
        in_specs=[pl.BlockSpec(memory_space=pltpu.SMEM), vmem, vmem, vmem] + [hbm] * 6,
        out_specs=[vmem, vmem, hbm, hbm],
        scratch_shapes=[
            pltpu.VMEM((rows, width), BF16),
            pltpu.VMEM((rows, width), BF16),
            pltpu.VMEM((width, hd + 2 * LANE), BF16),
            pltpu.VMEM((2, rows, seq, LANE), BF16),
            pltpu.VMEM((rows, LANE), F32),
            pltpu.VMEM((rows, LANE), F32),
            sem((10,)),
            sem((2, 4)),
        ],
        compiler_params=pltpu.CompilerParams(vmem_limit_bytes=VMEM_ALL),
    )(seq_lens, seq_lens.reshape(rows // LANE, LANE), g, freq, x_tok, k_blk.reshape(cache.shape), v_blk.reshape(cache.shape), wq, wk, wv)


def solution(mesh):
    cache_spec = P(None, "sp", "tp", None)
    col_spec = P(None, "tp")
    row_spec = P("tp", None)
    full_spec = P()

    def local_step(x_tok, seq_lens, k_blk, v_blk, g_attn, wq_loc, wk_loc, wv_loc, wo_loc, g_mlp, wg_loc, wu_loc, wd_loc):
        q, pos, ko, vo = project(x_tok, seq_lens, k_blk, v_blk, g_attn, wq_loc, wk_loc, wv_loc)
        y_out = layer(q, pos, x_tok, ko, vo, g_mlp, wo_loc, wg_loc, wu_loc, wd_loc)
        return y_out, ko.reshape(k_blk.shape), vo.reshape(v_blk.shape)

    return jax.shard_map(local_step, mesh=mesh, in_specs=(full_spec, full_spec, cache_spec, cache_spec, full_spec, col_spec, col_spec, col_spec, row_spec, full_spec, col_spec, col_spec, row_spec), out_specs=(full_spec, cache_spec, cache_spec), check_vma=False)
```

```python
import jax
import jax.numpy as jnp
import numpy as np
from jax import lax
from jax.experimental import pallas as pl
from jax.experimental.pallas import tpu as pltpu
from jax.sharding import PartitionSpec as P

ROPE_BASE = 500000.0
NORM_EPS = 1e-5
MESH = pl.DeviceIdType.MESH
F32 = jnp.float32
BF16 = jnp.bfloat16
NX, NZ, NY, NC = 4, 4, 4, 2
LANE = 128
VMEM_ALL = 67043328


def coords():
    s = lax.axis_index("sp")
    return lax.axis_index("tp"), s // (NY * NC), (s // NC) % NY, s % NC


def dev(x, z, y, c):
    return (x, (z * NY + y) * NC + c)


def turn(v, d, n):
    return lax.rem(v + d, n)


def entry_barrier(peers):
    barrier = pltpu.get_barrier_semaphore()
    for peer in peers:
        pl.semaphore_signal(barrier, inc=1, device_id=peer, device_id_type=MESH)
    pl.semaphore_wait(barrier, len(peers))


def remote(src, dst, send_sem, recv_sem, peer):
    return pltpu.make_async_remote_copy(
        src_ref=src, dst_ref=dst, send_sem=send_sem, recv_sem=recv_sem, device_id=peer, device_id_type=MESH
    )


XY = [(dx, dy) for dx in range(4) for dy in range(4)][1:]
WIN = 256


def layer_kernel(
    q_hbm, pos_hbm, g_hbm, x_hbm, k_hbm, v_hbm, wo_hbm, wg_hbm, wu_hbm, wd_hbm, out_hbm,
    q_ref, pos_ref, g_ref, kv, res, pack, swap, merged, slots, part, xslots, chunk, hid, hn, acc, cslot, buf,
    wg, wu, wd,
    w_sem, out_sem, in_sem, gv_send, gv_recv, rs_send, rs_recv, xs_send, xs_recv, ag_send, ag_recv, fw_send, fw_recv,
    c_sem, xo_send, xo_recv, p1_send, p1_recv, p2_send, p2_recv, cc_send, cc_recv,
):
    x, z, y, c = coords()
    w = chunk.shape[1]
    heads = w // LANE
    half = LANE // 2
    mate = turn(c, 1, NC)
    partner = dev(x, z, y, mate)
    steps = wg.shape[0]
    wide = steps * WIN
    ff = wg_hbm.shape[1]
    window = wide + LANE
    first = pl.multiple_of(c * (ff - window), LANE)
    keep = wd.shape[0] - wo_hbm.shape[0]

    def fetch(i):
        cols = pl.ds(pl.multiple_of(first + i * WIN, LANE), WIN)
        return (
            pltpu.make_async_copy(wg_hbm.at[:, cols], wg.at[i], w_sem.at[0, i]),
            pltpu.make_async_copy(wu_hbm.at[:, cols], wu.at[i], w_sem.at[1, i]),
        )

    def fetch_down(i):
        rows = pl.ds(pl.multiple_of(first + i * WIN, LANE), WIN)
        here = pl.ds(pl.multiple_of(i * WIN, LANE), WIN)
        return pltpu.make_async_copy(wd_hbm.at[rows, :], wd.at[here, :], w_sem.at[2, i])

    wg_t, wu_t = kv.at[0, :wg.shape[1], :], kv.at[1, :wu.shape[1], :]
    tail = pl.ds(pl.multiple_of(first + wide, LANE), LANE)
    tails = (
        pltpu.make_async_copy(wg_hbm.at[:, tail], wg_t, w_sem.at[0, steps]),
        pltpu.make_async_copy(wu_hbm.at[:, tail], wu_t, w_sem.at[1, steps]),
        pltpu.make_async_copy(wd_hbm.at[tail, :], wd.at[wide:, :], w_sem.at[2, steps]),
    )
    get_wo = pltpu.make_async_copy(wo_hbm, wd.at[keep:, :], w_sem.at[3, 0])
    n_keep = keep // WIN

    at_me = lax.axis_index("sp")
    get_in = [
        pltpu.make_async_copy(k_hbm, kv.at[0], in_sem.at[0]),
        pltpu.make_async_copy(v_hbm, kv.at[1], in_sem.at[1]),
        pltpu.make_async_copy(x_hbm.at[pl.ds(pl.multiple_of(at_me * 8, 8), 8), pl.ds(pl.multiple_of(x * w, LANE), w)], res, in_sem.at[2]),
        pltpu.make_async_copy(q_hbm, q_ref, in_sem.at[3]),
        pltpu.make_async_copy(pos_hbm, pos_ref, in_sem.at[4]),
        pltpu.make_async_copy(g_hbm, g_ref, in_sem.at[5]),
    ]
    for copy in (get_in[3], get_in[4], get_in[0], get_in[1], get_in[2], get_in[5]):
        copy.start()
    fetch(0)[0].start()
    planes = [
        [(turn(x, a, NX), z, turn(y, b, NY)) for a, b in XY],
        [(x, turn(z, a, NZ), turn(y, b, NY)) for a, b in XY],
        [(turn(x, a, NX), turn(z, b, NZ), y) for a, b in XY],
    ]
    near = planes[0] + [(x, turn(z, a, NZ), turn(y, b, NY)) for a in range(1, NZ) for b in range(NY)]
    near += [(turn(x, a, NX), turn(z, b, NZ), y) for a in range(1, NX) for b in range(1, NZ)]
    entry_barrier([dev(*p, c) for p in near] + [partner])

    n_grp = NZ * NY
    seq = kv.shape[1] // q_ref.shape[1]
    span = GRP * seq
    low = lax.broadcasted_iota(jnp.int32, (8, LANE), 1) < half

    def place(k):
        return turn(z, ((k + 1) // NY) % NZ, NZ), turn(y, (k + 1) % NY, NY)

    def give(k):
        return remote(pack.at[k, mate], swap.at[k], gv_send.at[k], gv_recv.at[k], partner)

    def deliver(k):
        pz, py = place(k)
        return remote(merged.at[k], slots.at[k], rs_send.at[k], rs_recv.at[k], dev(x, pz, py, c))

    def attend(k):
        pz, py = place(k)
        g = pz * NY + py
        at = pl.ds(pl.multiple_of(g * GRP, GRP), GRP)
        keys = pl.ds(pl.multiple_of(g * span, span), span)
        qs = jnp.concatenate([q_ref[h, at, :] for h in range(heads)], axis=0)
        col = lax.broadcasted_iota(jnp.int32, (GRP, span), 1)
        own = (col // seq) == lax.broadcasted_iota(jnp.int32, (GRP, span), 0)
        p = jnp.concatenate([pos_ref[at, :]] * (span // LANE), axis=1)
        valid = own & (at_me * seq + col % seq <= p)
        valid = jnp.concatenate([valid.astype(F32)] * heads, axis=0) > 0.5
        scores = lax.dot_general(qs, kv[0, keys, :], (((1,), (1,)), ((), ())), preferred_element_type=F32) * (LANE ** -0.5)
        scores = jnp.where(valid, scores, -1e30)
        top = jnp.max(scores, axis=1, keepdims=True)
        wt = jnp.where(valid, jnp.exp(scores - top), 0.0)
        tot = jnp.sum(wt, axis=1, keepdims=True)
        mix = jnp.dot(wt.astype(BF16), kv[1, keys, :], preferred_element_type=F32)
        lane = lax.broadcasted_iota(jnp.int32, (8, LANE), 1)
        for e in range(NC):
            stats = jnp.zeros((8, LANE), F32)
            for h in range(heads):
                rows = slice(h * GRP + e * 8, h * GRP + e * 8 + 8)
                pack[k, e, :, h * LANE:(h + 1) * LANE] = mix[rows]
                stats = jnp.where(lane == h, top[rows], stats)
                stats = jnp.where(lane == half + h, tot[rows], stats)
            pack[k, e, :, w:] = stats
        give(k).start()

    def pair(k):
        give(k).wait_recv()
        s1, s2 = pack[k, c, :, w:], swap[k, :, w:]
        top = jnp.maximum(s1, s2)
        f1, f2 = jnp.exp(s1 - top), jnp.exp(s2 - top)
        total = pltpu.roll(f1, half, 1) * s1 + pltpu.roll(f2, half, 1) * s2
        mix = []
        for h in range(heads):
            cut = slice(h * LANE, (h + 1) * LANE)
            mix.append(f1[:, h:h + 1] * pack[k, c, :, cut] + f2[:, h:h + 1] * swap[k, :, cut])
        return mix, jnp.where(low, top, total)

    def pass_on(k):
        mix, stats = pair(k)
        for h in range(heads):
            merged[k, :, h * LANE:(h + 1) * LANE] = mix[h]
        merged[k, :, w:] = stats
        deliver(k).start()

    lag = 4
    for i in (0, 1, 3, 4):
        get_in[i].wait()

    def begin(k, carry):
        attend(k)
        return carry

    def both(k, carry):
        for j in (2 * k, 2 * k + 1):
            attend(j)
            pass_on(j - lag)
        fetch(k - lag // 2 + 1)[0].start()
        return carry

    def finish(k, carry):
        pass_on(k)
        return carry

    lax.fori_loop(0, lag, begin, 0)
    lax.fori_loop(lag // 2, n_grp // 2, both, 0)
    lax.fori_loop(n_grp - lag, n_grp - 1, finish, 0)
    rs = [deliver(k) for k in range(n_grp - 1)]
    gives = [give(k) for k in range(n_grp)]
    early = 1 + (n_grp - lag) // 2
    get_wo.start()
    for i in range(steps):
        fetch(i)[1].start()
    for i in range(early, steps):
        fetch(i)[0].start()
    fetch_down(0).start()
    own_mix, own_stats = pair(n_grp - 1)
    for copy in rs:
        copy.wait_recv()
    top = own_stats
    for k in range(len(rs)):
        top = jnp.maximum(top, slots[k, :, w:])

    def add(stats, mix, acc_mix, total):
        factor = jnp.exp(stats - top)
        total = total + pltpu.roll(factor, half, 1) * stats
        return [acc_mix[h] + factor[:, h:h + 1] * mix[h] for h in range(heads)], total

    mixed, total = add(own_stats, own_mix, [jnp.zeros((8, LANE), F32)] * heads, jnp.zeros((8, LANE), F32))
    for k in range(len(rs)):
        mix = [slots[k, :, h * LANE:(h + 1) * LANE] for h in range(heads)]
        mixed, total = add(slots[k, :, w:], mix, mixed, total)
    attn = jnp.concatenate([mixed[h] / total[:, half + h:half + h + 1] for h in range(heads)], axis=1).astype(BF16)

    get_wo.wait()
    for n in range(0, part.shape[1], 4 * LANE):
        part[:, n:n + 4 * LANE] = jnp.dot(attn, wd[keep:, n:n + 4 * LANE], preferred_element_type=F32)
    my_cols = pl.ds(pl.multiple_of(x * w, LANE), w)
    my_rows = pl.ds(pl.multiple_of(c * 8, 8), 8)
    line = [turn(x, k, NX) for k in range(1, NX)]
    cols = [pl.ds(pl.multiple_of(px * w, LANE), w) for px in line]
    xs = []
    for k, px in enumerate(line):
        copy = remote(part.at[:, cols[k]], xslots.at[k], xs_send.at[k], xs_recv.at[k], dev(px, z, y, c))
        copy.start()
        xs.append(copy)
    for i in range(1, 5):
        fetch_down(i).start()
    sums = part[:, my_cols]
    for k, copy in enumerate(xs):
        copy.wait_recv()
        sums = sums + xslots[k]
    get_in[2].wait()
    hidden = (res[...].astype(F32) + sums).astype(BF16).astype(F32)
    chunk[...] = hidden
    ag = []
    for k, px in enumerate(line):
        copy = remote(chunk, hid.at[my_rows, my_cols], ag_send.at[k], ag_recv.at[k], dev(px, z, y, c))
        copy.start()
        ag.append(copy)
    fw = [remote(chunk, hid.at[my_rows, my_cols], fw_send.at[3], fw_recv.at[3], partner)]
    fw[0].start()
    hid[my_rows, my_cols] = hidden
    for i in range(5, steps):
        fetch_down(i).start()
    for copy in tails:
        copy.start()
    for k, copy in enumerate(ag):
        copy.wait_recv()
        block = hid.at[my_rows, cols[2 - k]]
        copy = remote(block, block, fw_send.at[k], fw_recv.at[k], partner)
        copy.start()
        fw.append(copy)
    for copy in fw:
        copy.wait_recv()

    get_in[5].wait()

    h32 = hid[...]
    inv = lax.rsqrt(jnp.mean(h32 * h32, axis=-1, keepdims=True) + NORM_EPS)
    hn[...] = (h32 * inv * g_ref[...].astype(F32)).astype(BF16)
    acc[...] = jnp.zeros_like(acc)
    mid = (ff // LANE + 1) // 2 * LANE

    def gated(gate, up, start):
        gate = gate.astype(BF16).astype(F32)
        up = up.astype(BF16).astype(F32)
        col = lax.broadcasted_iota(jnp.int32, gate.shape, 1) + start
        lo = c * mid
        act = jax.nn.silu(gate) * up
        return jnp.where((col >= lo) & (col < mid + c * ff), act, 0.0).astype(BF16)

    def mlp_step(i, carry):
        cg, cu = fetch(i)
        cg.wait()
        gate = jnp.dot(hn[...], wg[i], preferred_element_type=F32)
        cu.wait()
        up = jnp.dot(hn[...], wu[i], preferred_element_type=F32)
        act = gated(gate, up, first + i * WIN)
        fetch_down(i).wait()
        here = pl.ds(pl.multiple_of(i * WIN, LANE), WIN)
        acc[...] += jnp.dot(act, wd[here, :], preferred_element_type=F32)
        return carry

    lax.fori_loop(0, steps, mlp_step, 0)
    tails[0].wait()
    gate = jnp.dot(hn[...], wg_t[...], preferred_element_type=F32)
    tails[1].wait()
    up = jnp.dot(hn[...], wu_t[...], preferred_element_type=F32)
    act = gated(gate, up, first + wide)
    tails[2].wait()
    acc[...] += jnp.dot(act, wd[wide:, :], preferred_element_type=F32)

    mate_rows = pl.ds(pl.multiple_of(mate * 8, 8), 8)
    back = remote(acc.at[mate_rows, :], cslot, c_sem.at[0], c_sem.at[1], partner)
    back.start()
    for copy in xs:
        copy.wait_send()
    back.wait_recv()
    part[...] = acc[my_rows, :] + cslot[...]
    xo = []
    for k, px in enumerate(line):
        copy = remote(part.at[:, cols[k]], xslots.at[k + 3], xo_send.at[k], xo_recv.at[k], dev(px, z, y, c))
        copy.start()
        xo.append(copy)
    sums = part[:, my_cols]
    for k, copy in enumerate(xo):
        copy.wait_recv()
        sums = sums + xslots[k + 3]
    out = (hidden + sums).astype(BF16).astype(F32)
    for copy in ag + fw[:1]:
        copy.wait_send()
    chunk[...] = out

    cut = [(0, 2 * LANE), (2 * LANE, 2 * LANE), (4 * LANE, w - 4 * LANE)]
    p1 = []
    for p, (lo, n) in enumerate(cut):
        for k, peer in enumerate(planes[p]):
            src, dst = chunk.at[:, lo:lo + n], buf.at[z, y, c, x, :, lo:lo + n]
            copy = remote(src, dst, p1_send.at[p, k], p1_recv.at[p, k], dev(*peer, c))
            copy.start()
            p1.append(copy)
    buf[z, y, c, x] = out

    def block(p, v, h):
        lo, n = cut[p]
        cols_p = slice(lo, lo + n)
        two = slice(2 * h, 2 * h + 2)
        return [buf.at[v, two, c, :, :, cols_p], buf.at[two, :, c, v, :, cols_p], buf.at[two, v, c, :, :, cols_p]][p]

    here = [z, x, y]
    up1 = [dev(x, turn(z, 1, 4), y, c), dev(turn(x, 1, 4), z, y, c), dev(x, z, turn(y, 1, 4), c)]
    dn1 = [dev(x, turn(z, 3, 4), y, c), dev(turn(x, 3, 4), z, y, c), dev(x, z, turn(y, 3, 4), c)]
    done = []

    def send(p, v, h, to, i):
        copy = remote(block(p, v, h), block(p, v, h), p2_send.at[p, i], p2_recv.at[p, i], to)
        copy.start()
        done.append(copy)
        return copy

    def across(p, v, h, i):
        copy = remote(block(p, v, h), block(p, v, h), cc_send.at[p, i], cc_recv.at[p, i], partner)
        copy.start()
        done.append(copy)
        return copy

    direct, relayed, crossed = [], [], []
    for p in range(3):
        for copy in p1[p * 15:(p + 1) * 15]:
            copy.wait_recv()
        v = here[p]
        direct.append([send(p, v, 0, up1[p], 0), send(p, v, 1, dn1[p], 1), send(p, v, 1, up1[p], 2), send(p, v, 0, dn1[p], 3)])
        crossed += [across(p, v, 0, 0), across(p, v, 1, 1)]
    for p in range(3):
        below, above = turn(here[p], 3, 4), turn(here[p], 1, 4)
        direct[p][0].wait_recv()
        far = [send(p, below, 0, up1[p], 4)]
        direct[p][1].wait_recv()
        far += [send(p, above, 1, dn1[p], 5)]
        relayed.append(far)
        crossed += [across(p, below, 0, 2), across(p, above, 1, 3)]
    for p in range(3):
        below, above = turn(here[p], 3, 4), turn(here[p], 1, 4)
        direct[p][2].wait_recv()
        crossed += [across(p, below, 1, 4)]
        direct[p][3].wait_recv()
        crossed += [across(p, above, 0, 5)]
    for p in range(3):
        far = turn(here[p], 2, 4)
        relayed[p][0].wait_recv()
        crossed += [across(p, far, 0, 6)]
        relayed[p][1].wait_recv()
        crossed += [across(p, far, 1, 7)]
    for copy in crossed:
        copy.wait_recv()
    puts = []
    for a in range(NZ):
        for b in range(NY):
            for e in range(NC):
                r = ((a * NY + b) * NC + e) * 8
                for d in range(NX):
                    wd[r:r + 8, d * w:(d + 1) * w] = buf[a, b, e, d].astype(BF16)
        at = slice(a * NY * NC * 8, (a + 1) * NY * NC * 8)
        put = pltpu.make_async_copy(wd.at[at, :], out_hbm.at[at, :], out_sem.at[a])
        put.start()
        puts.append(put)
    for copy in gives + [back] + rs + fw[1:] + xo + p1 + done:
        copy.wait_send()
    for put in puts:
        put.wait()


def layer(q, pos, x_tok, ko, vo, g, wo, wg, wu, wd):
    rows, width = x_tok.shape
    w = width // NX
    keys = rows * ko.shape[1]
    steps = ((wg.shape[1] // LANE + 1) // 2 * LANE) // WIN
    sem = pltpu.SemaphoreType.DMA
    hbm = pl.BlockSpec(memory_space=pl.ANY)
    return pl.pallas_call(
        layer_kernel,
        name="layer",
        out_shape=jax.ShapeDtypeStruct((rows, width), BF16),
        in_specs=[hbm] * 10,
        out_specs=hbm,
        scratch_shapes=[
            pltpu.VMEM(q.shape, BF16),
            pltpu.VMEM(pos.shape, jnp.int32),
            pltpu.VMEM(g.shape, BF16),
            pltpu.VMEM((2, keys, LANE), BF16),
            pltpu.VMEM((8, w), BF16),
            pltpu.VMEM((NZ * NY, NC, 8, w + LANE), F32),
            pltpu.VMEM((NZ * NY, 8, w + LANE), F32),
            pltpu.VMEM((15, 8, w + LANE), F32),
            pltpu.VMEM((15, 8, w + LANE), F32),
            pltpu.VMEM((8, width), F32),
            pltpu.VMEM((6, 8, w), F32),
            pltpu.VMEM((8, w), F32),
            pltpu.VMEM((8 * NC, width), F32),
            pltpu.VMEM((8 * NC, width), BF16),
            pltpu.VMEM((8 * NC, width), F32),
            pltpu.VMEM((8, width), F32),
            pltpu.VMEM((NZ, NY, NC, NX, 8, w), F32),
            pltpu.VMEM((steps, width, WIN), BF16),
            pltpu.VMEM((steps, width, WIN), BF16),
            pltpu.VMEM((steps * WIN + LANE, width), BF16),
            sem((4, steps + 1)),
            sem((NZ,)),
            sem((6,)), sem((16,)), sem((16,)), sem((15,)), sem((15,)), sem((3,)), sem((3,)), sem((3,)), sem((3,)), sem((4,)), sem((4,)),
            sem((2,)), sem((3,)), sem((3,)), sem((3, 15)), sem((3, 15)), sem((3, 6)), sem((3, 6)), sem((3, 8)), sem((3, 8)),
        ],
        compiler_params=pltpu.CompilerParams(collective_id=0, has_side_effects=True, vmem_limit_bytes=VMEM_ALL),
    )(q, pos, g, x_tok, ko.reshape(keys, LANE), vo.reshape(keys, LANE), wo, wg, wu, wd)


GRP = 16


def project_kernel(
    lens_hbm, line_hbm, g_hbm, freq_hbm, x_hbm, k_hbm, v_hbm, wq_hbm, wk_hbm, wv_hbm, q_hbm, pos_hbm, ko_hbm, vo_hbm,
    lens_ref, lens_row, g_ref, freq_ref, q_ref, pos_ref, xs, u, w, kv, knew, vnew, sem, small_sem, out_sem, q_sem,
):
    rows, width = xs.shape
    heads = q_ref.shape[0]
    hd = heads * LANE
    seq = kv.shape[2]
    half = LANE // 2
    base = lax.axis_index("sp") * seq
    n_x, n_out = 2, 4
    part = rows // n_x
    get_x = [pltpu.make_async_copy(x_hbm.at[i * part:(i + 1) * part], xs.at[i * part:(i + 1) * part], sem.at[i]) for i in range(n_x)]
    get_kv = [
        pltpu.make_async_copy(wk_hbm, w.at[:, hd:hd + LANE], sem.at[2]),
        pltpu.make_async_copy(wv_hbm, w.at[:, hd + LANE:], sem.at[3]),
    ]
    get_cache = [pltpu.make_async_copy(k_hbm, kv.at[0], sem.at[4]), pltpu.make_async_copy(v_hbm, kv.at[1], sem.at[5])]
    cuts = [(i, min(2 * LANE, hd - i)) for i in range(0, hd, 2 * LANE)]
    get_q = [pltpu.make_async_copy(wq_hbm.at[:, i:i + n], w.at[:, i:i + n], sem.at[6 + j]) for j, (i, n) in enumerate(cuts)]
    get_small = [
        pltpu.make_async_copy(line_hbm, lens_row, small_sem.at[0]),
        pltpu.make_async_copy(freq_hbm, freq_ref, small_sem.at[1]),
        pltpu.make_async_copy(g_hbm, g_ref, small_sem.at[2]),
        pltpu.make_async_copy(lens_hbm, lens_ref, small_sem.at[3]),
    ]
    for copy in get_small + get_x + get_kv + get_cache + get_q:
        copy.start()
    for copy in get_small[:3]:
        copy.wait()

    eye = lax.broadcasted_iota(jnp.int32, (LANE, LANE), 0) == lax.broadcasted_iota(jnp.int32, (LANE, LANE), 1)
    cols = []
    for i in range(rows // LANE):
        line = lens_row[i:i + 1, :].astype(F32)
        col = jnp.sum(jnp.where(eye, line, 0.0), axis=1, keepdims=True)
        pos_ref[i * LANE:(i + 1) * LANE, :] = jnp.broadcast_to(col, (LANE, LANE)).astype(jnp.int32)
        cols.append(col)
    puts = [pltpu.make_async_copy(pos_ref, pos_hbm, q_sem.at[len(cuts)])]
    puts[0].start()
    low = lax.broadcasted_iota(jnp.int32, (LANE, LANE), 1) < half
    angles = jnp.where(low, cols[0], cols[1]) * freq_ref[...]
    cos = jnp.cos(angles)
    sin = jnp.sin(angles)
    cos_r = pltpu.roll(cos, half, 1)
    sin_r = pltpu.roll(sin, half, 1)
    cos_t = jnp.concatenate([jnp.where(low, cos, cos_r), jnp.where(low, cos_r, cos)], axis=0)
    sin_t = jnp.concatenate([jnp.where(low, -sin, sin_r), jnp.where(low, -sin_r, sin)], axis=0)

    def norm(i, carry):
        at = pl.ds(pl.multiple_of(i * GRP, GRP), GRP)
        x32 = xs[at, :].astype(F32)
        inv = lax.rsqrt(jnp.mean(x32 * x32, axis=-1, keepdims=True) + NORM_EPS)
        u[at, :] = (x32 * inv * g_ref[...].astype(F32)).astype(BF16)
        return carry

    for i in range(n_x):
        get_x[i].wait()
        lax.fori_loop(i * part // GRP, (i + 1) * part // GRP, norm, 0)

    def rope(t):
        return (t * cos_t + pltpu.roll(t, half, 1) * sin_t).astype(BF16)

    for copy in get_kv:
        copy.wait()
    out = jnp.dot(u[...], w[:, hd:], preferred_element_type=F32).astype(BF16).astype(F32)
    knew[...] = rope(out[:, :LANE]).astype(F32)
    vnew[...] = out[:, LANE:]
    for copy in get_cache + get_small[3:]:
        copy.wait()
    line = lax.broadcasted_iota(jnp.int32, (seq, LANE), 0)

    def put(i, carry):
        for j in range(GRP):
            b = i * GRP + j
            here = line == lens_ref[b] - base
            kv[0, b] = jnp.where(here, knew[pl.ds(b, 1), :], kv[0, b].astype(F32)).astype(BF16)
            kv[1, b] = jnp.where(here, vnew[pl.ds(b, 1), :], kv[1, b].astype(F32)).astype(BF16)
        return carry

    part = rows // n_out
    for i in range(n_out):
        lax.fori_loop(i * part // GRP, (i + 1) * part // GRP, put, 0)
        at = slice(i * part, (i + 1) * part)
        for j, ref in enumerate((ko_hbm, vo_hbm)):
            copy = pltpu.make_async_copy(kv.at[j, at], ref.at[at], out_sem.at[j, i])
            copy.start()
            puts.append(copy)
    for i, (copy, (a, n)) in enumerate(zip(get_q, cuts)):
        copy.wait()
        out = jnp.dot(u[...], w[:, a:a + n], preferred_element_type=F32).astype(BF16).astype(F32)
        for j in range(0, n, LANE):
            q_ref[(a + j) // LANE] = rope(out[:, j:j + LANE])
        at = slice(a // LANE, (a + n) // LANE)
        copy = pltpu.make_async_copy(q_ref.at[at], q_hbm.at[at], q_sem.at[i])
        copy.start()
        puts.append(copy)
    for copy in puts:
        copy.wait()


def project(x_tok, seq_lens, k_blk, v_blk, g, wq, wk, wv):
    rows, width = x_tok.shape
    seq = k_blk.shape[1]
    hd = wq.shape[1]
    half = LANE // 2
    freq = np.float32(ROPE_BASE) ** (np.arange(half, dtype=np.float32) * np.float32(-2.0 / LANE))
    freq = jnp.asarray(np.concatenate([freq, freq]).reshape(1, LANE).astype(np.float32))
    hbm = pl.BlockSpec(memory_space=pl.ANY)
    sem = pltpu.SemaphoreType.DMA
    cache = jax.ShapeDtypeStruct((rows, seq, LANE), BF16)
    return pl.pallas_call(
        project_kernel,
        name="project",
        out_shape=[
            jax.ShapeDtypeStruct((hd // LANE, rows, LANE), BF16),
            jax.ShapeDtypeStruct((rows, LANE), jnp.int32),
            cache,
            cache,
        ],
        in_specs=[hbm] * 10,
        out_specs=[hbm] * 4,
        scratch_shapes=[
            pltpu.SMEM(seq_lens.shape, jnp.int32),
            pltpu.VMEM((rows // LANE, LANE), jnp.int32),
            pltpu.VMEM(g.shape, BF16),
            pltpu.VMEM((1, LANE), F32),
            pltpu.VMEM((hd // LANE, rows, LANE), BF16),
            pltpu.VMEM((rows, LANE), jnp.int32),
            pltpu.VMEM((rows, width), BF16),
            pltpu.VMEM((rows, width), BF16),
            pltpu.VMEM((width, hd + 2 * LANE), BF16),
            pltpu.VMEM((2, rows, seq, LANE), BF16),
            pltpu.VMEM((rows, LANE), F32),
            pltpu.VMEM((rows, LANE), F32),
            sem((10,)),
            sem((4,)),
            sem((2, 4)),
            sem((6,)),
        ],
        compiler_params=pltpu.CompilerParams(vmem_limit_bytes=VMEM_ALL),
    )(seq_lens, seq_lens.reshape(rows // LANE, LANE), g, freq, x_tok, k_blk.reshape(cache.shape), v_blk.reshape(cache.shape), wq, wk, wv)


def solution(mesh):
    cache_spec = P(None, "sp", "tp", None)
    col_spec = P(None, "tp")
    row_spec = P("tp", None)
    full_spec = P()

    def local_step(x_tok, seq_lens, k_blk, v_blk, g_attn, wq_loc, wk_loc, wv_loc, wo_loc, g_mlp, wg_loc, wu_loc, wd_loc):
        q, pos, ko, vo = project(x_tok, seq_lens, k_blk, v_blk, g_attn, wq_loc, wk_loc, wv_loc)
        y_out = layer(q, pos, x_tok, ko, vo, g_mlp, wo_loc, wg_loc, wu_loc, wd_loc)
        return y_out, ko.reshape(k_blk.shape), vo.reshape(v_blk.shape)

    return jax.shard_map(local_step, mesh=mesh, in_specs=(full_spec, full_spec, cache_spec, cache_spec, full_spec, col_spec, col_spec, col_spec, row_spec, full_spec, col_spec, col_spec, row_spec), out_specs=(full_spec, cache_spec, cache_spec), check_vma=False)
```

```python
import jax
import jax.numpy as jnp
import numpy as np
from jax import lax
from jax.experimental import pallas as pl
from jax.experimental.pallas import tpu as pltpu
from jax.sharding import PartitionSpec as P

ROPE_BASE = 500000.0
NORM_EPS = 1e-5
MESH = pl.DeviceIdType.MESH
F32 = jnp.float32
BF16 = jnp.bfloat16
NX, NZ, NY, NC = 4, 4, 4, 2
LANE = 128
VMEM_ALL = 67043328


def coords():
    s = lax.axis_index("sp")
    return lax.axis_index("tp"), s // (NY * NC), (s // NC) % NY, s % NC


def dev(x, z, y, c):
    return (x, (z * NY + y) * NC + c)


def turn(v, d, n):
    return lax.rem(v + d, n)


def entry_barrier(peers):
    barrier = pltpu.get_barrier_semaphore()
    for peer in peers:
        pl.semaphore_signal(barrier, inc=1, device_id=peer, device_id_type=MESH)
    pl.semaphore_wait(barrier, len(peers))


def remote(src, dst, send_sem, recv_sem, peer):
    return pltpu.make_async_remote_copy(
        src_ref=src, dst_ref=dst, send_sem=send_sem, recv_sem=recv_sem, device_id=peer, device_id_type=MESH
    )


XY = [(dx, dy) for dx in range(4) for dy in range(4)][1:]
WIN = 256


def layer_kernel(
    q_hbm, pos_hbm, g_hbm, x_hbm, k_hbm, v_hbm, wo_hbm, wg_hbm, wu_hbm, wd_hbm, out_hbm,
    q_ref, pos_ref, g_ref, kv, res, pack, swap, merged, slots, part, xslots, chunk, hid, hn, acc, cslot, buf,
    wg, wu, wd,
    w_sem, out_sem, in_sem, gv_send, gv_recv, rs_send, rs_recv, xs_send, xs_recv, ag_send, ag_recv, fw_send, fw_recv,
    c_sem, xo_send, xo_recv, p1_send, p1_recv, p2_send, p2_recv, cc_send, cc_recv,
):
    x, z, y, c = coords()
    w = chunk.shape[1]
    heads = w // LANE
    half = LANE // 2
    mate = turn(c, 1, NC)
    partner = dev(x, z, y, mate)
    steps = wg.shape[0]
    wide = steps * WIN
    ff = wg_hbm.shape[1]
    window = wide + LANE
    first = pl.multiple_of(c * (ff - window), LANE)
    keep = wd.shape[0] - wo_hbm.shape[0]

    def fetch(i):
        cols = pl.ds(pl.multiple_of(first + i * WIN, LANE), WIN)
        return (
            pltpu.make_async_copy(wg_hbm.at[:, cols], wg.at[i], w_sem.at[0, i]),
            pltpu.make_async_copy(wu_hbm.at[:, cols], wu.at[i], w_sem.at[1, i]),
        )

    def fetch_down(i):
        rows = pl.ds(pl.multiple_of(first + i * WIN, LANE), WIN)
        here = pl.ds(pl.multiple_of(i * WIN, LANE), WIN)
        return pltpu.make_async_copy(wd_hbm.at[rows, :], wd.at[here, :], w_sem.at[2, i])

    wg_t, wu_t = kv.at[0, :wg.shape[1], :], kv.at[1, :wu.shape[1], :]
    tail = pl.ds(pl.multiple_of(first + wide, LANE), LANE)
    tails = (
        pltpu.make_async_copy(wg_hbm.at[:, tail], wg_t, w_sem.at[0, steps]),
        pltpu.make_async_copy(wu_hbm.at[:, tail], wu_t, w_sem.at[1, steps]),
        pltpu.make_async_copy(wd_hbm.at[tail, :], wd.at[wide:, :], w_sem.at[2, steps]),
    )
    get_wo = pltpu.make_async_copy(wo_hbm, wd.at[keep:, :], w_sem.at[3, 0])
    n_keep = keep // WIN

    at_me = lax.axis_index("sp")
    get_in = [
        pltpu.make_async_copy(k_hbm, kv.at[0], in_sem.at[0]),
        pltpu.make_async_copy(v_hbm, kv.at[1], in_sem.at[1]),
        pltpu.make_async_copy(x_hbm.at[pl.ds(pl.multiple_of(at_me * 8, 8), 8), pl.ds(pl.multiple_of(x * w, LANE), w)], res, in_sem.at[2]),
        pltpu.make_async_copy(q_hbm, q_ref, in_sem.at[3]),
        pltpu.make_async_copy(pos_hbm, pos_ref, in_sem.at[4]),
        pltpu.make_async_copy(g_hbm, g_ref, in_sem.at[5]),
    ]
    for copy in (get_in[3], get_in[4], get_in[0], get_in[1], get_in[2], get_in[5]):
        copy.start()
    fetch(0)[0].start()
    planes = [
        [(turn(x, a, NX), z, turn(y, b, NY)) for a, b in XY],
        [(x, turn(z, a, NZ), turn(y, b, NY)) for a, b in XY],
        [(turn(x, a, NX), turn(z, b, NZ), y) for a, b in XY],
    ]
    near = planes[0] + [(x, turn(z, a, NZ), turn(y, b, NY)) for a in range(1, NZ) for b in range(NY)]
    near += [(turn(x, a, NX), turn(z, b, NZ), y) for a in range(1, NX) for b in range(1, NZ)]
    entry_barrier([dev(*p, c) for p in near] + [partner])

    n_grp = NZ * NY
    seq = kv.shape[1] // q_ref.shape[1]
    span = GRP * seq
    low = lax.broadcasted_iota(jnp.int32, (8, LANE), 1) < half

    def place(k):
        return turn(z, ((k + 1) // NY) % NZ, NZ), turn(y, (k + 1) % NY, NY)

    def give(k):
        return remote(pack.at[k, mate], swap.at[k], gv_send.at[k], gv_recv.at[k], partner)

    def deliver(k):
        pz, py = place(k)
        return remote(merged.at[k], slots.at[k], rs_send.at[k], rs_recv.at[k], dev(x, pz, py, c))

    def attend(k):
        pz, py = place(k)
        g = pz * NY + py
        at = pl.ds(pl.multiple_of(g * GRP, GRP), GRP)
        keys = pl.ds(pl.multiple_of(g * span, span), span)
        qs = jnp.concatenate([q_ref[h, at, :] for h in range(heads)], axis=0)
        col = lax.broadcasted_iota(jnp.int32, (GRP, span), 1)
        own = (col // seq) == lax.broadcasted_iota(jnp.int32, (GRP, span), 0)
        p = jnp.concatenate([pos_ref[at, :]] * (span // LANE), axis=1)
        valid = own & (at_me * seq + col % seq <= p)
        valid = jnp.concatenate([valid.astype(F32)] * heads, axis=0) > 0.5
        scores = lax.dot_general(qs, kv[0, keys, :], (((1,), (1,)), ((), ())), preferred_element_type=F32) * (LANE ** -0.5)
        scores = jnp.where(valid, scores, -1e30)
        top = jnp.max(scores, axis=1, keepdims=True)
        wt = jnp.where(valid, jnp.exp(scores - top), 0.0)
        tot = jnp.sum(wt, axis=1, keepdims=True)
        mix = jnp.dot(wt.astype(BF16), kv[1, keys, :], preferred_element_type=F32)
        lane = lax.broadcasted_iota(jnp.int32, (8, LANE), 1)
        for e in range(NC):
            stats = jnp.zeros((8, LANE), F32)
            for h in range(heads):
                rows = slice(h * GRP + e * 8, h * GRP + e * 8 + 8)
                pack[k, e, :, h * LANE:(h + 1) * LANE] = mix[rows]
                stats = jnp.where(lane == h, top[rows], stats)
                stats = jnp.where(lane == half + h, tot[rows], stats)
            pack[k, e, :, w:] = stats
        give(k).start()

    def pair(k):
        give(k).wait_recv()
        s1, s2 = pack[k, c, :, w:], swap[k, :, w:]
        top = jnp.maximum(s1, s2)
        f1, f2 = jnp.exp(s1 - top), jnp.exp(s2 - top)
        total = pltpu.roll(f1, half, 1) * s1 + pltpu.roll(f2, half, 1) * s2
        mix = []
        for h in range(heads):
            cut = slice(h * LANE, (h + 1) * LANE)
            mix.append(f1[:, h:h + 1] * pack[k, c, :, cut] + f2[:, h:h + 1] * swap[k, :, cut])
        return mix, jnp.where(low, top, total)

    def pass_on(k):
        mix, stats = pair(k)
        for h in range(heads):
            merged[k, :, h * LANE:(h + 1) * LANE] = mix[h]
        merged[k, :, w:] = stats
        deliver(k).start()

    lag = 4
    for i in (0, 1, 3, 4):
        get_in[i].wait()

    def begin(k, carry):
        attend(k)
        return carry

    def both(k, carry):
        for j in (2 * k, 2 * k + 1):
            attend(j)
            pass_on(j - lag)
        fetch(k - lag // 2 + 1)[0].start()
        return carry

    def finish(k, carry):
        pass_on(k)
        return carry

    lax.fori_loop(0, lag, begin, 0)
    lax.fori_loop(lag // 2, n_grp // 2, both, 0)
    lax.fori_loop(n_grp - lag, n_grp - 1, finish, 0)
    rs = [deliver(k) for k in range(n_grp - 1)]
    gives = [give(k) for k in range(n_grp)]
    early = 1 + (n_grp - lag) // 2
    get_wo.start()
    for i in range(steps):
        fetch(i)[1].start()
    for i in range(early, steps):
        fetch(i)[0].start()
    fetch_down(0).start()
    own_mix, own_stats = pair(n_grp - 1)
    for copy in rs:
        copy.wait_recv()
    top = own_stats
    for k in range(len(rs)):
        top = jnp.maximum(top, slots[k, :, w:])

    def add(stats, mix, acc_mix, total):
        factor = jnp.exp(stats - top)
        total = total + pltpu.roll(factor, half, 1) * stats
        return [acc_mix[h] + factor[:, h:h + 1] * mix[h] for h in range(heads)], total

    mixed, total = add(own_stats, own_mix, [jnp.zeros((8, LANE), F32)] * heads, jnp.zeros((8, LANE), F32))
    for k in range(len(rs)):
        mix = [slots[k, :, h * LANE:(h + 1) * LANE] for h in range(heads)]
        mixed, total = add(slots[k, :, w:], mix, mixed, total)
    attn = jnp.concatenate([mixed[h] / total[:, half + h:half + h + 1] for h in range(heads)], axis=1).astype(BF16)

    get_wo.wait()
    for n in range(0, part.shape[1], 4 * LANE):
        part[:, n:n + 4 * LANE] = jnp.dot(attn, wd[keep:, n:n + 4 * LANE], preferred_element_type=F32)
    my_cols = pl.ds(pl.multiple_of(x * w, LANE), w)
    my_rows = pl.ds(pl.multiple_of(c * 8, 8), 8)
    line = [turn(x, k, NX) for k in range(1, NX)]
    cols = [pl.ds(pl.multiple_of(px * w, LANE), w) for px in line]
    xs = []
    for k, px in enumerate(line):
        copy = remote(part.at[:, cols[k]], xslots.at[k], xs_send.at[k], xs_recv.at[k], dev(px, z, y, c))
        copy.start()
        xs.append(copy)
    for i in range(1, 5):
        fetch_down(i).start()
    sums = part[:, my_cols]
    for k, copy in enumerate(xs):
        copy.wait_recv()
        sums = sums + xslots[k]
    get_in[2].wait()
    hidden = (res[...].astype(F32) + sums).astype(BF16).astype(F32)
    chunk[...] = hidden
    ag = []
    for k, px in enumerate(line):
        copy = remote(chunk, hid.at[my_rows, my_cols], ag_send.at[k], ag_recv.at[k], dev(px, z, y, c))
        copy.start()
        ag.append(copy)
    fw = [remote(chunk, hid.at[my_rows, my_cols], fw_send.at[3], fw_recv.at[3], partner)]
    fw[0].start()
    hid[my_rows, my_cols] = hidden
    for i in range(5, steps):
        fetch_down(i).start()
    for copy in tails:
        copy.start()
    for k, copy in enumerate(ag):
        copy.wait_recv()
        block = hid.at[my_rows, cols[2 - k]]
        copy = remote(block, block, fw_send.at[k], fw_recv.at[k], partner)
        copy.start()
        fw.append(copy)
    for copy in fw:
        copy.wait_recv()

    get_in[5].wait()

    h32 = hid[...]
    inv = lax.rsqrt(jnp.mean(h32 * h32, axis=-1, keepdims=True) + NORM_EPS)
    hn[...] = (h32 * inv * g_ref[...].astype(F32)).astype(BF16)
    acc[...] = jnp.zeros_like(acc)
    mid = (ff // LANE + 1) // 2 * LANE

    def gated(gate, up, start):
        gate = gate.astype(BF16).astype(F32)
        up = up.astype(BF16).astype(F32)
        col = lax.broadcasted_iota(jnp.int32, gate.shape, 1) + start
        lo = c * mid
        act = jax.nn.silu(gate) * up
        return jnp.where((col >= lo) & (col < mid + c * ff), act, 0.0).astype(BF16)

    def mlp_step(i, carry):
        cg, cu = fetch(i)
        cg.wait()
        gate = jnp.dot(hn[...], wg[i], preferred_element_type=F32)
        cu.wait()
        up = jnp.dot(hn[...], wu[i], preferred_element_type=F32)
        act = gated(gate, up, first + i * WIN)
        fetch_down(i).wait()
        here = pl.ds(pl.multiple_of(i * WIN, LANE), WIN)
        acc[...] += jnp.dot(act, wd[here, :], preferred_element_type=F32)
        return carry

    lax.fori_loop(0, steps, mlp_step, 0)
    tails[0].wait()
    gate = jnp.dot(hn[...], wg_t[...], preferred_element_type=F32)
    tails[1].wait()
    up = jnp.dot(hn[...], wu_t[...], preferred_element_type=F32)
    act = gated(gate, up, first + wide)
    tails[2].wait()
    acc[...] += jnp.dot(act, wd[wide:, :], preferred_element_type=F32)

    mate_rows = pl.ds(pl.multiple_of(mate * 8, 8), 8)
    back = remote(acc.at[mate_rows, :], cslot, c_sem.at[0], c_sem.at[1], partner)
    back.start()
    for copy in xs:
        copy.wait_send()
    back.wait_recv()
    part[...] = acc[my_rows, :] + cslot[...]
    xo = []
    for k, px in enumerate(line):
        copy = remote(part.at[:, cols[k]], xslots.at[k + 3], xo_send.at[k], xo_recv.at[k], dev(px, z, y, c))
        copy.start()
        xo.append(copy)
    sums = part[:, my_cols]
    for k, copy in enumerate(xo):
        copy.wait_recv()
        sums = sums + xslots[k + 3]
    out = (hidden + sums).astype(BF16).astype(F32)
    for copy in ag + fw[:1]:
        copy.wait_send()
    chunk[...] = out

    cut = [(0, 2 * LANE), (2 * LANE, 2 * LANE), (4 * LANE, w - 4 * LANE)]
    order = (0, 1, 3, 2)
    p1 = {}
    for d in order:
        for p, (lo, n) in enumerate(cut):
            for k in range(15):
                if XY[k][1] == d:
                    src, dst = chunk.at[:, lo:lo + n], buf.at[z, y, c, x, :, lo:lo + n]
                    p1[p, k] = remote(src, dst, p1_send.at[p, k], p1_recv.at[p, k], dev(*planes[p][k], c))
                    p1[p, k].start()
    buf[z, y, c, x] = out

    def line_of(p, v, d):
        lo, n = cut[p]
        cols_p = slice(lo, lo + n)
        b = turn((y, y, z)[p], (4 - d) % 4, 4)
        return [buf.at[v, b, c, :, :, cols_p], buf.at[:, b, c, v, :, cols_p], buf.at[b, v, c, :, :, cols_p]][p]

    here = [z, x, y]
    up1 = [dev(x, turn(z, 1, 4), y, c), dev(turn(x, 1, 4), z, y, c), dev(x, z, turn(y, 1, 4), c)]
    dn1 = [dev(x, turn(z, 3, 4), y, c), dev(turn(x, 3, 4), z, y, c), dev(x, z, turn(y, 3, 4), c)]
    done, crossed = [], []

    def send(p, v, d, to, kind):
        ref = line_of(p, v, d)
        copy = remote(ref, ref, p2_send.at[p, kind * 4 + d], p2_recv.at[p, kind * 4 + d], to)
        copy.start()
        done.append(copy)
        return copy

    def across(p, v, d, kind):
        ref = line_of(p, v, d)
        copy = remote(ref, ref, cc_send.at[p, kind * 4 + d], cc_recv.at[p, kind * 4 + d], partner)
        copy.start()
        done.append(copy)
        crossed.append(copy)

    ups, downs, relays = {}, {}, {}
    for d in order:
        for p in range(3):
            for k in range(15):
                if XY[k][1] == d:
                    p1[p, k].wait_recv()
            ups[p, d] = send(p, here[p], d, up1[p], 0)
            downs[p, d] = send(p, here[p], d, dn1[p], 1)
            across(p, here[p], d, 0)
    for d in order:
        for p in range(3):
            below, above = turn(here[p], 3, 4), turn(here[p], 1, 4)
            ups[p, d].wait_recv()
            if d < 2:
                relays[p, d] = send(p, below, d, up1[p], 2)
            downs[p, d].wait_recv()
            if d >= 2:
                relays[p, d] = send(p, above, d, dn1[p], 2)
            across(p, below, d, 1)
            across(p, above, d, 2)
    for d in order:
        for p in range(3):
            relays[p, d].wait_recv()
            across(p, turn(here[p], 2, 4), d, 3)
    for copy in crossed:
        copy.wait_recv()
    puts = []
    for a in range(NZ):
        for b in range(NY):
            for e in range(NC):
                r = ((a * NY + b) * NC + e) * 8
                for d in range(NX):
                    wd[r:r + 8, d * w:(d + 1) * w] = buf[a, b, e, d].astype(BF16)
        at = slice(a * NY * NC * 8, (a + 1) * NY * NC * 8)
        put = pltpu.make_async_copy(wd.at[at, :], out_hbm.at[at, :], out_sem.at[a])
        put.start()
        puts.append(put)
    for copy in gives + [back] + rs + fw[1:] + xo + list(p1.values()) + done:
        copy.wait_send()
    for put in puts:
        put.wait()


def layer(q, pos, x_tok, ko, vo, g, wo, wg, wu, wd):
    rows, width = x_tok.shape
    w = width // NX
    keys = rows * ko.shape[1]
    steps = ((wg.shape[1] // LANE + 1) // 2 * LANE) // WIN
    sem = pltpu.SemaphoreType.DMA
    hbm = pl.BlockSpec(memory_space=pl.ANY)
    return pl.pallas_call(
        layer_kernel,
        name="layer",
        out_shape=jax.ShapeDtypeStruct((rows, width), BF16),
        in_specs=[hbm] * 10,
        out_specs=hbm,
        scratch_shapes=[
            pltpu.VMEM(q.shape, BF16),
            pltpu.VMEM(pos.shape, jnp.int32),
            pltpu.VMEM(g.shape, BF16),
            pltpu.VMEM((2, keys, LANE), BF16),
            pltpu.VMEM((8, w), BF16),
            pltpu.VMEM((NZ * NY, NC, 8, w + LANE), F32),
            pltpu.VMEM((NZ * NY, 8, w + LANE), F32),
            pltpu.VMEM((15, 8, w + LANE), F32),
            pltpu.VMEM((15, 8, w + LANE), F32),
            pltpu.VMEM((8, width), F32),
            pltpu.VMEM((6, 8, w), F32),
            pltpu.VMEM((8, w), F32),
            pltpu.VMEM((8 * NC, width), F32),
            pltpu.VMEM((8 * NC, width), BF16),
            pltpu.VMEM((8 * NC, width), F32),
            pltpu.VMEM((8, width), F32),
            pltpu.VMEM((NZ, NY, NC, NX, 8, w), F32),
            pltpu.VMEM((steps, width, WIN), BF16),
            pltpu.VMEM((steps, width, WIN), BF16),
            pltpu.VMEM((steps * WIN + LANE, width), BF16),
            sem((4, steps + 1)),
            sem((NZ,)),
            sem((6,)), sem((16,)), sem((16,)), sem((15,)), sem((15,)), sem((3,)), sem((3,)), sem((3,)), sem((3,)), sem((4,)), sem((4,)),
            sem((2,)), sem((3,)), sem((3,)), sem((3, 15)), sem((3, 15)), sem((3, 12)), sem((3, 12)), sem((3, 16)), sem((3, 16)),
        ],
        compiler_params=pltpu.CompilerParams(collective_id=0, has_side_effects=True, vmem_limit_bytes=VMEM_ALL),
    )(q, pos, g, x_tok, ko.reshape(keys, LANE), vo.reshape(keys, LANE), wo, wg, wu, wd)


GRP = 16


def project_kernel(lens_ref, lens_row, g_ref, freq_ref, x_hbm, k_hbm, v_hbm, wq_hbm, wk_hbm, wv_hbm, q_ref, pos_ref, ko_hbm, vo_hbm, xs, u, w, kv, knew, vnew, sem, out_sem):
    rows, width = xs.shape
    heads = q_ref.shape[0]
    hd = heads * LANE
    seq = kv.shape[2]
    half = LANE // 2
    base = lax.axis_index("sp") * seq
    n_x, n_out = 2, 4
    part = rows // n_x
    get_x = [pltpu.make_async_copy(x_hbm.at[i * part:(i + 1) * part], xs.at[i * part:(i + 1) * part], sem.at[i]) for i in range(n_x)]
    get_kv = [
        pltpu.make_async_copy(wk_hbm, w.at[:, hd:hd + LANE], sem.at[2]),
        pltpu.make_async_copy(wv_hbm, w.at[:, hd + LANE:], sem.at[3]),
    ]
    get_cache = [pltpu.make_async_copy(k_hbm, kv.at[0], sem.at[4]), pltpu.make_async_copy(v_hbm, kv.at[1], sem.at[5])]
    cuts = [(i, min(2 * LANE, hd - i)) for i in range(0, hd, 2 * LANE)]
    get_q = [pltpu.make_async_copy(wq_hbm.at[:, i:i + n], w.at[:, i:i + n], sem.at[6 + j]) for j, (i, n) in enumerate(cuts)]
    for copy in get_x + get_kv + get_cache + get_q:
        copy.start()

    eye = lax.broadcasted_iota(jnp.int32, (LANE, LANE), 0) == lax.broadcasted_iota(jnp.int32, (LANE, LANE), 1)
    cols = []
    for i in range(rows // LANE):
        line = lens_row[i:i + 1, :].astype(F32)
        col = jnp.sum(jnp.where(eye, line, 0.0), axis=1, keepdims=True)
        pos_ref[i * LANE:(i + 1) * LANE, :] = jnp.broadcast_to(col, (LANE, LANE)).astype(jnp.int32)
        cols.append(col)
    low = lax.broadcasted_iota(jnp.int32, (LANE, LANE), 1) < half
    angles = jnp.where(low, cols[0], cols[1]) * freq_ref[...]
    cos = jnp.cos(angles)
    sin = jnp.sin(angles)
    cos_r = pltpu.roll(cos, half, 1)
    sin_r = pltpu.roll(sin, half, 1)
    cos_t = jnp.concatenate([jnp.where(low, cos, cos_r), jnp.where(low, cos_r, cos)], axis=0)
    sin_t = jnp.concatenate([jnp.where(low, -sin, sin_r), jnp.where(low, -sin_r, sin)], axis=0)

    def norm(i, carry):
        at = pl.ds(pl.multiple_of(i * GRP, GRP), GRP)
        x32 = xs[at, :].astype(F32)
        inv = lax.rsqrt(jnp.mean(x32 * x32, axis=-1, keepdims=True) + NORM_EPS)
        u[at, :] = (x32 * inv * g_ref[...].astype(F32)).astype(BF16)
        return carry

    for i in range(n_x):
        get_x[i].wait()
        lax.fori_loop(i * part // GRP, (i + 1) * part // GRP, norm, 0)

    def rope(t):
        return (t * cos_t + pltpu.roll(t, half, 1) * sin_t).astype(BF16)

    for copy in get_kv:
        copy.wait()
    out = jnp.dot(u[...], w[:, hd:], preferred_element_type=F32).astype(BF16).astype(F32)
    knew[...] = rope(out[:, :LANE]).astype(F32)
    vnew[...] = out[:, LANE:]
    for copy in get_cache:
        copy.wait()
    line = lax.broadcasted_iota(jnp.int32, (seq, LANE), 0)

    def put(i, carry):
        for j in range(GRP):
            b = i * GRP + j
            here = line == lens_ref[b] - base
            kv[0, b] = jnp.where(here, knew[pl.ds(b, 1), :], kv[0, b].astype(F32)).astype(BF16)
            kv[1, b] = jnp.where(here, vnew[pl.ds(b, 1), :], kv[1, b].astype(F32)).astype(BF16)
        return carry

    puts = []
    part = rows // n_out
    for i in range(n_out):
        lax.fori_loop(i * part // GRP, (i + 1) * part // GRP, put, 0)
        at = slice(i * part, (i + 1) * part)
        for j, ref in enumerate((ko_hbm, vo_hbm)):
            copy = pltpu.make_async_copy(kv.at[j, at], ref.at[at], out_sem.at[j, i])
            copy.start()
            puts.append(copy)
    for copy, (a, n) in zip(get_q, cuts):
        copy.wait()
        out = jnp.dot(u[...], w[:, a:a + n], preferred_element_type=F32).astype(BF16).astype(F32)
        for j in range(0, n, LANE):
            q_ref[(a + j) // LANE] = rope(out[:, j:j + LANE])
    for copy in puts:
        copy.wait()


def project(x_tok, seq_lens, k_blk, v_blk, g, wq, wk, wv):
    rows, width = x_tok.shape
    seq = k_blk.shape[1]
    hd = wq.shape[1]
    half = LANE // 2
    freq = np.float32(ROPE_BASE) ** (np.arange(half, dtype=np.float32) * np.float32(-2.0 / LANE))
    freq = jnp.asarray(np.concatenate([freq, freq]).reshape(1, LANE).astype(np.float32))
    vmem = pl.BlockSpec(memory_space=pltpu.VMEM)
    hbm = pl.BlockSpec(memory_space=pl.ANY)
    sem = pltpu.SemaphoreType.DMA
    cache = jax.ShapeDtypeStruct((rows, seq, LANE), BF16)
    return pl.pallas_call(
        project_kernel,
        name="project",
        out_shape=[
            jax.ShapeDtypeStruct((hd // LANE, rows, LANE), BF16),
            jax.ShapeDtypeStruct((rows, LANE), jnp.int32),
            cache,
            cache,
        ],
        in_specs=[pl.BlockSpec(memory_space=pltpu.SMEM), vmem, vmem, vmem] + [hbm] * 6,
        out_specs=[vmem, vmem, hbm, hbm],
        scratch_shapes=[
            pltpu.VMEM((rows, width), BF16),
            pltpu.VMEM((rows, width), BF16),
            pltpu.VMEM((width, hd + 2 * LANE), BF16),
            pltpu.VMEM((2, rows, seq, LANE), BF16),
            pltpu.VMEM((rows, LANE), F32),
            pltpu.VMEM((rows, LANE), F32),
            sem((10,)),
            sem((2, 4)),
        ],
        compiler_params=pltpu.CompilerParams(vmem_limit_bytes=VMEM_ALL),
    )(seq_lens, seq_lens.reshape(rows // LANE, LANE), g, freq, x_tok, k_blk.reshape(cache.shape), v_blk.reshape(cache.shape), wq, wk, wv)


def solution(mesh):
    cache_spec = P(None, "sp", "tp", None)
    col_spec = P(None, "tp")
    row_spec = P("tp", None)
    full_spec = P()

    def local_step(x_tok, seq_lens, k_blk, v_blk, g_attn, wq_loc, wk_loc, wv_loc, wo_loc, g_mlp, wg_loc, wu_loc, wd_loc):
        q, pos, ko, vo = project(x_tok, seq_lens, k_blk, v_blk, g_attn, wq_loc, wk_loc, wv_loc)
        y_out = layer(q, pos, x_tok, ko, vo, g_mlp, wo_loc, wg_loc, wu_loc, wd_loc)
        return y_out, ko.reshape(k_blk.shape), vo.reshape(v_blk.shape)

    return jax.shard_map(local_step, mesh=mesh, in_specs=(full_spec, full_spec, cache_spec, cache_spec, full_spec, col_spec, col_spec, col_spec, row_spec, full_spec, col_spec, col_spec, row_spec), out_specs=(full_spec, cache_spec, cache_spec), check_vma=False)
```

```python
import jax
import jax.numpy as jnp
import numpy as np
from jax import lax
from jax.experimental import pallas as pl
from jax.experimental.pallas import tpu as pltpu
from jax.sharding import PartitionSpec as P

ROPE_BASE = 500000.0
NORM_EPS = 1e-5
MESH = pl.DeviceIdType.MESH
F32 = jnp.float32
BF16 = jnp.bfloat16
NX, NZ, NY, NC = 4, 4, 4, 2
LANE = 128
VMEM_ALL = 67043328


def coords():
    s = lax.axis_index("sp")
    return lax.axis_index("tp"), s // (NY * NC), (s // NC) % NY, s % NC


def dev(x, z, y, c):
    return (x, (z * NY + y) * NC + c)


def turn(v, d, n):
    return lax.rem(v + d, n)


def entry_barrier(peers):
    barrier = pltpu.get_barrier_semaphore()
    for peer in peers:
        pl.semaphore_signal(barrier, inc=1, device_id=peer, device_id_type=MESH)
    pl.semaphore_wait(barrier, len(peers))


def remote(src, dst, send_sem, recv_sem, peer):
    return pltpu.make_async_remote_copy(
        src_ref=src, dst_ref=dst, send_sem=send_sem, recv_sem=recv_sem, device_id=peer, device_id_type=MESH
    )


XY = [(dx, dy) for dx in range(4) for dy in range(4)][1:]
WIN = 256


def layer_kernel(
    q_hbm, pos_hbm, g_hbm, x_hbm, k_hbm, v_hbm, wo_hbm, wg_hbm, wu_hbm, wd_hbm, out_hbm,
    q_ref, pos_ref, g_ref, kv, res, pack, swap, merged, slots, part, xslots, chunk, hid, hn, acts, acc, outs, cslot, buf,
    wg, wu, wd,
    w_sem, out_sem, in_sem, gv_send, gv_recv, rs_send, rs_recv, xs_send, xs_recv, ag_send, ag_recv, fw_send, fw_recv,
    c_send, c_recv, xo_send, xo_recv, p1_send, p1_recv, p2_send, p2_recv, cc_send, cc_recv,
):
    x, z, y, c = coords()
    w = chunk.shape[1]
    heads = w // LANE
    half = LANE // 2
    mate = turn(c, 1, NC)
    partner = dev(x, z, y, mate)
    steps = wg.shape[0]
    wide = steps * WIN
    ff = wg_hbm.shape[1]
    window = wide + LANE
    first = pl.multiple_of(c * (ff - window), LANE)
    keep = wd.shape[0] - wo_hbm.shape[0]

    def fetch(i):
        cols = pl.ds(pl.multiple_of(first + i * WIN, LANE), WIN)
        return (
            pltpu.make_async_copy(wg_hbm.at[:, cols], wg.at[i], w_sem.at[0, i]),
            pltpu.make_async_copy(wu_hbm.at[:, cols], wu.at[i], w_sem.at[1, i]),
        )

    def fetch_down(i):
        rows = pl.ds(pl.multiple_of(first + i * WIN, LANE), WIN)
        here = pl.ds(pl.multiple_of(i * WIN, LANE), WIN)
        return pltpu.make_async_copy(wd_hbm.at[rows, :], wd.at[here, :], w_sem.at[2, i])

    wg_t, wu_t = kv.at[0, :wg.shape[1], :], kv.at[1, :wu.shape[1], :]
    tail = pl.ds(pl.multiple_of(first + wide, LANE), LANE)
    tails = (
        pltpu.make_async_copy(wg_hbm.at[:, tail], wg_t, w_sem.at[0, steps]),
        pltpu.make_async_copy(wu_hbm.at[:, tail], wu_t, w_sem.at[1, steps]),
        pltpu.make_async_copy(wd_hbm.at[tail, :], wd.at[wide:, :], w_sem.at[2, steps]),
    )
    get_wo = pltpu.make_async_copy(wo_hbm, wd.at[keep:, :], w_sem.at[3, 0])
    n_keep = keep // WIN

    at_me = lax.axis_index("sp")
    get_in = [
        pltpu.make_async_copy(k_hbm, kv.at[0], in_sem.at[0]),
        pltpu.make_async_copy(v_hbm, kv.at[1], in_sem.at[1]),
        pltpu.make_async_copy(x_hbm.at[pl.ds(pl.multiple_of(at_me * 8, 8), 8), pl.ds(pl.multiple_of(x * w, LANE), w)], res, in_sem.at[2]),
        pltpu.make_async_copy(q_hbm, q_ref, in_sem.at[3]),
        pltpu.make_async_copy(pos_hbm, pos_ref, in_sem.at[4]),
        pltpu.make_async_copy(g_hbm, g_ref, in_sem.at[5]),
    ]
    for copy in (get_in[3], get_in[4], get_in[0], get_in[1], get_in[2], get_in[5]):
        copy.start()
    planes = [
        [(turn(x, a, NX), z, turn(y, b, NY)) for a, b in XY],
        [(x, turn(z, a, NZ), turn(y, b, NY)) for a, b in XY],
        [(turn(x, a, NX), turn(z, b, NZ), y) for a, b in XY],
    ]
    near = planes[0] + [(x, turn(z, a, NZ), turn(y, b, NY)) for a in range(1, NZ) for b in range(NY)]
    near += [(turn(x, a, NX), turn(z, b, NZ), y) for a in range(1, NX) for b in range(1, NZ)]
    entry_barrier([dev(*p, c) for p in near] + [partner])

    n_grp = NZ * NY
    seq = kv.shape[1] // q_ref.shape[1]
    span = GRP * seq
    low = lax.broadcasted_iota(jnp.int32, (8, LANE), 1) < half

    def place(k):
        return turn(z, ((k + 1) // NY) % NZ, NZ), turn(y, (k + 1) % NY, NY)

    def give(k):
        return remote(pack.at[k, mate], swap.at[k], gv_send.at[k], gv_recv.at[k], partner)

    def deliver(k):
        pz, py = place(k)
        return remote(merged.at[k], slots.at[k], rs_send.at[k], rs_recv.at[k], dev(x, pz, py, c))

    def attend(k):
        pz, py = place(k)
        g = pz * NY + py
        at = pl.ds(pl.multiple_of(g * GRP, GRP), GRP)
        keys = pl.ds(pl.multiple_of(g * span, span), span)
        qs = jnp.concatenate([q_ref[h, at, :] for h in range(heads)], axis=0)
        col = lax.broadcasted_iota(jnp.int32, (GRP, span), 1)
        own = (col // seq) == lax.broadcasted_iota(jnp.int32, (GRP, span), 0)
        p = jnp.concatenate([pos_ref[at, :]] * (span // LANE), axis=1)
        valid = own & (at_me * seq + col % seq <= p)
        valid = jnp.concatenate([valid.astype(F32)] * heads, axis=0) > 0.5
        scores = lax.dot_general(qs, kv[0, keys, :], (((1,), (1,)), ((), ())), preferred_element_type=F32) * (LANE ** -0.5)
        scores = jnp.where(valid, scores, -1e30)
        top = jnp.max(scores, axis=1, keepdims=True)
        wt = jnp.where(valid, jnp.exp(scores - top), 0.0)
        tot = jnp.sum(wt, axis=1, keepdims=True)
        mix = jnp.dot(wt.astype(BF16), kv[1, keys, :], preferred_element_type=F32)
        lane = lax.broadcasted_iota(jnp.int32, (8, LANE), 1)
        for e in range(NC):
            stats = jnp.zeros((8, LANE), F32)
            for h in range(heads):
                rows = slice(h * GRP + e * 8, h * GRP + e * 8 + 8)
                pack[k, e, :, h * LANE:(h + 1) * LANE] = mix[rows]
                stats = jnp.where(lane == h, top[rows], stats)
                stats = jnp.where(lane == half + h, tot[rows], stats)
            pack[k, e, :, w:] = stats
        give(k).start()

    def pair(k):
        give(k).wait_recv()
        s1, s2 = pack[k, c, :, w:], swap[k, :, w:]
        top = jnp.maximum(s1, s2)
        f1, f2 = jnp.exp(s1 - top), jnp.exp(s2 - top)
        total = pltpu.roll(f1, half, 1) * s1 + pltpu.roll(f2, half, 1) * s2
        mix = []
        for h in range(heads):
            cut = slice(h * LANE, (h + 1) * LANE)
            mix.append(f1[:, h:h + 1] * pack[k, c, :, cut] + f2[:, h:h + 1] * swap[k, :, cut])
        return mix, jnp.where(low, top, total)

    def pass_on(k):
        mix, stats = pair(k)
        for h in range(heads):
            merged[k, :, h * LANE:(h + 1) * LANE] = mix[h]
        merged[k, :, w:] = stats
        deliver(k).start()

    lag = 4
    for i in (0, 1, 3, 4):
        get_in[i].wait()
    get_wo.start()
    fetch(0)[0].start()

    def begin(k, carry):
        attend(k)
        return carry

    def both(k, carry):
        for j in (2 * k, 2 * k + 1):
            attend(j)
            pass_on(j - lag)
        fetch(k - lag // 2 + 1)[0].start()
        return carry

    def finish(k, carry):
        pass_on(k)
        return carry

    lax.fori_loop(0, lag, begin, 0)
    lax.fori_loop(lag // 2, n_grp // 2, both, 0)
    lax.fori_loop(n_grp - lag, n_grp - 1, finish, 0)
    rs = [deliver(k) for k in range(n_grp - 1)]
    gives = [give(k) for k in range(n_grp)]
    early = 1 + (n_grp - lag) // 2
    for i in range(steps):
        fetch(i)[1].start()
    for i in range(early, steps):
        fetch(i)[0].start()
    fetch_down(0).start()
    own_mix, own_stats = pair(n_grp - 1)
    for copy in rs:
        copy.wait_recv()
    top = own_stats
    for k in range(len(rs)):
        top = jnp.maximum(top, slots[k, :, w:])

    def add(stats, mix, acc_mix, total):
        factor = jnp.exp(stats - top)
        total = total + pltpu.roll(factor, half, 1) * stats
        return [acc_mix[h] + factor[:, h:h + 1] * mix[h] for h in range(heads)], total

    mixed, total = add(own_stats, own_mix, [jnp.zeros((8, LANE), F32)] * heads, jnp.zeros((8, LANE), F32))
    for k in range(len(rs)):
        mix = [slots[k, :, h * LANE:(h + 1) * LANE] for h in range(heads)]
        mixed, total = add(slots[k, :, w:], mix, mixed, total)
    attn = jnp.concatenate([mixed[h] / total[:, half + h:half + h + 1] for h in range(heads)], axis=1).astype(BF16)

    get_wo.wait()
    for n in range(0, part.shape[1], 4 * LANE):
        part[:, n:n + 4 * LANE] = jnp.dot(attn, wd[keep:, n:n + 4 * LANE], preferred_element_type=F32)
    my_cols = pl.ds(pl.multiple_of(x * w, LANE), w)
    my_rows = pl.ds(pl.multiple_of(c * 8, 8), 8)
    line = [turn(x, k, NX) for k in range(1, NX)]
    cols = [pl.ds(pl.multiple_of(px * w, LANE), w) for px in line]
    xs = []
    for k, px in enumerate(line):
        copy = remote(part.at[:, cols[k]], xslots.at[k], xs_send.at[k], xs_recv.at[k], dev(px, z, y, c))
        copy.start()
        xs.append(copy)
    for i in range(1, 5):
        fetch_down(i).start()
    sums = part[:, my_cols]
    for k, copy in enumerate(xs):
        copy.wait_recv()
        sums = sums + xslots[k]
    get_in[2].wait()
    hidden = (res[...].astype(F32) + sums).astype(BF16).astype(F32)
    chunk[...] = hidden
    ag = []
    for k, px in enumerate(line):
        copy = remote(chunk, hid.at[my_rows, my_cols], ag_send.at[k], ag_recv.at[k], dev(px, z, y, c))
        copy.start()
        ag.append(copy)
    fw = [remote(chunk, hid.at[my_rows, my_cols], fw_send.at[3], fw_recv.at[3], partner)]
    fw[0].start()
    hid[my_rows, my_cols] = hidden
    for i in range(5, steps):
        fetch_down(i).start()
    for copy in tails:
        copy.start()
    for k, copy in enumerate(ag):
        copy.wait_recv()
        block = hid.at[my_rows, cols[2 - k]]
        copy = remote(block, block, fw_send.at[k], fw_recv.at[k], partner)
        copy.start()
        fw.append(copy)
    for copy in fw:
        copy.wait_recv()

    get_in[5].wait()

    h32 = hid[...]
    inv = lax.rsqrt(jnp.mean(h32 * h32, axis=-1, keepdims=True) + NORM_EPS)
    hn[...] = (h32 * inv * g_ref[...].astype(F32)).astype(BF16)
    mid = (ff // LANE + 1) // 2 * LANE

    def gated(gate, up, start):
        gate = gate.astype(BF16).astype(F32)
        up = up.astype(BF16).astype(F32)
        col = lax.broadcasted_iota(jnp.int32, gate.shape, 1) + start
        lo = c * mid
        act = jax.nn.silu(gate) * up
        return jnp.where((col >= lo) & (col < mid + c * ff), act, 0.0).astype(BF16)

    def mlp_step(i, carry):
        cg, cu = fetch(i)
        cg.wait()
        gate = jnp.dot(hn[...], wg[i], preferred_element_type=F32)
        cu.wait()
        up = jnp.dot(hn[...], wu[i], preferred_element_type=F32)
        act = gated(gate, up, first + i * WIN)
        acts[:, pl.ds(pl.multiple_of(i * WIN, LANE), WIN)] = act
        return carry

    lax.fori_loop(0, steps, mlp_step, 0)
    tails[0].wait()
    gate = jnp.dot(hn[...], wg_t[...], preferred_element_type=F32)
    tails[1].wait()
    up = jnp.dot(hn[...], wu_t[...], preferred_element_type=F32)
    acts[:, wide:] = gated(gate, up, first + wide)
    for i in range(steps):
        fetch_down(i).wait()
    tails[2].wait()

    mate_rows = pl.ds(pl.multiple_of(mate * 8, 8), 8)
    hops = (2, 1, 3, 0)
    back, xo = [], []

    def to_owner(j):
        back[j].wait_recv()
        outs[j] = acc[j, my_rows, :] + cslot[j]
        owner = dev(turn(x, hops[j], NX), z, y, c)
        copy = remote(outs.at[j], xslots.at[j + 3], xo_send.at[j], xo_recv.at[j], owner)
        copy.start()
        xo.append(copy)

    for j, hop in enumerate(hops):
        own = pl.ds(pl.multiple_of(turn(x, hop, NX) * w, LANE), w)
        acc[j] = jnp.dot(acts[...], wd[:, own], preferred_element_type=F32)
        copy = remote(acc.at[j, mate_rows, :], cslot.at[j], c_send.at[j], c_recv.at[j], partner)
        copy.start()
        back.append(copy)
        if j >= 2:
            to_owner(j - 2)
    to_owner(2)
    back[3].wait_recv()
    sums = acc[3, my_rows, :] + cslot[3]
    for copy in xs:
        copy.wait_send()
    for k, copy in enumerate(xo):
        copy.wait_recv()
        sums = sums + xslots[k + 3]
    out = (hidden + sums).astype(BF16).astype(F32)
    for copy in ag + fw[:1]:
        copy.wait_send()
    chunk[...] = out

    cut = [(0, 2 * LANE), (2 * LANE, 2 * LANE), (4 * LANE, w - 4 * LANE)]
    order = (0, 1, 3, 2)
    p1 = {}
    for d in order:
        for p, (lo, n) in enumerate(cut):
            for k in range(15):
                if XY[k][1] == d:
                    src, dst = chunk.at[:, lo:lo + n], buf.at[z, y, c, x, :, lo:lo + n]
                    p1[p, k] = remote(src, dst, p1_send.at[p, k], p1_recv.at[p, k], dev(*planes[p][k], c))
                    p1[p, k].start()
    buf[z, y, c, x] = out

    def line_of(p, v, d):
        lo, n = cut[p]
        cols_p = slice(lo, lo + n)
        b = turn((y, y, z)[p], (4 - d) % 4, 4)
        return [buf.at[v, b, c, :, :, cols_p], buf.at[:, b, c, v, :, cols_p], buf.at[b, v, c, :, :, cols_p]][p]

    here = [z, x, y]
    up1 = [dev(x, turn(z, 1, 4), y, c), dev(turn(x, 1, 4), z, y, c), dev(x, z, turn(y, 1, 4), c)]
    dn1 = [dev(x, turn(z, 3, 4), y, c), dev(turn(x, 3, 4), z, y, c), dev(x, z, turn(y, 3, 4), c)]
    far1 = [dev(x, turn(z, 2, 4), y, c), dev(turn(x, 2, 4), z, y, c), dev(x, z, turn(y, 2, 4), c)]
    done, crossed = [], []

    def send(p, v, d, to, kind):
        ref = line_of(p, v, d)
        copy = remote(ref, ref, p2_send.at[p, kind * 4 + d], p2_recv.at[p, kind * 4 + d], to)
        copy.start()
        done.append(copy)
        return copy

    def across(p, v, d, kind):
        ref = line_of(p, v, d)
        copy = remote(ref, ref, cc_send.at[p, kind * 4 + d], cc_recv.at[p, kind * 4 + d], partner)
        copy.start()
        done.append(copy)
        crossed.append(copy)

    ups, downs, relays = {}, {}, {}
    for d in order:
        for p in range(3):
            for k in range(15):
                if XY[k][1] == d:
                    p1[p, k].wait_recv()
            ups[p, d] = send(p, here[p], d, up1[p], 0)
            downs[p, d] = send(p, here[p], d, dn1[p], 1)
            if d == 2:
                relays[p, d] = send(p, here[p], d, far1[p], 2)
            across(p, here[p], d, 0)
    for d in order:
        for p in range(3):
            below, above = turn(here[p], 3, 4), turn(here[p], 1, 4)
            ups[p, d].wait_recv()
            if d < 2:
                relays[p, d] = send(p, below, d, up1[p], 2)
            downs[p, d].wait_recv()
            if d == 3:
                relays[p, d] = send(p, above, d, dn1[p], 2)
            across(p, below, d, 1)
            across(p, above, d, 2)
    for d in order:
        for p in range(3):
            relays[p, d].wait_recv()
            across(p, turn(here[p], 2, 4), d, 3)
    for copy in crossed:
        copy.wait_recv()
    puts = []
    for a in range(NZ):
        for b in range(NY):
            for e in range(NC):
                r = ((a * NY + b) * NC + e) * 8
                for d in range(NX):
                    wd[r:r + 8, d * w:(d + 1) * w] = buf[a, b, e, d].astype(BF16)
        at = slice(a * NY * NC * 8, (a + 1) * NY * NC * 8)
        put = pltpu.make_async_copy(wd.at[at, :], out_hbm.at[at, :], out_sem.at[a])
        put.start()
        puts.append(put)
    for copy in gives + back + rs + fw[1:] + xo + list(p1.values()) + done:
        copy.wait_send()
    for put in puts:
        put.wait()


def layer(q, pos, x_tok, ko, vo, g, wo, wg, wu, wd):
    rows, width = x_tok.shape
    w = width // NX
    keys = rows * ko.shape[1]
    steps = ((wg.shape[1] // LANE + 1) // 2 * LANE) // WIN
    sem = pltpu.SemaphoreType.DMA
    hbm = pl.BlockSpec(memory_space=pl.ANY)
    return pl.pallas_call(
        layer_kernel,
        name="layer",
        out_shape=jax.ShapeDtypeStruct((rows, width), BF16),
        in_specs=[hbm] * 10,
        out_specs=hbm,
        scratch_shapes=[
            pltpu.VMEM(q.shape, BF16),
            pltpu.VMEM(pos.shape, jnp.int32),
            pltpu.VMEM(g.shape, BF16),
            pltpu.VMEM((2, keys, LANE), BF16),
            pltpu.VMEM((8, w), BF16),
            pltpu.VMEM((NZ * NY, NC, 8, w + LANE), F32),
            pltpu.VMEM((NZ * NY, 8, w + LANE), F32),
            pltpu.VMEM((15, 8, w + LANE), F32),
            pltpu.VMEM((15, 8, w + LANE), F32),
            pltpu.VMEM((8, width), F32),
            pltpu.VMEM((6, 8, w), F32),
            pltpu.VMEM((8, w), F32),
            pltpu.VMEM((8 * NC, width), F32),
            pltpu.VMEM((8 * NC, width), BF16),
            pltpu.VMEM((8 * NC, steps * WIN + LANE), BF16),
            pltpu.VMEM((NX, 8 * NC, w), F32),
            pltpu.VMEM((NX - 1, 8, w), F32),
            pltpu.VMEM((NX, 8, w), F32),
            pltpu.VMEM((NZ, NY, NC, NX, 8, w), F32),
            pltpu.VMEM((steps, width, WIN), BF16),
            pltpu.VMEM((steps, width, WIN), BF16),
            pltpu.VMEM((steps * WIN + LANE, width), BF16),
            sem((4, steps + 1)),
            sem((NZ,)),
            sem((6,)), sem((16,)), sem((16,)), sem((15,)), sem((15,)), sem((3,)), sem((3,)), sem((3,)), sem((3,)), sem((4,)), sem((4,)),
            sem((4,)), sem((4,)), sem((3,)), sem((3,)), sem((3, 15)), sem((3, 15)), sem((3, 12)), sem((3, 12)), sem((3, 16)), sem((3, 16)),
        ],
        compiler_params=pltpu.CompilerParams(collective_id=0, has_side_effects=True, vmem_limit_bytes=VMEM_ALL),
    )(q, pos, g, x_tok, ko.reshape(keys, LANE), vo.reshape(keys, LANE), wo, wg, wu, wd)


GRP = 16


def project_kernel(lens_ref, lens_row, g_ref, freq_ref, x_hbm, k_hbm, v_hbm, wq_hbm, wk_hbm, wv_hbm, q_ref, pos_ref, ko_hbm, vo_hbm, xs, u, w, kv, knew, vnew, sem, out_sem):
    rows, width = xs.shape
    heads = q_ref.shape[0]
    hd = heads * LANE
    seq = kv.shape[2]
    half = LANE // 2
    base = lax.axis_index("sp") * seq
    n_x, n_out = 2, 4
    part = rows // n_x
    get_x = [pltpu.make_async_copy(x_hbm.at[i * part:(i + 1) * part], xs.at[i * part:(i + 1) * part], sem.at[i]) for i in range(n_x)]
    get_kv = [
        pltpu.make_async_copy(wk_hbm, w.at[:, hd:hd + LANE], sem.at[2]),
        pltpu.make_async_copy(wv_hbm, w.at[:, hd + LANE:], sem.at[3]),
    ]
    get_cache = [pltpu.make_async_copy(k_hbm, kv.at[0], sem.at[4]), pltpu.make_async_copy(v_hbm, kv.at[1], sem.at[5])]
    cuts = [(i, min(2 * LANE, hd - i)) for i in range(0, hd, 2 * LANE)]
    get_q = [pltpu.make_async_copy(wq_hbm.at[:, i:i + n], w.at[:, i:i + n], sem.at[6 + j]) for j, (i, n) in enumerate(cuts)]
    for copy in get_x:
        copy.start()
    then = [get_kv + get_cache, get_q]

    eye = lax.broadcasted_iota(jnp.int32, (LANE, LANE), 0) == lax.broadcasted_iota(jnp.int32, (LANE, LANE), 1)
    cols = []
    for i in range(rows // LANE):
        line = lens_row[i:i + 1, :].astype(F32)
        col = jnp.sum(jnp.where(eye, line, 0.0), axis=1, keepdims=True)
        pos_ref[i * LANE:(i + 1) * LANE, :] = jnp.broadcast_to(col, (LANE, LANE)).astype(jnp.int32)
        cols.append(col)
    low = lax.broadcasted_iota(jnp.int32, (LANE, LANE), 1) < half
    angles = jnp.where(low, cols[0], cols[1]) * freq_ref[...]
    cos = jnp.cos(angles)
    sin = jnp.sin(angles)
    cos_r = pltpu.roll(cos, half, 1)
    sin_r = pltpu.roll(sin, half, 1)
    cos_t = jnp.concatenate([jnp.where(low, cos, cos_r), jnp.where(low, cos_r, cos)], axis=0)
    sin_t = jnp.concatenate([jnp.where(low, -sin, sin_r), jnp.where(low, -sin_r, sin)], axis=0)

    def norm(i, carry):
        at = pl.ds(pl.multiple_of(i * GRP, GRP), GRP)
        x32 = xs[at, :].astype(F32)
        inv = lax.rsqrt(jnp.mean(x32 * x32, axis=-1, keepdims=True) + NORM_EPS)
        u[at, :] = (x32 * inv * g_ref[...].astype(F32)).astype(BF16)
        return carry

    for i in range(n_x):
        get_x[i].wait()
        for copy in then[i]:
            copy.start()
        lax.fori_loop(i * part // GRP, (i + 1) * part // GRP, norm, 0)

    def rope(t):
        return (t * cos_t + pltpu.roll(t, half, 1) * sin_t).astype(BF16)

    for copy in get_kv:
        copy.wait()
    out = jnp.dot(u[...], w[:, hd:], preferred_element_type=F32).astype(BF16).astype(F32)
    knew[...] = rope(out[:, :LANE]).astype(F32)
    vnew[...] = out[:, LANE:]
    for copy in get_cache:
        copy.wait()
    line = lax.broadcasted_iota(jnp.int32, (seq, LANE), 0)

    def put(i, carry):
        for j in range(GRP):
            b = i * GRP + j
            here = line == lens_ref[b] - base
            kv[0, b] = jnp.where(here, knew[pl.ds(b, 1), :], kv[0, b].astype(F32)).astype(BF16)
            kv[1, b] = jnp.where(here, vnew[pl.ds(b, 1), :], kv[1, b].astype(F32)).astype(BF16)
        return carry

    puts = []
    part = rows // n_out
    for i in range(n_out):
        lax.fori_loop(i * part // GRP, (i + 1) * part // GRP, put, 0)
        at = slice(i * part, (i + 1) * part)
        for j, ref in enumerate((ko_hbm, vo_hbm)):
            copy = pltpu.make_async_copy(kv.at[j, at], ref.at[at], out_sem.at[j, i])
            copy.start()
            puts.append(copy)
    for copy, (a, n) in zip(get_q, cuts):
        copy.wait()
        out = jnp.dot(u[...], w[:, a:a + n], preferred_element_type=F32).astype(BF16).astype(F32)
        for j in range(0, n, LANE):
            q_ref[(a + j) // LANE] = rope(out[:, j:j + LANE])
    for copy in puts:
        copy.wait()


def project(x_tok, seq_lens, k_blk, v_blk, g, wq, wk, wv):
    rows, width = x_tok.shape
    seq = k_blk.shape[1]
    hd = wq.shape[1]
    half = LANE // 2
    freq = np.float32(ROPE_BASE) ** (np.arange(half, dtype=np.float32) * np.float32(-2.0 / LANE))
    freq = jnp.asarray(np.concatenate([freq, freq]).reshape(1, LANE).astype(np.float32))
    vmem = pl.BlockSpec(memory_space=pltpu.VMEM)
    hbm = pl.BlockSpec(memory_space=pl.ANY)
    sem = pltpu.SemaphoreType.DMA
    cache = jax.ShapeDtypeStruct((rows, seq, LANE), BF16)
    return pl.pallas_call(
        project_kernel,
        name="project",
        out_shape=[
            jax.ShapeDtypeStruct((hd // LANE, rows, LANE), BF16),
            jax.ShapeDtypeStruct((rows, LANE), jnp.int32),
            cache,
            cache,
        ],
        in_specs=[pl.BlockSpec(memory_space=pltpu.SMEM), vmem, vmem, vmem] + [hbm] * 6,
        out_specs=[vmem, vmem, hbm, hbm],
        scratch_shapes=[
            pltpu.VMEM((rows, width), BF16),
            pltpu.VMEM((rows, width), BF16),
            pltpu.VMEM((width, hd + 2 * LANE), BF16),
            pltpu.VMEM((2, rows, seq, LANE), BF16),
            pltpu.VMEM((rows, LANE), F32),
            pltpu.VMEM((rows, LANE), F32),
            sem((10,)),
            sem((2, 4)),
        ],
        compiler_params=pltpu.CompilerParams(vmem_limit_bytes=VMEM_ALL),
    )(seq_lens, seq_lens.reshape(rows // LANE, LANE), g, freq, x_tok, k_blk.reshape(cache.shape), v_blk.reshape(cache.shape), wq, wk, wv)


def solution(mesh):
    cache_spec = P(None, "sp", "tp", None)
    col_spec = P(None, "tp")
    row_spec = P("tp", None)
    full_spec = P()

    def local_step(x_tok, seq_lens, k_blk, v_blk, g_attn, wq_loc, wk_loc, wv_loc, wo_loc, g_mlp, wg_loc, wu_loc, wd_loc):
        q, pos, ko, vo = project(x_tok, seq_lens, k_blk, v_blk, g_attn, wq_loc, wk_loc, wv_loc)
        y_out = layer(q, pos, x_tok, ko, vo, g_mlp, wo_loc, wg_loc, wu_loc, wd_loc)
        return y_out, ko.reshape(k_blk.shape), vo.reshape(v_blk.shape)

    return jax.shard_map(local_step, mesh=mesh, in_specs=(full_spec, full_spec, cache_spec, cache_spec, full_spec, col_spec, col_spec, col_spec, row_spec, full_spec, col_spec, col_spec, row_spec), out_specs=(full_spec, cache_spec, cache_spec), check_vma=False)
```

```python
import jax
import jax.numpy as jnp
import numpy as np
from jax import lax
from jax.experimental import pallas as pl
from jax.experimental.pallas import tpu as pltpu
from jax.sharding import PartitionSpec as P

ROPE_BASE = 500000.0
NORM_EPS = 1e-5
MESH = pl.DeviceIdType.MESH
F32 = jnp.float32
BF16 = jnp.bfloat16
NX, NZ, NY, NC = 4, 4, 4, 2
LANE = 128
VMEM_ALL = 67043328


def coords():
    s = lax.axis_index("sp")
    return lax.axis_index("tp"), s // (NY * NC), (s // NC) % NY, s % NC


def dev(x, z, y, c):
    return (x, (z * NY + y) * NC + c)


def turn(v, d, n):
    return lax.rem(v + d, n)


def entry_barrier(peers):
    barrier = pltpu.get_barrier_semaphore()
    for peer in peers:
        pl.semaphore_signal(barrier, inc=1, device_id=peer, device_id_type=MESH)
    pl.semaphore_wait(barrier, len(peers))


def remote(src, dst, send_sem, recv_sem, peer):
    return pltpu.make_async_remote_copy(
        src_ref=src, dst_ref=dst, send_sem=send_sem, recv_sem=recv_sem, device_id=peer, device_id_type=MESH
    )


XY = [(dx, dy) for dx in range(4) for dy in range(4)][1:]
WIN = 256


def layer_kernel(
    q_hbm, pos_hbm, g_hbm, x_hbm, k_hbm, v_hbm, wo_hbm, wg_hbm, wu_hbm, wd_hbm, out_hbm,
    q_ref, pos_ref, g_ref, kv, res, pack, swap, merged, slots, part, xslots, chunk, hid, hn, acts, acc, outs, cslot, buf,
    wg, wu, wd,
    w_sem, out_sem, in_sem, gv_send, gv_recv, rs_send, rs_recv, xs_send, xs_recv, ag_send, ag_recv, fw_send, fw_recv,
    c_send, c_recv, xo_send, xo_recv, p1_send, p1_recv, p2_send, p2_recv, cc_send, cc_recv,
):
    x, z, y, c = coords()
    w = chunk.shape[1]
    heads = w // LANE
    half = LANE // 2
    mate = turn(c, 1, NC)
    partner = dev(x, z, y, mate)
    steps = wg.shape[0]
    wide = steps * WIN
    ff = wg_hbm.shape[1]
    window = wide + LANE
    first = pl.multiple_of(c * (ff - window), LANE)
    keep = wd.shape[0] - wo_hbm.shape[0]

    def fetch(i):
        cols = pl.ds(pl.multiple_of(first + i * WIN, LANE), WIN)
        return (
            pltpu.make_async_copy(wg_hbm.at[:, cols], wg.at[i], w_sem.at[0, i]),
            pltpu.make_async_copy(wu_hbm.at[:, cols], wu.at[i], w_sem.at[1, i]),
        )

    def fetch_down(i):
        rows = pl.ds(pl.multiple_of(first + i * WIN, LANE), WIN)
        here = pl.ds(pl.multiple_of(i * WIN, LANE), WIN)
        return pltpu.make_async_copy(wd_hbm.at[rows, :], wd.at[here, :], w_sem.at[2, i])

    wg_t, wu_t = kv.at[0, :wg.shape[1], :], kv.at[1, :wu.shape[1], :]
    tail = pl.ds(pl.multiple_of(first + wide, LANE), LANE)
    tails = (
        pltpu.make_async_copy(wg_hbm.at[:, tail], wg_t, w_sem.at[0, steps]),
        pltpu.make_async_copy(wu_hbm.at[:, tail], wu_t, w_sem.at[1, steps]),
        pltpu.make_async_copy(wd_hbm.at[tail, :], wd.at[wide:, :], w_sem.at[2, steps]),
    )
    get_wo = pltpu.make_async_copy(wo_hbm, wd.at[keep:, :], w_sem.at[3, 0])
    n_keep = keep // WIN

    at_me = lax.axis_index("sp")
    get_in = [
        pltpu.make_async_copy(k_hbm, kv.at[0], in_sem.at[0]),
        pltpu.make_async_copy(v_hbm, kv.at[1], in_sem.at[1]),
        pltpu.make_async_copy(x_hbm.at[pl.ds(pl.multiple_of(at_me * 8, 8), 8), pl.ds(pl.multiple_of(x * w, LANE), w)], res, in_sem.at[2]),
        pltpu.make_async_copy(q_hbm, q_ref, in_sem.at[3]),
        pltpu.make_async_copy(pos_hbm, pos_ref, in_sem.at[4]),
        pltpu.make_async_copy(g_hbm, g_ref, in_sem.at[5]),
    ]
    for copy in (get_in[3], get_in[4], get_in[0], get_in[1], get_in[2], get_in[5]):
        copy.start()
    planes = [
        [(turn(x, a, NX), z, turn(y, b, NY)) for a, b in XY],
        [(x, turn(z, a, NZ), turn(y, b, NY)) for a, b in XY],
        [(turn(x, a, NX), turn(z, b, NZ), y) for a, b in XY],
    ]
    near = planes[0] + [(x, turn(z, a, NZ), turn(y, b, NY)) for a in range(1, NZ) for b in range(NY)]
    near += [(turn(x, a, NX), turn(z, b, NZ), y) for a in range(1, NX) for b in range(1, NZ)]
    entry_barrier([dev(*p, c) for p in near] + [partner])

    n_grp = NZ * NY
    seq = kv.shape[1] // q_ref.shape[1]
    span = GRP * seq
    low = lax.broadcasted_iota(jnp.int32, (8, LANE), 1) < half

    def far_first(i):
        return (2 + i + i // 2 + 2 * (i // 3)) % 4

    def place(k):
        return turn(z, far_first(k // NY), NZ), turn(y, far_first(k % NY), NY)

    def give(k):
        return remote(pack.at[k, mate], swap.at[k], gv_send.at[k], gv_recv.at[k], partner)

    def deliver(k):
        pz, py = place(k)
        return remote(merged.at[k], slots.at[k], rs_send.at[k], rs_recv.at[k], dev(x, pz, py, c))

    def attend(k):
        pz, py = place(k)
        g = pz * NY + py
        at = pl.ds(pl.multiple_of(g * GRP, GRP), GRP)
        keys = pl.ds(pl.multiple_of(g * span, span), span)
        qs = jnp.concatenate([q_ref[h, at, :] for h in range(heads)], axis=0)
        col = lax.broadcasted_iota(jnp.int32, (GRP, span), 1)
        own = (col // seq) == lax.broadcasted_iota(jnp.int32, (GRP, span), 0)
        p = jnp.concatenate([pos_ref[at, :]] * (span // LANE), axis=1)
        valid = own & (at_me * seq + col % seq <= p)
        valid = jnp.concatenate([valid.astype(F32)] * heads, axis=0) > 0.5
        scores = lax.dot_general(qs, kv[0, keys, :], (((1,), (1,)), ((), ())), preferred_element_type=F32) * (LANE ** -0.5)
        scores = jnp.where(valid, scores, -1e30)
        top = jnp.max(scores, axis=1, keepdims=True)
        wt = jnp.where(valid, jnp.exp(scores - top), 0.0)
        tot = jnp.sum(wt, axis=1, keepdims=True)
        mix = jnp.dot(wt.astype(BF16), kv[1, keys, :], preferred_element_type=F32)
        lane = lax.broadcasted_iota(jnp.int32, (8, LANE), 1)
        for e in range(NC):
            stats = jnp.zeros((8, LANE), F32)
            for h in range(heads):
                rows = slice(h * GRP + e * 8, h * GRP + e * 8 + 8)
                pack[k, e, :, h * LANE:(h + 1) * LANE] = mix[rows]
                stats = jnp.where(lane == h, top[rows], stats)
                stats = jnp.where(lane == half + h, tot[rows], stats)
            pack[k, e, :, w:] = stats
        give(k).start()

    def pair(k):
        give(k).wait_recv()
        s1, s2 = pack[k, c, :, w:], swap[k, :, w:]
        top = jnp.maximum(s1, s2)
        f1, f2 = jnp.exp(s1 - top), jnp.exp(s2 - top)
        total = pltpu.roll(f1, half, 1) * s1 + pltpu.roll(f2, half, 1) * s2
        mix = []
        for h in range(heads):
            cut = slice(h * LANE, (h + 1) * LANE)
            mix.append(f1[:, h:h + 1] * pack[k, c, :, cut] + f2[:, h:h + 1] * swap[k, :, cut])
        return mix, jnp.where(low, top, total)

    def pass_on(k):
        mix, stats = pair(k)
        for h in range(heads):
            merged[k, :, h * LANE:(h + 1) * LANE] = mix[h]
        merged[k, :, w:] = stats
        deliver(k).start()

    lag = 4
    for i in (0, 1, 3, 4):
        get_in[i].wait()
    get_wo.start()
    fetch(0)[0].start()

    def begin(k, carry):
        attend(k)
        return carry

    def both(k, carry):
        for j in (2 * k, 2 * k + 1):
            attend(j)
            pass_on(j - lag)
        fetch(k - lag // 2 + 1)[0].start()
        return carry

    def finish(k, carry):
        pass_on(k)
        return carry

    lax.fori_loop(0, lag, begin, 0)
    lax.fori_loop(lag // 2, n_grp // 2, both, 0)
    lax.fori_loop(n_grp - lag, n_grp - 1, finish, 0)
    rs = [deliver(k) for k in range(n_grp - 1)]
    gives = [give(k) for k in range(n_grp)]
    early = 1 + (n_grp - lag) // 2
    for i in range(steps):
        fetch(i)[1].start()
    for i in range(early, steps):
        fetch(i)[0].start()
    fetch_down(0).start()
    own_mix, own_stats = pair(n_grp - 1)
    for copy in rs:
        copy.wait_recv()
    top = own_stats
    for k in range(len(rs)):
        top = jnp.maximum(top, slots[k, :, w:])

    def add(stats, mix, acc_mix, total):
        factor = jnp.exp(stats - top)
        total = total + pltpu.roll(factor, half, 1) * stats
        return [acc_mix[h] + factor[:, h:h + 1] * mix[h] for h in range(heads)], total

    mixed, total = add(own_stats, own_mix, [jnp.zeros((8, LANE), F32)] * heads, jnp.zeros((8, LANE), F32))
    for k in range(len(rs)):
        mix = [slots[k, :, h * LANE:(h + 1) * LANE] for h in range(heads)]
        mixed, total = add(slots[k, :, w:], mix, mixed, total)
    attn = jnp.concatenate([mixed[h] / total[:, half + h:half + h + 1] for h in range(heads)], axis=1).astype(BF16)

    get_wo.wait()
    my_cols = pl.ds(pl.multiple_of(x * w, LANE), w)
    my_rows = pl.ds(pl.multiple_of(c * 8, 8), 8)
    line = [turn(x, k, NX) for k in range(1, NX)]
    cols = [pl.ds(pl.multiple_of(px * w, LANE), w) for px in line]
    hops = (2, 1, 3, 0)
    xs = []
    for j, hop in enumerate(hops):
        px = turn(x, hop, NX)
        own = pl.ds(pl.multiple_of(px * w, LANE), w)
        here = slice(j * w, (j + 1) * w)
        part[:, here] = jnp.dot(attn, wd[keep:, own], preferred_element_type=F32)
        if hop:
            copy = remote(part.at[:, here], xslots.at[j], xs_send.at[j], xs_recv.at[j], dev(px, z, y, c))
            copy.start()
            xs.append(copy)
    for i in range(1, 5):
        fetch_down(i).start()
    sums = part[:, 3 * w:]
    for k, copy in enumerate(xs):
        copy.wait_recv()
        sums = sums + xslots[k]
    get_in[2].wait()
    hidden = (res[...].astype(F32) + sums).astype(BF16).astype(F32)
    chunk[...] = hidden
    ag = [None] * 3
    for k in (1, 0, 2):
        ag[k] = remote(chunk, hid.at[my_rows, my_cols], ag_send.at[k], ag_recv.at[k], dev(line[k], z, y, c))
        ag[k].start()
    fw = [remote(chunk, hid.at[my_rows, my_cols], fw_send.at[3], fw_recv.at[3], partner)]
    fw[0].start()
    hid[my_rows, my_cols] = hidden
    for i in range(5, steps):
        fetch_down(i).start()
    for copy in tails:
        copy.start()
    for k in (0, 2, 1):
        ag[k].wait_recv()
        block = hid.at[my_rows, cols[2 - k]]
        copy = remote(block, block, fw_send.at[k], fw_recv.at[k], partner)
        copy.start()
        fw.append(copy)
    for copy in fw:
        copy.wait_recv()

    get_in[5].wait()

    h32 = hid[...]
    inv = lax.rsqrt(jnp.mean(h32 * h32, axis=-1, keepdims=True) + NORM_EPS)
    hn[...] = (h32 * inv * g_ref[...].astype(F32)).astype(BF16)
    mid = (ff // LANE + 1) // 2 * LANE

    def gated(gate, up, start):
        gate = gate.astype(BF16).astype(F32)
        up = up.astype(BF16).astype(F32)
        col = lax.broadcasted_iota(jnp.int32, gate.shape, 1) + start
        lo = c * mid
        act = jax.nn.silu(gate) * up
        return jnp.where((col >= lo) & (col < mid + c * ff), act, 0.0).astype(BF16)

    def mlp_step(i, carry):
        cg, cu = fetch(i)
        cg.wait()
        gate = jnp.dot(hn[...], wg[i], preferred_element_type=F32)
        cu.wait()
        up = jnp.dot(hn[...], wu[i], preferred_element_type=F32)
        act = gated(gate, up, first + i * WIN)
        acts[:, pl.ds(pl.multiple_of(i * WIN, LANE), WIN)] = act
        return carry

    lax.fori_loop(0, steps, mlp_step, 0)
    tails[0].wait()
    gate = jnp.dot(hn[...], wg_t[...], preferred_element_type=F32)
    tails[1].wait()
    up = jnp.dot(hn[...], wu_t[...], preferred_element_type=F32)
    acts[:, wide:] = gated(gate, up, first + wide)
    for i in range(steps):
        fetch_down(i).wait()
    tails[2].wait()

    mate_rows = pl.ds(pl.multiple_of(mate * 8, 8), 8)
    back, xo = [], []

    def to_owner(j):
        back[j].wait_recv()
        outs[j] = acc[j, my_rows, :] + cslot[j]
        owner = dev(turn(x, hops[j], NX), z, y, c)
        copy = remote(outs.at[j], xslots.at[j + 3], xo_send.at[j], xo_recv.at[j], owner)
        copy.start()
        xo.append(copy)

    for j, hop in enumerate(hops):
        own = pl.ds(pl.multiple_of(turn(x, hop, NX) * w, LANE), w)
        acc[j] = jnp.dot(acts[...], wd[:, own], preferred_element_type=F32)
        copy = remote(acc.at[j, mate_rows, :], cslot.at[j], c_send.at[j], c_recv.at[j], partner)
        copy.start()
        back.append(copy)
        if j >= 2:
            to_owner(j - 2)
    to_owner(2)
    back[3].wait_recv()
    sums = acc[3, my_rows, :] + cslot[3]
    for copy in xs:
        copy.wait_send()
    for k, copy in enumerate(xo):
        copy.wait_recv()
        sums = sums + xslots[k + 3]
    out = (hidden + sums).astype(BF16).astype(F32)
    for copy in ag + fw[:1]:
        copy.wait_send()
    chunk[...] = out

    cut = [(0, 2 * LANE), (2 * LANE, 2 * LANE), (4 * LANE, w - 4 * LANE)]
    order = (0, 1, 3, 2)
    p1 = {}
    for d in order:
        for p, (lo, n) in enumerate(cut):
            for k in range(15):
                if XY[k][1] == d:
                    src, dst = chunk.at[:, lo:lo + n], buf.at[z, y, c, x, :, lo:lo + n]
                    p1[p, k] = remote(src, dst, p1_send.at[p, k], p1_recv.at[p, k], dev(*planes[p][k], c))
                    p1[p, k].start()
    buf[z, y, c, x] = out

    def line_of(p, v, d):
        lo, n = cut[p]
        cols_p = slice(lo, lo + n)
        b = turn((y, y, z)[p], (4 - d) % 4, 4)
        return [buf.at[v, b, c, :, :, cols_p], buf.at[:, b, c, v, :, cols_p], buf.at[b, v, c, :, :, cols_p]][p]

    here = [z, x, y]
    up1 = [dev(x, turn(z, 1, 4), y, c), dev(turn(x, 1, 4), z, y, c), dev(x, z, turn(y, 1, 4), c)]
    dn1 = [dev(x, turn(z, 3, 4), y, c), dev(turn(x, 3, 4), z, y, c), dev(x, z, turn(y, 3, 4), c)]
    far1 = [dev(x, turn(z, 2, 4), y, c), dev(turn(x, 2, 4), z, y, c), dev(x, z, turn(y, 2, 4), c)]
    done, crossed = [], []

    def send(p, v, d, to, kind):
        ref = line_of(p, v, d)
        copy = remote(ref, ref, p2_send.at[p, kind * 4 + d], p2_recv.at[p, kind * 4 + d], to)
        copy.start()
        done.append(copy)
        return copy

    def across(p, v, d, kind):
        ref = line_of(p, v, d)
        copy = remote(ref, ref, cc_send.at[p, kind * 4 + d], cc_recv.at[p, kind * 4 + d], partner)
        copy.start()
        done.append(copy)
        crossed.append(copy)

    ups, downs, relays = {}, {}, {}
    for d in order:
        for p in range(3):
            for k in range(15):
                if XY[k][1] == d:
                    p1[p, k].wait_recv()
            ups[p, d] = send(p, here[p], d, up1[p], 0)
            downs[p, d] = send(p, here[p], d, dn1[p], 1)
            if d == 2:
                relays[p, d] = send(p, here[p], d, far1[p], 2)
            across(p, here[p], d, 0)
    for d in order:
        for p in range(3):
            below, above = turn(here[p], 3, 4), turn(here[p], 1, 4)
            ups[p, d].wait_recv()
            if d < 2:
                relays[p, d] = send(p, below, d, up1[p], 2)
            downs[p, d].wait_recv()
            if d == 3:
                relays[p, d] = send(p, above, d, dn1[p], 2)
            across(p, below, d, 1)
            across(p, above, d, 2)
    for d in order:
        for p in range(3):
            relays[p, d].wait_recv()
            across(p, turn(here[p], 2, 4), d, 3)
    for copy in crossed:
        copy.wait_recv()
    puts = []
    for a in range(NZ):
        for b in range(NY):
            for e in range(NC):
                r = ((a * NY + b) * NC + e) * 8
                for d in range(NX):
                    wd[r:r + 8, d * w:(d + 1) * w] = buf[a, b, e, d].astype(BF16)
        at = slice(a * NY * NC * 8, (a + 1) * NY * NC * 8)
        put = pltpu.make_async_copy(wd.at[at, :], out_hbm.at[at, :], out_sem.at[a])
        put.start()
        puts.append(put)
    for copy in gives + back + rs + fw[1:] + xo + list(p1.values()) + done:
        copy.wait_send()
    for put in puts:
        put.wait()


def layer(q, pos, x_tok, ko, vo, g, wo, wg, wu, wd):
    rows, width = x_tok.shape
    w = width // NX
    keys = rows * ko.shape[1]
    steps = ((wg.shape[1] // LANE + 1) // 2 * LANE) // WIN
    sem = pltpu.SemaphoreType.DMA
    hbm = pl.BlockSpec(memory_space=pl.ANY)
    return pl.pallas_call(
        layer_kernel,
        name="layer",
        out_shape=jax.ShapeDtypeStruct((rows, width), BF16),
        in_specs=[hbm] * 10,
        out_specs=hbm,
        scratch_shapes=[
            pltpu.VMEM(q.shape, BF16),
            pltpu.VMEM(pos.shape, jnp.int32),
            pltpu.VMEM(g.shape, BF16),
            pltpu.VMEM((2, keys, LANE), BF16),
            pltpu.VMEM((8, w), BF16),
            pltpu.VMEM((NZ * NY, NC, 8, w + LANE), F32),
            pltpu.VMEM((NZ * NY, 8, w + LANE), F32),
            pltpu.VMEM((15, 8, w + LANE), F32),
            pltpu.VMEM((15, 8, w + LANE), F32),
            pltpu.VMEM((8, width), F32),
            pltpu.VMEM((6, 8, w), F32),
            pltpu.VMEM((8, w), F32),
            pltpu.VMEM((8 * NC, width), F32),
            pltpu.VMEM((8 * NC, width), BF16),
            pltpu.VMEM((8 * NC, steps * WIN + LANE), BF16),
            pltpu.VMEM((NX, 8 * NC, w), F32),
            pltpu.VMEM((NX - 1, 8, w), F32),
            pltpu.VMEM((NX, 8, w), F32),
            pltpu.VMEM((NZ, NY, NC, NX, 8, w), F32),
            pltpu.VMEM((steps, width, WIN), BF16),
            pltpu.VMEM((steps, width, WIN), BF16),
            pltpu.VMEM((steps * WIN + LANE, width), BF16),
            sem((4, steps + 1)),
            sem((NZ,)),
            sem((6,)), sem((16,)), sem((16,)), sem((15,)), sem((15,)), sem((3,)), sem((3,)), sem((3,)), sem((3,)), sem((4,)), sem((4,)),
            sem((4,)), sem((4,)), sem((3,)), sem((3,)), sem((3, 15)), sem((3, 15)), sem((3, 12)), sem((3, 12)), sem((3, 16)), sem((3, 16)),
        ],
        compiler_params=pltpu.CompilerParams(collective_id=0, has_side_effects=True, vmem_limit_bytes=VMEM_ALL),
    )(q, pos, g, x_tok, ko.reshape(keys, LANE), vo.reshape(keys, LANE), wo, wg, wu, wd)


GRP = 16


def project_kernel(lens_ref, lens_row, g_ref, freq_ref, x_hbm, k_hbm, v_hbm, wq_hbm, wk_hbm, wv_hbm, q_ref, pos_ref, ko_hbm, vo_hbm, xs, u, w, kv, knew, vnew, sem, out_sem):
    rows, width = xs.shape
    heads = q_ref.shape[0]
    hd = heads * LANE
    seq = kv.shape[2]
    half = LANE // 2
    base = lax.axis_index("sp") * seq
    n_x, n_out = 2, 4
    part = rows // n_x
    get_x = [pltpu.make_async_copy(x_hbm.at[i * part:(i + 1) * part], xs.at[i * part:(i + 1) * part], sem.at[i]) for i in range(n_x)]
    get_kv = [
        pltpu.make_async_copy(wk_hbm, w.at[:, hd:hd + LANE], sem.at[2]),
        pltpu.make_async_copy(wv_hbm, w.at[:, hd + LANE:], sem.at[3]),
    ]
    get_cache = [pltpu.make_async_copy(k_hbm, kv.at[0], sem.at[4]), pltpu.make_async_copy(v_hbm, kv.at[1], sem.at[5])]
    cuts = [(i, min(2 * LANE, hd - i)) for i in range(0, hd, 2 * LANE)]
    get_q = [pltpu.make_async_copy(wq_hbm.at[:, i:i + n], w.at[:, i:i + n], sem.at[6 + j]) for j, (i, n) in enumerate(cuts)]
    for copy in get_x:
        copy.start()
    then = [get_kv + get_cache, get_q]

    eye = lax.broadcasted_iota(jnp.int32, (LANE, LANE), 0) == lax.broadcasted_iota(jnp.int32, (LANE, LANE), 1)
    cols = []
    for i in range(rows // LANE):
        line = lens_row[i:i + 1, :].astype(F32)
        col = jnp.sum(jnp.where(eye, line, 0.0), axis=1, keepdims=True)
        pos_ref[i * LANE:(i + 1) * LANE, :] = jnp.broadcast_to(col, (LANE, LANE)).astype(jnp.int32)
        cols.append(col)
    low = lax.broadcasted_iota(jnp.int32, (LANE, LANE), 1) < half
    angles = jnp.where(low, cols[0], cols[1]) * freq_ref[...]
    cos = jnp.cos(angles)
    sin = jnp.sin(angles)
    cos_r = pltpu.roll(cos, half, 1)
    sin_r = pltpu.roll(sin, half, 1)
    cos_t = jnp.concatenate([jnp.where(low, cos, cos_r), jnp.where(low, cos_r, cos)], axis=0)
    sin_t = jnp.concatenate([jnp.where(low, -sin, sin_r), jnp.where(low, -sin_r, sin)], axis=0)

    def norm(i, carry):
        at = pl.ds(pl.multiple_of(i * GRP, GRP), GRP)
        x32 = xs[at, :].astype(F32)
        inv = lax.rsqrt(jnp.mean(x32 * x32, axis=-1, keepdims=True) + NORM_EPS)
        u[at, :] = (x32 * inv * g_ref[...].astype(F32)).astype(BF16)
        return carry

    for i in range(n_x):
        get_x[i].wait()
        for copy in then[i]:
            copy.start()
        lax.fori_loop(i * part // GRP, (i + 1) * part // GRP, norm, 0)

    def rope(t):
        return (t * cos_t + pltpu.roll(t, half, 1) * sin_t).astype(BF16)

    for copy in get_kv:
        copy.wait()
    out = jnp.dot(u[...], w[:, hd:], preferred_element_type=F32).astype(BF16).astype(F32)
    knew[...] = rope(out[:, :LANE]).astype(F32)
    vnew[...] = out[:, LANE:]
    for copy in get_cache:
        copy.wait()
    line = lax.broadcasted_iota(jnp.int32, (seq, LANE), 0)

    def put(i, carry):
        for j in range(GRP):
            b = i * GRP + j
            here = line == lens_ref[b] - base
            kv[0, b] = jnp.where(here, knew[pl.ds(b, 1), :], kv[0, b].astype(F32)).astype(BF16)
            kv[1, b] = jnp.where(here, vnew[pl.ds(b, 1), :], kv[1, b].astype(F32)).astype(BF16)
        return carry

    puts = []
    part = rows // n_out
    for i in range(n_out):
        lax.fori_loop(i * part // GRP, (i + 1) * part // GRP, put, 0)
        at = slice(i * part, (i + 1) * part)
        for j, ref in enumerate((ko_hbm, vo_hbm)):
            copy = pltpu.make_async_copy(kv.at[j, at], ref.at[at], out_sem.at[j, i])
            copy.start()
            puts.append(copy)
    for copy, (a, n) in zip(get_q, cuts):
        copy.wait()
        out = jnp.dot(u[...], w[:, a:a + n], preferred_element_type=F32).astype(BF16).astype(F32)
        for j in range(0, n, LANE):
            q_ref[(a + j) // LANE] = rope(out[:, j:j + LANE])
    for copy in puts:
        copy.wait()


def project(x_tok, seq_lens, k_blk, v_blk, g, wq, wk, wv):
    rows, width = x_tok.shape
    seq = k_blk.shape[1]
    hd = wq.shape[1]
    half = LANE // 2
    freq = np.float32(ROPE_BASE) ** (np.arange(half, dtype=np.float32) * np.float32(-2.0 / LANE))
    freq = jnp.asarray(np.concatenate([freq, freq]).reshape(1, LANE).astype(np.float32))
    vmem = pl.BlockSpec(memory_space=pltpu.VMEM)
    hbm = pl.BlockSpec(memory_space=pl.ANY)
    sem = pltpu.SemaphoreType.DMA
    cache = jax.ShapeDtypeStruct((rows, seq, LANE), BF16)
    return pl.pallas_call(
        project_kernel,
        name="project",
        out_shape=[
            jax.ShapeDtypeStruct((hd // LANE, rows, LANE), BF16),
            jax.ShapeDtypeStruct((rows, LANE), jnp.int32),
            cache,
            cache,
        ],
        in_specs=[pl.BlockSpec(memory_space=pltpu.SMEM), vmem, vmem, vmem] + [hbm] * 6,
        out_specs=[vmem, vmem, hbm, hbm],
        scratch_shapes=[
            pltpu.VMEM((rows, width), BF16),
            pltpu.VMEM((rows, width), BF16),
            pltpu.VMEM((width, hd + 2 * LANE), BF16),
            pltpu.VMEM((2, rows, seq, LANE), BF16),
            pltpu.VMEM((rows, LANE), F32),
            pltpu.VMEM((rows, LANE), F32),
            sem((10,)),
            sem((2, 4)),
        ],
        compiler_params=pltpu.CompilerParams(vmem_limit_bytes=VMEM_ALL),
    )(seq_lens, seq_lens.reshape(rows // LANE, LANE), g, freq, x_tok, k_blk.reshape(cache.shape), v_blk.reshape(cache.shape), wq, wk, wv)


def solution(mesh):
    cache_spec = P(None, "sp", "tp", None)
    col_spec = P(None, "tp")
    row_spec = P("tp", None)
    full_spec = P()

    def local_step(x_tok, seq_lens, k_blk, v_blk, g_attn, wq_loc, wk_loc, wv_loc, wo_loc, g_mlp, wg_loc, wu_loc, wd_loc):
        q, pos, ko, vo = project(x_tok, seq_lens, k_blk, v_blk, g_attn, wq_loc, wk_loc, wv_loc)
        y_out = layer(q, pos, x_tok, ko, vo, g_mlp, wo_loc, wg_loc, wu_loc, wd_loc)
        return y_out, ko.reshape(k_blk.shape), vo.reshape(v_blk.shape)

    return jax.shard_map(local_step, mesh=mesh, in_specs=(full_spec, full_spec, cache_spec, cache_spec, full_spec, col_spec, col_spec, col_spec, row_spec, full_spec, col_spec, col_spec, row_spec), out_specs=(full_spec, cache_spec, cache_spec), check_vma=False)
```
